256 devices in a mesh: seq: 64 (over y, z, core), mp: 4 (over x).
Axes of the slice: x: 4, y: 4, z: 8, core: 2. Of those that a mesh axis runs over, the one named last changes fastest.
Arguments:
- hidden_in: bfloat16 [2, 8192, 2048], P(None, 'seq'), may hold values from -6 to 6
- attn_gain: float32 [2048], replicated, may hold values from 0.1 to 1.9
- q_weight: bfloat16 [2048, 2048], P(None, 'mp'), may hold values from -0.125 to 0.125
- q_bias: float32 [2048], P('mp'), may hold values from -60 to 60
- k_weight: bfloat16 [2048, 256], replicated, may hold values from -0.125 to 0.125
- k_bias: float32 [256], replicated, may hold values from -60 to 60
- v_weight: bfloat16 [2048, 256], replicated, may hold values from -0.125 to 0.125
- v_bias: float32 [256], replicated, may hold values from -3 to 3
- o_weight: bfloat16 [2048, 2048], P('mp'), may hold values from -0.125 to 0.125
- mlp_gain: float32 [2048], replicated, may hold values from 0.1 to 1.9
- gate_weight: bfloat16 [2048, 5632], P('seq', 'mp'), may hold values from -0.125 to 0.125
- up_weight: bfloat16 [2048, 5632], P('seq', 'mp'), may hold values from -0.125 to 0.125
- down_weight: bfloat16 [2048, 5632], P('seq', 'mp'), may hold values from -0.078125 to 0.078125
- lengths: int32 [2], replicated, may hold values from 4096 to 8192
Outputs:
- layer_out: bfloat16 [2, 8192, 2048], P(None, 'seq', 'mp')
- influence: float32 [2, 8192], P(None, 'seq')
- score: float32 [2], replicated
The draws below stay inside these ranges and needn't reach their ends.
Inputs may be any that keep to these rules, and one draw needn't show every extreme that they name: `lengths`: tokens at positions 4096 and later may be invalid.
All inputs are finite; a program needn't handle non-finite values.
Results may differ from the reference program's by a relative error of at most 0.02.
The reference program's roundings to bfloat16 on the way (of `normed`, `attn`, `residual`, `mlp_in` and `activated`) count: a program that leaves them out, or rounds other values in their place, can miss the bound.
Values may be sent and summed in bfloat16 or wider, within the bound.
A program may use at most 192 MiB of HBM per device.

```python
import jax
import jax.numpy as jnp
from jax import lax

D = 2048
HEADS = 16
KV_HEADS = 2
HEAD = 128
FF = 5632
SEQS = 2
SEQ_LEN = 8192
N_MP = 4


def draw_q_bias(key, part):
    noise = jax.random.normal(jax.random.fold_in(key, 11), (HEADS * HEAD,), jnp.float32)
    return jnp.clip(noise * 0.5, -3.0, 3.0)


def draw_k_bias(key, part):
    noise = jax.random.normal(jax.random.fold_in(key, 12), (KV_HEADS * HEAD,), jnp.float32)
    return jnp.clip(noise * 0.5, -3.0, 3.0)


def shard_levels(stream_key, dims, shards, low, top_value):
    factor_of, own = 1.0, jax.random.fold_in(stream_key, 6)
    for axis_at, parts in shards:
        steps = jnp.exp(jax.random.uniform(jax.random.fold_in(own, axis_at), (parts,), jnp.float32, low / len(shards), top_value / len(shards)))
        factor_of = factor_of * jnp.repeat(steps, dims[axis_at] // parts).reshape([-1 if axis == axis_at else 1 for axis in range(len(dims))])
    return factor_of


def centred(key, shape, scale, most, cuts=(), held_as=jnp.bfloat16):
    drawn = scale * jax.random.normal(key, shape, jnp.float32)
    if cuts:
        drawn = drawn * shard_levels(key, shape, cuts, -0.22, 0.18)
    return jnp.clip(drawn, -most, most).astype(held_as)


def setup_inputs(seed: int = 0) -> dict:
    seeds = jax.random.split(jax.random.key(seed), 15)
    return {
        "hidden_in": centred(seeds[0], (SEQS, SEQ_LEN, D), 1.0, 6.0, ((1, 64),)),
        "attn_gain": jnp.clip(1.0 + 0.18 * jax.random.normal(seeds[1], (D,), jnp.float32), 0.1, 1.9),
        "q_weight": centred(seeds[2], (D, HEADS * HEAD), D ** -0.5, 0.125, ((1, 4),)),
        "q_bias": draw_q_bias(jax.random.fold_in(seeds[14], 71), 0),
        "k_weight": centred(seeds[4], (D, KV_HEADS * HEAD), D ** -0.5, 0.125),
        "k_bias": draw_k_bias(jax.random.fold_in(seeds[14], 71), 0),
        "v_weight": centred(seeds[6], (D, KV_HEADS * HEAD), D ** -0.5, 0.125),
        "v_bias": centred(seeds[7], (KV_HEADS * HEAD,), 0.5, 3.0, (), jnp.float32),
        "o_weight": centred(seeds[8], (HEADS * HEAD, D), (HEADS * HEAD) ** -0.5, 0.125, ((0, 4),)),
        "mlp_gain": jnp.clip(1.0 + 0.18 * jax.random.normal(seeds[9], (D,), jnp.float32), 0.1, 1.9),
        "gate_weight": centred(seeds[10], (D, FF), D ** -0.5, 0.125, ((0, 64), (1, 4))),
        "up_weight": centred(seeds[11], (D, FF), D ** -0.5, 0.125, ((0, 64), (1, 4))),
        "down_weight": centred(seeds[12], (D, FF), FF ** -0.5, 0.078125, ((0, 64), (1, 4))),
        "lengths": jax.random.randint(seeds[13], (SEQS,), SEQ_LEN // 2, SEQ_LEN + 1).astype(jnp.int32),
    }


rope_base = 1000000.0
norm_eps = 1e-06
masked_score = -1e+30

def rms_scale(values, gain):
    widened = values.astype(jnp.float32)
    factor = lax.rsqrt(lax.optimization_barrier(jnp.mean(widened * widened, axis=-1, keepdims=True)) + norm_eps)
    return (widened * factor * gain.astype(jnp.float32)).astype(jnp.bfloat16)

def rotate(values, positions):
    head_width = values.shape[-1]
    half_width = head_width // 2
    inv_freq = rope_base ** (-(jnp.arange(half_width, dtype=jnp.float32) * 2.0) / head_width)
    angles = positions.astype(jnp.float32)[:, None] * inv_freq[None, :]
    angles = jnp.concatenate([angles, angles], axis=-1)
    first_part = values[..., :half_width]
    second_part = values[..., half_width:]
    turned = jnp.concatenate([-second_part, first_part], axis=-1)
    return values * jnp.cos(angles) + turned * jnp.sin(angles)

def round_trip(values):
    return lax.optimization_barrier(values.astype(jnp.bfloat16)).astype(jnp.float32)

def reference(hidden_in, attn_gain, q_weight, q_bias, k_weight, k_bias, v_weight, v_bias, o_weight, mlp_gain, gate_weight, up_weight, down_weight, lengths):
    seqs_n, seq_len, width = hidden_in.shape
    flat_in = hidden_in.reshape(seqs_n * seq_len, width)
    normed = rms_scale(flat_in, attn_gain)
    query_all = jnp.dot(normed, q_weight, preferred_element_type=jnp.float32) + q_bias
    key_all = jnp.dot(normed, k_weight, preferred_element_type=jnp.float32) + k_bias
    value_all = (jnp.dot(normed, v_weight, preferred_element_type=jnp.float32) + v_bias).astype(jnp.bfloat16)
    positions = jnp.arange(seq_len, dtype=jnp.int32)
    queries = rotate(query_all.reshape(seqs_n, seq_len, HEADS, HEAD).transpose(0, 2, 1, 3), positions).astype(jnp.bfloat16)
    keys = rotate(key_all.reshape(seqs_n, seq_len, KV_HEADS, HEAD).transpose(0, 2, 1, 3), positions).astype(jnp.bfloat16)
    values = value_all.reshape(seqs_n, seq_len, KV_HEADS, HEAD).transpose(0, 2, 1, 3)
    group_size = HEADS // KV_HEADS
    score_scale = HEAD ** (-0.5)
    allowed = positions[None, :] <= positions[:, None]

    def one_head(index):
        seq_index = index // HEADS
        head_index = index % HEADS
        query_rows = queries[seq_index, head_index]
        key_rows = keys[seq_index, head_index // group_size]
        value_rows = values[seq_index, head_index // group_size]
        scores = jnp.dot(query_rows, key_rows.T, preferred_element_type=jnp.float32) * score_scale
        scores = jnp.where(allowed, scores, masked_score)
        top_score = lax.optimization_barrier(jnp.max(scores, axis=-1, keepdims=True))
        weights = jnp.where(allowed, jnp.exp(scores - top_score), 0.0)
        totals = lax.optimization_barrier(jnp.sum(weights, axis=-1, keepdims=True))
        mixed = jnp.dot(weights.astype(jnp.bfloat16), value_rows, preferred_element_type=jnp.float32)
        return (mixed / totals).astype(jnp.bfloat16)
    attn = lax.map(one_head, jnp.arange(seqs_n * HEADS, dtype=jnp.int32))
    attn = attn.reshape(seqs_n, HEADS, seq_len, HEAD).transpose(0, 2, 1, 3).reshape(seqs_n * seq_len, HEADS * HEAD)
    group_cols = HEADS // N_MP * HEAD
    attn_out = jnp.zeros((seqs_n * seq_len, width), jnp.float32)
    for group in range(N_MP):
        partial_out = jnp.dot(attn[:, group * group_cols:(group + 1) * group_cols], o_weight[group * group_cols:(group + 1) * group_cols], preferred_element_type=jnp.float32)
        attn_out = attn_out + round_trip(partial_out)
    residual = (flat_in.astype(jnp.float32) + attn_out).astype(jnp.bfloat16)
    mlp_in = rms_scale(residual, mlp_gain)
    gate_sum = jnp.dot(mlp_in, gate_weight, preferred_element_type=jnp.float32)
    up_sum = jnp.dot(mlp_in, up_weight, preferred_element_type=jnp.float32)
    activated = (jax.nn.silu(gate_sum) * up_sum).astype(jnp.bfloat16)
    ff_cols = FF // N_MP
    mlp_out = jnp.zeros((seqs_n * seq_len, width), jnp.float32)
    for group in range(N_MP):
        partial_out = jnp.dot(activated[:, group * ff_cols:(group + 1) * ff_cols], down_weight[:, group * ff_cols:(group + 1) * ff_cols].T, preferred_element_type=jnp.float32)
        mlp_out = mlp_out + round_trip(partial_out)
    layer_out = (residual.astype(jnp.float32) + mlp_out).astype(jnp.bfloat16)
    in_wide = flat_in.astype(jnp.float32)
    out_wide = layer_out.astype(jnp.float32)
    cross = lax.optimization_barrier(jnp.sum(in_wide * out_wide, axis=-1)).reshape(seqs_n, seq_len)
    in_norm = lax.optimization_barrier(jnp.sum(in_wide * in_wide, axis=-1)).reshape(seqs_n, seq_len)
    out_norm = lax.optimization_barrier(jnp.sum(out_wide * out_wide, axis=-1)).reshape(seqs_n, seq_len)
    cosine = cross / jnp.sqrt((in_norm + norm_eps) * (out_norm + norm_eps))
    valid = positions[None, :] < lengths[:, None]
    influence = jnp.where(valid, 1.0 - cosine, 0.0)
    score = lax.optimization_barrier(jnp.sum(influence, axis=1)) / lengths.astype(jnp.float32)
    return (layer_out.reshape(seqs_n, seq_len, width), influence, score)
```

```python
import jax
import jax.numpy as jnp
from jax import lax
from jax.experimental import pallas as pl
from jax.experimental.pallas import tpu as pltpu
from jax.sharding import PartitionSpec as P

HEADS = 16
KV_HEADS = 2
HEAD = 128
D = 2048
NY, NZ = 4, 8
MP = 4
TOK = 128
ROWS = 2 * TOK
OWN_HEADS = HEADS // MP
QCOLS = OWN_HEADS * HEAD
QUART = D // MP
FFP = 1408
WR = 32

rope_base = 1000000.0
norm_eps = 1e-06
masked_score = -1e30
EXP2_SCALE = HEAD ** (-0.5) * 1.4426950408889634

MESH = pl.DeviceIdType.MESH
F32, BF16 = jnp.float32, jnp.bfloat16

Z_OFF = (0, -1, 1, -2, 2, -3, 3, -4)


def layer_kernel(
    hid_hbm, ag_ref, qw_hbm, qb_ref, kw_hbm, kb_ref, vw_hbm, vb_ref, ow_hbm, mg_ref,
    gate_hbm, up_hbm, down_hbm, cos_ref, sin_ref, len_ref,
    out_ref, infl_ref, score_ref,
    hid, hidq, normed, qw, kvw, ow, qbuf, kv, gate, ud, mbuf, lbuf, accbuf, attn,
    stage, rs1, resid, rs2, mlp_in, act, innp, sums, tot1, tot2, gbuf,
    lsem, a_send, a_recv, b_send, b_recv, x_send, x_recv, t_send, t_recv,
):
    s = lax.axis_index("seq")
    m = lax.axis_index("mp")
    y = s // (2 * NZ)
    z = lax.rem(s // 2, NZ)
    c = lax.rem(s, 2)
    kvi = m // 2

    def wrap(v, n):
        return lax.rem(v + 2 * n, n)

    def dev(yy, zz, cc):
        return (wrap(yy, NY) * NZ + wrap(zz, NZ)) * 2 + cc

    zp, zm = dev(y, z + 1, c), dev(y, z - 1, c)
    yp, ym = dev(y + 1, z, c), dev(y - 1, z, c)
    partner = dev(y, z, 1 - c)

    def rc(src, dst, ssem, rsem, sdev):
        return pltpu.make_async_remote_copy(
            src_ref=src, dst_ref=dst, send_sem=ssem, recv_sem=rsem,
            device_id={"seq": sdev, "mp": m}, device_id_type=MESH,
        )

    def rcx(src, dst, ssem, rsem, mdev):
        return pltpu.make_async_remote_copy(
            src_ref=src, dst_ref=dst, send_sem=ssem, recv_sem=rsem,
            device_id={"seq": s, "mp": mdev}, device_id_type=MESH,
        )

    own_gate = gate.at[y, z, c]
    own_up = ud.at[y, z, c, 0]
    own_down = ud.at[y, z, c, 1]
    loads = [
        pltpu.make_async_copy(up_hbm, own_up, lsem.at[0]),
        pltpu.make_async_copy(down_hbm, own_down, lsem.at[1]),
        pltpu.make_async_copy(gate_hbm, own_gate, lsem.at[2]),
        pltpu.make_async_copy(hid_hbm, hid, lsem.at[3]),
        pltpu.make_async_copy(
            kw_hbm.at[:, pl.ds(pl.multiple_of(kvi * HEAD, HEAD), HEAD)],
            kvw.at[:, pl.ds(0, HEAD)], lsem.at[4]),
        pltpu.make_async_copy(
            vw_hbm.at[:, pl.ds(pl.multiple_of(kvi * HEAD, HEAD), HEAD)],
            kvw.at[:, pl.ds(HEAD, HEAD)], lsem.at[5]),
        pltpu.make_async_copy(qw_hbm, qw, lsem.at[6]),
        pltpu.make_async_copy(
            hid_hbm.at[:, pl.ds(pl.multiple_of(m * QUART, QUART), QUART)], hidq, lsem.at[7]),
    ] + [
        pltpu.make_async_copy(ow_hbm.at[:, pl.ds(q * QUART, QUART)], ow.at[q], lsem.at[8 + q])
        for q in range(MP)
    ]
    for copy in loads:
        copy.start()

    bar = pltpu.get_barrier_semaphore()

    def greet_plane(i, _):
        pl.semaphore_signal(
            bar, inc=1, device_id={"seq": y * (2 * NZ) + lax.rem(s + i, 2 * NZ), "mp": m},
            device_id_type=MESH)
        return 0

    lax.fori_loop(1, 2 * NZ, greet_plane, 0)
    for i in range(1, NY):
        pl.semaphore_signal(bar, inc=1, device_id={"seq": dev(y + i, z, c), "mp": m}, device_id_type=MESH)
    for i in range(1, MP):
        pl.semaphore_signal(bar, inc=1, device_id={"seq": s, "mp": wrap(m + i, MP)}, device_id_type=MESH)
    pl.semaphore_wait(bar, 2 * NZ - 1 + NY - 1 + MP - 1)

    ZS, YPS, YMS, HPS, HMS, DS = range(6)

    def block(st, yy, zz):
        buf = kv if st == 0 else gate
        return buf.at[wrap(yy, NY), wrap(zz, NZ), c]

    def half(st, ref, i):
        return ref.at[i] if st == 0 else ref.at[pl.ds(i * (WR // 2), WR // 2)]

    def z_copy(st, k_to, zoff_here, right):
        ref = block(st, y, z + zoff_here)
        return rc(ref, ref, a_send.at[st, ZS, k_to], a_recv.at[st, ZS, k_to], zp if right else zm)

    def yp_copy(st, k, zz):
        ref = block(st, y, zz)
        return rc(ref, ref, a_send.at[st, YPS, k], a_recv.at[st, YPS, k], yp)

    def ym_copy(st, k, zz):
        ref = block(st, y, zz)
        return rc(ref, ref, a_send.at[st, YMS, k], a_recv.at[st, YMS, k], ym)

    def yp_recv(st, k, zz):
        ref = block(st, y - 1, zz)
        return rc(ref, ref, a_send.at[st, YPS, k], a_recv.at[st, YPS, k], yp)

    def ym_recv(st, k, zz):
        ref = block(st, y + 1, zz)
        return rc(ref, ref, a_send.at[st, YMS, k], a_recv.at[st, YMS, k], ym)

    def hp_copy(st, k, zz):
        ref = half(st, block(st, y - 1, zz), 0)
        return rc(ref, ref, a_send.at[st, HPS, k], a_recv.at[st, HPS, k], yp)

    def hm_copy(st, k, zz):
        ref = half(st, block(st, y + 1, zz), 1)
        return rc(ref, ref, a_send.at[st, HMS, k], a_recv.at[st, HMS, k], ym)

    def hp_recv(st, k, zz):
        ref = half(st, block(st, y + 2, zz), 0)
        return rc(ref, ref, a_send.at[st, HPS, k], a_recv.at[st, HPS, k], yp)

    def hm_recv(st, k, zz):
        ref = half(st, block(st, y + 2, zz), 1)
        return rc(ref, ref, a_send.at[st, HMS, k], a_recv.at[st, HMS, k], ym)

    def d_copy(st, k, zz):
        buf = kv if st == 0 else gate
        ref = buf.at[:, wrap(zz, NZ), c]
        return rc(ref, ref, a_send.at[st, DS, k], a_recv.at[st, DS, k], partner)

    def d_recv(st, k, zz):
        buf = kv if st == 0 else gate
        ref = buf.at[:, wrap(zz, NZ), 1 - c]
        return rc(ref, ref, a_send.at[st, DS, k], a_recv.at[st, DS, k], partner)

    def zk_of(k):
        return z + jnp.where(lax.rem(k, 2) == 1, -((k + 1) // 2), k // 2)

    def z_start(st):
        z_copy(st, 1, 0, True).start()
        z_copy(st, 2, 0, False).start()

    def z_hop(st, h, with_y):
        for k in (2 * h - 1, 2 * h):
            if k >= NZ:
                continue
            right = k % 2 == 1
            z_copy(st, k, Z_OFF[k], right).wait_recv()
            if k + 2 < NZ:
                z_copy(st, k + 2, Z_OFF[k], right).start()
            if with_y:
                yp_copy(st, k, z + Z_OFF[k]).start()
                ym_copy(st, k, z + Z_OFF[k]).start()

    BYP, BYM, BHP, BHM = range(4)
    RZ, LZ, DZ = 4, 12, 20

    def b_block(yy, w=None):
        ref = ud.at[wrap(yy, NY), z, c]
        return ref if w is None else ref.at[w]

    def b_copy(ref, i, d):
        return rc(ref, ref, b_send.at[i], b_recv.at[i], d)

    def group(zz, w):
        return ud.at[:, wrap(zz, NZ), c, w]

    def r_copy(i, w):
        return b_copy(group(z - (i - 1), w), RZ + 2 * (i - 1) + w, zp)

    def r_recv(i, w):
        return b_copy(group(z - i, w), RZ + 2 * (i - 1) + w, zp)

    def l_copy(i, w):
        return b_copy(group(z + (i - 1), w), LZ + 2 * (i - 1) + w, zm)

    def l_recv(i, w):
        return b_copy(group(z + i, w), LZ + 2 * (i - 1) + w, zm)

    def r_steps(w):
        return 4 if w == 0 else 3

    def l_steps(w):
        return 3 if w == 0 else 4

    def bd_copy(k):
        return b_copy(ud.at[:, wrap(z + Z_OFF[k], NZ), c], DZ + k, partner)

    def bd_recv(k):
        return b_copy(ud.at[:, wrap(z + Z_OFF[k], NZ), 1 - c], DZ + k, partner)

    def b_hop(h, w):
        if h <= r_steps(w):
            r_recv(h, w).wait_recv()
            if h + 1 <= r_steps(w):
                r_copy(h + 1, w).start()
        if h <= l_steps(w):
            l_recv(h, w).wait_recv()
            if h + 1 <= l_steps(w):
                l_copy(h + 1, w).start()

    loads[0].wait()
    loads[1].wait()
    b_copy(b_block(y), BYP, yp).start()
    b_copy(b_block(y), BYM, ym).start()
    loads[2].wait()
    z_start(1)

    loads[3].wait()

    def norm_rows(i, _):
        r = pl.ds(pl.multiple_of(i * 16, 16), 16)
        x = hid[r, :].astype(F32)
        sq = x * x
        part = sq[:, 0:HEAD]
        for j in range(1, D // HEAD):
            part = part + sq[:, j * HEAD:(j + 1) * HEAD]
        innp[r, :] = part
        factor = lax.rsqrt(jnp.sum(part, axis=-1, keepdims=True) * (1.0 / D) + norm_eps)
        normed[r, :] = (x * factor * ag_ref[...]).astype(BF16)
        return 0

    lax.fori_loop(0, ROWS // 16, norm_rows, 0)

    cos = cos_ref[...]
    sin = sin_ref[...]

    def rope(u):
        return u * cos + pltpu.roll(u, HEAD // 2, 1) * sin

    loads[4].wait()
    loads[5].wait()
    kv_all = jnp.dot(normed[...], kvw[...], preferred_element_type=F32)
    kb = kb_ref[pl.ds(kvi, 1), :]
    vb = vb_ref[pl.ds(kvi, 1), :]
    for sq in range(2):
        kk = kv_all[sq * TOK:(sq + 1) * TOK, 0:HEAD] + kb
        vv = kv_all[sq * TOK:(sq + 1) * TOK, HEAD:2 * HEAD] + vb
        kv[y, z, c, sq, :, 0:HEAD] = rope(kk).astype(BF16)
        kv[y, z, c, sq, :, HEAD:2 * HEAD] = vv.astype(BF16)

    loads[6].wait()
    q_all = jnp.dot(normed[...], qw[...], preferred_element_type=F32) + qb_ref[...]
    for sq in range(2):
        for h in range(OWN_HEADS):
            u = q_all[sq * TOK:(sq + 1) * TOK, h * HEAD:(h + 1) * HEAD]
            qbuf[sq, h * TOK:(h + 1) * TOK, :] = rope(u).astype(BF16)

    z_start(0)
    yp_copy(0, 0, z).start()
    ym_copy(0, 0, z).start()

    b_copy(b_block(y - 1), BYP, yp).wait_recv()
    b_copy(b_block(y - 1, 0), BHP, yp).start()
    b_copy(b_block(y + 1), BYM, ym).wait_recv()
    b_copy(b_block(y + 1, 1), BHM, ym).start()

    z_hop(1, 1, False)
    z_hop(0, 1, True)
    z_hop(1, 2, False)
    z_hop(0, 2, True)
    z_hop(1, 3, False)
    z_hop(0, 3, True)
    z_hop(1, 4, False)
    z_hop(0, 4, True)

    b_copy(b_block(y + 2, 0), BHP, yp).wait_recv()
    b_copy(b_block(y + 2, 1), BHM, ym).wait_recv()
    for w in range(2):
        r_copy(1, w).start()
        l_copy(1, w).start()
    bd_copy(0).start()

    for sq in range(2):
        mbuf[sq] = jnp.full((OWN_HEADS * TOK, HEAD), masked_score, F32)
        lbuf[sq] = jnp.zeros((OWN_HEADS * TOK, HEAD), F32)
        accbuf[sq] = jnp.zeros((OWN_HEADS * TOK, HEAD), F32)

    def attend(sq, yk, zk, diagonal):
        pair = kv[yk, zk, :, sq]
        kb_ = pair[:, :, 0:HEAD].reshape(2 * TOK, HEAD)
        vb_ = pair[:, :, HEAD:2 * HEAD].reshape(2 * TOK, HEAD)
        sc = lax.dot_general(qbuf[sq], kb_, (((1,), (1,)), ((), ())), preferred_element_type=F32)
        if diagonal:
            row = lax.rem(lax.broadcasted_iota(jnp.int32, sc.shape, 0), TOK) + c * TOK
            col = lax.broadcasted_iota(jnp.int32, sc.shape, 1)
            sc = jnp.where(col <= row, sc, masked_score)
        m_old = mbuf[sq]
        m_new = jnp.maximum(m_old, jnp.max(sc, axis=1, keepdims=True))
        p = jnp.exp2((sc - jnp.concatenate([m_new, m_new], axis=1)) * EXP2_SCALE)
        alpha = jnp.exp2((m_old - m_new) * EXP2_SCALE)
        mbuf[sq] = m_new
        lbuf[sq] = lbuf[sq] * alpha + jnp.sum(p, axis=1, keepdims=True)
        accbuf[sq] = accbuf[sq] * alpha + jnp.dot(p.astype(BF16), vb_, preferred_element_type=F32)

    def attend_round(k):
        zk = wrap(zk_of(k), NZ)

        @pl.when(k == 0)
        def _():
            for sq in range(2):
                attend(sq, y, zk, True)

        def step(yk, _):
            for sq in range(2):
                attend(sq, yk, zk, False)
            return 0

        lax.fori_loop(0, y + jnp.where(zk < z, 1, 0), step, 0)

    def kv_round(k, _):
        @pl.when(k < NZ)
        def _():
            zk = zk_of(k)
            yp_recv(0, k, zk).wait_recv()
            hp_copy(0, k, zk).start()
            ym_recv(0, k, zk).wait_recv()
            hm_copy(0, k, zk).start()

        @pl.when((k >= 1) & (k < NZ + 1))
        def _():
            zk = zk_of(k - 1)
            hp_recv(0, k - 1, zk).wait_recv()
            hm_recv(0, k - 1, zk).wait_recv()
            d_copy(0, k - 1, zk).start()

        @pl.when(k >= 2)
        def _():
            d_recv(0, k - 2, zk_of(k - 2)).wait_recv()
            attend_round(k - 2)

        return 0

    lax.fori_loop(0, NZ + 2, kv_round, 0)

    def gate_send(k, _):
        yp_copy(1, k, zk_of(k)).start()
        ym_copy(1, k, zk_of(k)).start()
        return 0

    lax.fori_loop(0, NZ, gate_send, 0)
    b_hop(1, 0)
    b_hop(1, 1)
    bd_copy(1).start()
    bd_copy(2).start()

    for sq in range(2):
        for h in range(OWN_HEADS):
            r = slice(h * TOK, (h + 1) * TOK)
            attn[sq * TOK:(sq + 1) * TOK, h * HEAD:(h + 1) * HEAD] = (
                accbuf[sq, r, :] / lbuf[sq, r, :]
            ).astype(BF16)
    for q in range(MP):
        loads[8 + q].wait()

    def x_copy(ph, j, dst_buf):
        return rcx(stage.at[ph, j], dst_buf.at[m], x_send.at[ph, j], x_recv.at[ph, j], wrap(m + j, MP))

    def x_recv_of(ph, j, dst_buf):
        src = wrap(m - j, MP)
        return rcx(dst_buf.at[src], dst_buf.at[src], x_send.at[ph, j], x_recv.at[ph, j], src)

    for j in (2, 1, 3, 0):
        q = wrap(m + j, MP)
        part = jnp.dot(attn[...], ow[q], preferred_element_type=F32).astype(BF16)
        if j == 0:
            rs1[m] = part
        else:
            stage[0, j] = part
    for j in (2, 1, 3):
        x_copy(0, j, rs1).start()

    def gate_round(k, _):
        zk = zk_of(k)
        yp_recv(1, k, zk).wait_recv()
        hp_copy(1, k, zk).start()
        ym_recv(1, k, zk).wait_recv()
        hm_copy(1, k, zk).start()
        return 0

    lax.fori_loop(0, NZ // 2, gate_round, 0)
    b_hop(2, 0)

    loads[7].wait()
    for j in (1, 3, 2):
        x_recv_of(0, j, rs1).wait_recv()
    total = hidq[...].astype(F32)
    add = rs1[0].astype(F32)
    for q in range(1, MP):
        add = add + rs1[q].astype(F32)
    resid[m] = (total + add).astype(BF16)
    b_hop(2, 1)
    bd_copy(3).start()
    bd_copy(4).start()
    lax.fori_loop(NZ // 2, NZ, gate_round, 0)

    def ag_copy(j):
        return rcx(resid.at[m], resid.at[m], x_send.at[1, j], x_recv.at[1, j], wrap(m + j, MP))

    for j in (2, 1, 3):
        ag_copy(j).start()

    def gate_last(k, _):
        zk = zk_of(k)
        hp_recv(1, k, zk).wait_recv()
        hm_recv(1, k, zk).wait_recv()
        d_copy(1, k, zk).start()
        return 0

    lax.fori_loop(0, NZ, gate_last, 0)
    b_hop(3, 0)
    b_hop(3, 1)
    bd_copy(5).start()
    bd_copy(6).start()
    for j in (1, 3, 2):
        x_recv_of(1, j, resid).wait_recv()

    def norm2_rows(i, _):
        r = pl.ds(pl.multiple_of(i * 16, 16), 16)
        xs = [resid[q, r, :].astype(F32) for q in range(MP)]
        part = None
        for x in xs:
            sq = x * x
            for j in range(QUART // HEAD):
                t = sq[:, j * HEAD:(j + 1) * HEAD]
                part = t if part is None else part + t
        factor = lax.rsqrt(jnp.sum(part, axis=-1, keepdims=True) * (1.0 / D) + norm_eps)
        for q in range(MP):
            cols = slice(q * QUART, (q + 1) * QUART)
            mlp_in[r, cols] = (xs[q] * factor * mg_ref[:, cols]).astype(BF16)
        return 0

    lax.fori_loop(0, ROWS // 16, norm2_rows, 0)

    def gate_in(k, _):
        d_recv(1, k, zk_of(k)).wait_recv()
        return 0

    lax.fori_loop(0, NZ, gate_in, 0)
    gbuf[...] = jnp.dot(mlp_in[...], gate[...].reshape(D, FFP), preferred_element_type=F32)
    b_hop(4, 0)
    b_hop(4, 1)
    bd_copy(7).start()
    for k in range(NZ):
        bd_recv(k).wait_recv()
    up_sum = jnp.dot(mlp_in[...], ud[:, :, :, 0].reshape(D, FFP), preferred_element_type=F32)
    g = gbuf[...]
    act[...] = (g / (1.0 + jnp.exp(-g)) * up_sum).astype(BF16)

    for j in (2, 1, 3, 0):
        q = wrap(m + j, MP)
        rows = ud[q, :, :, 1].reshape(QUART, FFP)
        part = lax.dot_general(
            act[...], rows, (((1,), (1,)), ((), ())), preferred_element_type=F32
        ).astype(BF16)
        if j == 0:
            rs2[m] = part
        else:
            stage[1, j] = part
            rcx(stage.at[1, j], rs2.at[m], x_send.at[2, j], x_recv.at[2, j], q).start()

    def stream_done(k, _):
        for st in range(2):
            yp_copy(st, k, zk_of(k)).wait_send()
            ym_copy(st, k, zk_of(k)).wait_send()
            hp_copy(st, k, zk_of(k)).wait_send()
            hm_copy(st, k, zk_of(k)).wait_send()
            d_copy(st, k, zk_of(k)).wait_send()
        return 0

    lax.fori_loop(0, NZ, stream_done, 0)
    for st in range(2):
        for k in range(1, NZ):
            z_copy(st, k, 0, True).wait_send()
    b_copy(b_block(y), BYP, yp).wait_send()
    b_copy(b_block(y), BYM, ym).wait_send()
    b_copy(b_block(y, 0), BHP, yp).wait_send()
    b_copy(b_block(y, 1), BHM, ym).wait_send()
    for w in range(2):
        for i in range(1, r_steps(w) + 1):
            r_copy(i, w).wait_send()
        for i in range(1, l_steps(w) + 1):
            l_copy(i, w).wait_send()
    for k in range(NZ):
        bd_copy(k).wait_send()
    for j in (1, 2, 3):
        x_copy(0, j, rs1).wait_send()
        ag_copy(j).wait_send()

    def lane_sums(part):
        return jnp.sum(part.T, axis=0, keepdims=True)

    in_norm = lane_sums(innp[...])

    def x2_recv(j):
        src = wrap(m - j, MP)
        return rcx(rs2.at[src], rs2.at[src], x_send.at[2, j], x_recv.at[2, j], src)

    for j in (1, 3, 2):
        x2_recv(j).wait_recv()

    add = rs2[0].astype(F32)
    for q in range(1, MP):
        add = add + rs2[q].astype(F32)
    layer = (resid[m].astype(F32) + add).astype(BF16)
    out_ref[...] = layer
    wide = layer.astype(F32)
    cp = hidq[...].astype(F32) * wide
    op = wide * wide
    cpart, opart = cp[:, 0:HEAD], op[:, 0:HEAD]
    for j in range(1, QUART // HEAD):
        cols = slice(j * HEAD, (j + 1) * HEAD)
        cpart = cpart + cp[:, cols]
        opart = opart + op[:, cols]
    rowi = lax.broadcasted_iota(jnp.int32, (8, ROWS), 0)
    sums[m] = jnp.where(rowi == 0, lane_sums(cpart), lane_sums(opart))

    def s_copy(j):
        return rcx(sums.at[m], sums.at[m], t_send.at[0, j], t_recv.at[0, j], wrap(m + j, MP))

    def s_recv(j):
        src = wrap(m - j, MP)
        return rcx(sums.at[src], sums.at[src], t_send.at[0, j], t_recv.at[0, j], src)

    for j in (2, 1, 3):
        s_copy(j).start()
    for j in (1, 3, 2):
        s_recv(j).wait_recv()
    both = sums[0] + sums[1] + sums[2] + sums[3]
    cross, out_norm = both[0:1, :], both[1:2, :]
    cosine = cross / jnp.sqrt((in_norm + norm_eps) * (out_norm + norm_eps))
    lane = lax.broadcasted_iota(jnp.int32, (1, ROWS), 1)
    pos = s * TOK + lax.rem(lane, TOK)
    limit = jnp.where(lane < TOK, len_ref[0], len_ref[1])
    influence = jnp.where(pos < limit, 1.0 - cosine, 0.0)
    infl_ref[0:1, :] = influence[:, 0:TOK]
    infl_ref[1:2, :] = influence[:, TOK:2 * TOK]
    t0 = jnp.sum(influence[:, 0:TOK], axis=1, keepdims=True)
    t1 = jnp.sum(influence[:, TOK:2 * TOK], axis=1, keepdims=True)
    row = lax.broadcasted_iota(jnp.int32, (8, HEAD), 0)
    i1 = lax.rem(s, 2 * NZ)
    tot1[i1] = jnp.where(row == 0, t0, t1)

    def t1_copy(i):
        return rc(tot1.at[i1], tot1.at[i1], t_send.at[1, i], t_recv.at[1, i],
                  y * (2 * NZ) + lax.rem(i1 + i, 2 * NZ))

    def t1_recv(i):
        src = lax.rem(i1 + 2 * NZ - i, 2 * NZ)
        return rc(tot1.at[src], tot1.at[src], t_send.at[1, i], t_recv.at[1, i], y * (2 * NZ) + src)

    def t1_start(i, _):
        t1_copy(i).start()
        return 0

    def t1_wait(i, _):
        t1_recv(i).wait_recv()
        t1_copy(i).wait_send()
        return 0

    lax.fori_loop(1, 2 * NZ, t1_start, 0)
    lax.fori_loop(1, 2 * NZ, t1_wait, 0)
    acc = tot1[0]
    for i in range(1, 2 * NZ):
        acc = acc + tot1[i]
    tot2[y] = acc

    def t2_copy(i):
        return rc(tot2.at[y], tot2.at[y], t_send.at[2, i], t_recv.at[2, i], dev(y + i, z, c))

    def t2_recv(i):
        src = wrap(y - i, NY)
        return rc(tot2.at[src], tot2.at[src], t_send.at[2, i], t_recv.at[2, i], dev(y - i, z, c))

    for i in range(1, NY):
        t2_copy(i).start()
    for i in range(1, NY):
        t2_recv(i).wait_recv()
        t2_copy(i).wait_send()
    acc = tot2[0] + tot2[1] + tot2[2] + tot2[3]
    tokens = jnp.where(row == 0, len_ref[0], len_ref[1]).astype(F32)
    score_ref[...] = acc / tokens

    for j in (1, 2, 3):
        rcx(stage.at[1, j], rs2.at[m], x_send.at[2, j], x_recv.at[2, j], wrap(m + j, MP)).wait_send()
        s_copy(j).wait_send()


def local(
    hidden_in, attn_gain, q_weight, q_bias, k_weight, k_bias, v_weight, v_bias, o_weight,
    mlp_gain, gate_weight, up_weight, down_weight, lengths,
):
    seqs_n, tok_n, width = hidden_in.shape
    seq_rank = lax.axis_index("seq")
    positions = seq_rank * tok_n + jnp.arange(tok_n, dtype=jnp.int32)
    half_width = HEAD // 2
    inv_freq = rope_base ** (-(jnp.arange(half_width, dtype=jnp.float32) * 2.0) / HEAD)
    angles = positions.astype(jnp.float32)[:, None] * inv_freq[None, :]
    cos = jnp.cos(angles)
    sin = jnp.sin(angles)
    cos_t = jnp.concatenate([cos, cos], axis=-1)
    sin_t = jnp.concatenate([-sin, sin], axis=-1)

    hbm = pl.BlockSpec(memory_space=pltpu.HBM)
    vmem = pl.BlockSpec(memory_space=pltpu.VMEM)
    smem = pl.BlockSpec(memory_space=pltpu.SMEM)
    dma = pltpu.SemaphoreType.DMA
    layer_part, influence, score = pl.pallas_call(
        layer_kernel,
        out_shape=(
            jax.ShapeDtypeStruct((ROWS, QUART), BF16),
            jax.ShapeDtypeStruct((2, TOK), F32),
            jax.ShapeDtypeStruct((8, HEAD), F32),
        ),
        in_specs=[
            hbm, vmem, hbm, vmem, hbm, vmem, hbm, vmem, hbm, vmem,
            hbm, hbm, hbm, vmem, vmem, smem,
        ],
        out_specs=(vmem, vmem, vmem),
        scratch_shapes=[
            pltpu.VMEM((ROWS, D), BF16),
            pltpu.VMEM((ROWS, QUART), BF16),
            pltpu.VMEM((ROWS, D), BF16),
            pltpu.VMEM((D, QCOLS), BF16),
            pltpu.VMEM((D, 2 * HEAD), BF16),
            pltpu.VMEM((MP, QCOLS, QUART), BF16),
            pltpu.VMEM((2, OWN_HEADS * TOK, HEAD), BF16),
            pltpu.VMEM((NY, NZ, 2, 2, TOK, 2 * HEAD), BF16),
            pltpu.VMEM((NY, NZ, 2, WR, FFP), BF16),
            pltpu.VMEM((NY, NZ, 2, 2, WR, FFP), BF16),
            pltpu.VMEM((2, OWN_HEADS * TOK, HEAD), F32),
            pltpu.VMEM((2, OWN_HEADS * TOK, HEAD), F32),
            pltpu.VMEM((2, OWN_HEADS * TOK, HEAD), F32),
            pltpu.VMEM((ROWS, QCOLS), BF16),
            pltpu.VMEM((2, MP, ROWS, QUART), BF16),
            pltpu.VMEM((MP, ROWS, QUART), BF16),
            pltpu.VMEM((MP, ROWS, QUART), BF16),
            pltpu.VMEM((MP, ROWS, QUART), BF16),
            pltpu.VMEM((ROWS, D), BF16),
            pltpu.VMEM((ROWS, FFP), BF16),
            pltpu.VMEM((ROWS, HEAD), F32),
            pltpu.VMEM((MP, 8, ROWS), F32),
            pltpu.VMEM((2 * NZ, 8, HEAD), F32),
            pltpu.VMEM((NY, 8, HEAD), F32),
            pltpu.VMEM((ROWS, FFP), F32),
            dma((12,)),
            dma((2, 6, NZ)),
            dma((2, 6, NZ)),
            dma((28,)),
            dma((28,)),
            dma((3, MP)),
            dma((3, MP)),
            dma((3, 2 * NZ)),
            dma((3, 2 * NZ)),
        ],
        compiler_params=pltpu.CompilerParams(
            collective_id=0, has_side_effects=True, vmem_limit_bytes=62 * 1024 * 1024
        ),
        name="layer",
    )(
        hidden_in.reshape(ROWS, width), attn_gain.reshape(1, width), q_weight,
        q_bias.reshape(1, QCOLS), k_weight, k_bias.reshape(KV_HEADS, HEAD), v_weight,
        v_bias.reshape(KV_HEADS, HEAD), o_weight, mlp_gain.reshape(1, width), gate_weight,
        up_weight, down_weight, cos_t, sin_t, lengths,
    )
    return layer_part.reshape(seqs_n, tok_n, QUART), influence, score[0:2, 0]


def solution(mesh):
    placed = (
        P(None, "seq", None), P(), P(None, "mp"), P("mp"), P(), P(), P(), P(),
        P("mp", None), P(), P("seq", "mp"), P("seq", "mp"), P("seq", "mp"), P(),
    )
    return jax.shard_map(
        local, mesh=mesh, in_specs=placed,
        out_specs=(P(None, "seq", "mp"), P(None, "seq"), P()), check_vma=False,
    )
```

```python
import jax
import jax.numpy as jnp
from jax import lax
from jax.experimental import pallas as pl
from jax.experimental.pallas import tpu as pltpu
from jax.sharding import PartitionSpec as P

HEADS = 16
KV_HEADS = 2
HEAD = 128
D = 2048
NY, NZ = 4, 8
MP = 4
TOK = 128
ROWS = 2 * TOK
OWN_HEADS = HEADS // MP
QCOLS = OWN_HEADS * HEAD
QUART = D // MP
FFP = 1408
WR = 32
NS = NY * NZ * 2

rope_base = 1000000.0
norm_eps = 1e-06
masked_score = -1e30
EXP2_SCALE = HEAD ** (-0.5) * 1.4426950408889634

MESH = pl.DeviceIdType.MESH
F32, BF16 = jnp.float32, jnp.bfloat16

Z_OFF = (0, -1, 1, -2, 2, -3, 3, -4)


def layer_kernel(
    hid_hbm, ag_ref, qw_hbm, qb_ref, kw_hbm, kb_ref, vw_hbm, vb_ref, ow_hbm, mg_ref,
    gate_hbm, up_hbm, down_hbm, cos_ref, sin_ref, len_ref,
    out_hbm, infl_ref, score_ref,
    hid, hidq, normed, qw, kvw, ow, qbuf, kv, gate, up, down, mbuf, lbuf, accbuf, attn,
    stage1, rs1, resid, stage2, rs2, mlp_in, act, innp, sums, tot, gbuf, layer_v,
    lsem, osem, a_send, a_recv, b_send, b_recv, x_send, x_recv, r_send, r_recv,
    s_send, s_recv, t_send, t_recv,
):
    s = lax.axis_index("seq")
    m = lax.axis_index("mp")
    y = s // (2 * NZ)
    z = lax.rem(s // 2, NZ)
    c = lax.rem(s, 2)
    kvi = m // 2

    def wrap(v, n):
        return lax.rem(v + 2 * n, n)

    def dev(yy, zz, cc):
        return (wrap(yy, NY) * NZ + wrap(zz, NZ)) * 2 + cc

    zp, zm = dev(y, z + 1, c), dev(y, z - 1, c)
    yp, ym = dev(y + 1, z, c), dev(y - 1, z, c)
    partner = dev(y, z, 1 - c)

    def rc(src, dst, ssem, rsem, sdev):
        return pltpu.make_async_remote_copy(
            src_ref=src, dst_ref=dst, send_sem=ssem, recv_sem=rsem,
            device_id={"seq": sdev, "mp": m}, device_id_type=MESH,
        )

    def rcx(src, dst, ssem, rsem, mdev):
        return pltpu.make_async_remote_copy(
            src_ref=src, dst_ref=dst, send_sem=ssem, recv_sem=rsem,
            device_id={"seq": s, "mp": mdev}, device_id_type=MESH,
        )

    kv_cols = pl.ds(pl.multiple_of(kvi * HEAD, HEAD), HEAD)
    loads = [
        pltpu.make_async_copy(up_hbm, up.at[y, z, c], lsem.at[0]),
        pltpu.make_async_copy(gate_hbm, gate.at[y, z, c], lsem.at[1]),
        pltpu.make_async_copy(down_hbm, down.at[y, z, c], lsem.at[2]),
        pltpu.make_async_copy(hid_hbm, hid, lsem.at[3]),
        pltpu.make_async_copy(kw_hbm.at[:, kv_cols], kvw.at[:, pl.ds(0, HEAD)], lsem.at[4]),
        pltpu.make_async_copy(vw_hbm.at[:, kv_cols], kvw.at[:, pl.ds(HEAD, HEAD)], lsem.at[5]),
        pltpu.make_async_copy(qw_hbm, qw, lsem.at[6]),
        pltpu.make_async_copy(
            hid_hbm.at[:, pl.ds(pl.multiple_of(m * QUART, QUART), QUART)], hidq, lsem.at[7]),
    ] + [
        pltpu.make_async_copy(ow_hbm.at[:, pl.ds(q * QUART, QUART)], ow.at[q], lsem.at[8 + q])
        for q in range(MP)
    ]
    for copy in loads:
        copy.start()

    bar = pltpu.get_barrier_semaphore()
    for peer in (zp, zm, yp, ym, partner):
        pl.semaphore_signal(bar, inc=1, device_id={"seq": peer, "mp": m}, device_id_type=MESH)
    for i in range(1, MP):
        pl.semaphore_signal(bar, inc=1, device_id={"seq": s, "mp": wrap(m + i, MP)}, device_id_type=MESH)
    pl.semaphore_wait(bar, 5 + MP - 1)

    ZS, YPS, YMS, HPS, HMS, DS = range(6)
    A_HALF = (TOK // 2, WR // 2, WR // 2)
    ALL = slice(None)

    def a_ref(st, yy, zz, cc):
        if st == 0:
            return kv.at[0, yy, zz, cc]
        return (gate, down)[st - 1].at[yy, zz, cc]

    def block(st, yy, zz):
        return a_ref(st, wrap(yy, NY), wrap(zz, NZ), c)

    def half(st, ref, i):
        return ref.at[pl.ds(i * A_HALF[st], A_HALF[st])]

    def a_copy(ref, st, kind, k, d):
        return rc(ref, ref, a_send.at[st, kind, k], a_recv.at[st, kind, k], d)

    def zk_of(k):
        if isinstance(k, int):
            return z + Z_OFF[k]
        return z + jnp.where(lax.rem(k, 2) == 1, -((k + 1) // 2), k // 2)

    def z_copy(st, k_to, zz, right):
        return a_copy(block(st, y, zz), st, ZS, k_to, zp if right else zm)

    def y_send(st, k):
        ref = block(st, y, zk_of(k))
        a_copy(ref, st, YPS, k, yp).start()
        a_copy(ref, st, YMS, k, ym).start()

    def y_pass(st, k):
        zz = zk_of(k)
        ref = block(st, y - 1, zz)
        a_copy(ref, st, YPS, k, yp).wait_recv()
        a_copy(half(st, ref, 0), st, HPS, k, yp).start()
        ref = block(st, y + 1, zz)
        a_copy(ref, st, YMS, k, ym).wait_recv()
        a_copy(half(st, ref, 1), st, HMS, k, ym).start()

    def y_last(st, k):
        zz = zk_of(k)
        ref = block(st, y + 2, zz)
        a_copy(half(st, ref, 0), st, HPS, k, yp).wait_recv()
        a_copy(half(st, ref, 1), st, HMS, k, ym).wait_recv()
        a_copy(a_ref(st, ALL, wrap(zz, NZ), c), st, DS, k, partner).start()

    def a_wait(st, k):
        a_copy(a_ref(st, ALL, wrap(zk_of(k), NZ), 1 - c), st, DS, k, partner).wait_recv()

    def z_start(st):
        z_copy(st, 1, z, True).start()
        z_copy(st, 2, z, False).start()

    def z_hop(st, h, with_y=False):
        far_right = st != 1
        for k in (2 * h - 1, 2 * h):
            if k >= NZ:
                continue
            right = far_right if k == 7 else k % 2 == 1
            z_copy(st, k, zk_of(k), right).wait_recv()
            if k + 2 < NZ - 1:
                z_copy(st, k + 2, zk_of(k), right).start()
            if k == (5 if far_right else 6):
                z_copy(st, 7, zk_of(k), far_right).start()
            if with_y:
                y_send(st, k)

    BYP, BYM, BHP, BHM = range(4)
    RZ, LZ, DZ = 4, 12, 20
    B_HALF = (TOK // 2, WR // 2)

    def b_ref(st, yy, zz, cc):
        return kv.at[1, yy, zz, cc] if st == 0 else up.at[yy, zz, cc]

    def b_copy(st, ref, i, d):
        return rc(ref, ref, b_send.at[st, i], b_recv.at[st, i], d)

    def b_block(st, yy, w=None):
        ref = b_ref(st, wrap(yy, NY), z, c)
        return ref if w is None else ref.at[pl.ds(w * B_HALF[st], B_HALF[st])]

    def group(st, zz, w):
        rows = pl.ds(w * B_HALF[st], B_HALF[st])
        if st == 0:
            return kv.at[1, :, wrap(zz, NZ), c, rows]
        return up.at[:, wrap(zz, NZ), c, rows]

    def r_copy(st, i, w):
        return b_copy(st, group(st, z - (i - 1), w), RZ + 2 * (i - 1) + w, zp)

    def r_from(st, i, w):
        return b_copy(st, group(st, z - i, w), RZ + 2 * (i - 1) + w, zp)

    def l_copy(st, i, w):
        return b_copy(st, group(st, z + (i - 1), w), LZ + 2 * (i - 1) + w, zm)

    def l_from(st, i, w):
        return b_copy(st, group(st, z + i, w), LZ + 2 * (i - 1) + w, zm)

    def r_steps(w):
        return 4 if w == 0 else 3

    def l_steps(w):
        return 3 if w == 0 else 4

    def by_start(st):
        b_copy(st, b_block(st, y), BYP, yp).start()
        b_copy(st, b_block(st, y), BYM, ym).start()

    def by_pass(st):
        b_copy(st, b_block(st, y - 1), BYP, yp).wait_recv()
        b_copy(st, b_block(st, y - 1, 0), BHP, yp).start()
        b_copy(st, b_block(st, y + 1), BYM, ym).wait_recv()
        b_copy(st, b_block(st, y + 1, 1), BHM, ym).start()

    def by_last(st):
        b_copy(st, b_block(st, y + 2, 0), BHP, yp).wait_recv()
        b_copy(st, b_block(st, y + 2, 1), BHM, ym).wait_recv()

    def bz_start(st):
        for w in range(2):
            r_copy(st, 1, w).start()
            l_copy(st, 1, w).start()

    def bd_start(st, k):
        b_copy(st, b_ref(st, ALL, wrap(zk_of(k), NZ), c), DZ + k, partner).start()

    def b_wait(st, k):
        b_copy(st, b_ref(st, ALL, wrap(zk_of(k), NZ), 1 - c), DZ + k, partner).wait_recv()

    def b_hop(st, h, w):
        if h <= r_steps(w):
            r_from(st, h, w).wait_recv()
            if h + 1 <= r_steps(w):
                r_copy(st, h + 1, w).start()
        if h <= l_steps(w):
            l_from(st, h, w).wait_recv()
            if h + 1 <= l_steps(w):
                l_copy(st, h + 1, w).start()
        if w == 1:
            for k in (2 * h - 1, 2 * h):
                if k < NZ:
                    bd_start(st, k)

    loads[0].wait()
    by_start(1)
    loads[1].wait()
    z_start(1)

    loads[3].wait()

    def norm_rows(i, _):
        r = pl.ds(pl.multiple_of(i * 16, 16), 16)
        x = hid[r, :].astype(F32)
        sq = x * x
        part = sq[:, 0:HEAD]
        for j in range(1, D // HEAD):
            part = part + sq[:, j * HEAD:(j + 1) * HEAD]
        innp[r, :] = part
        factor = lax.rsqrt(jnp.sum(part, axis=-1, keepdims=True) * (1.0 / D) + norm_eps)
        normed[r, :] = (x * factor * ag_ref[...]).astype(BF16)
        return 0

    lax.fori_loop(0, ROWS // 16, norm_rows, 0, unroll=4)

    cos = cos_ref[...]
    sin = sin_ref[...]

    def rope(u):
        return u * cos + pltpu.roll(u, HEAD // 2, 1) * sin

    loads[4].wait()
    loads[5].wait()
    kv_all = jnp.dot(normed[...], kvw[...], preferred_element_type=F32)
    kb = kb_ref[pl.ds(kvi, 1), :]
    vb = vb_ref[pl.ds(kvi, 1), :]
    for sq in range(2):
        kk = kv_all[sq * TOK:(sq + 1) * TOK, 0:HEAD] + kb
        vv = kv_all[sq * TOK:(sq + 1) * TOK, HEAD:2 * HEAD] + vb
        kv[sq, y, z, c, :, 0:HEAD] = rope(kk).astype(BF16)
        kv[sq, y, z, c, :, HEAD:2 * HEAD] = vv.astype(BF16)

    loads[6].wait()
    q_all = jnp.dot(normed[...], qw[...], preferred_element_type=F32) + qb_ref[...]
    for sq in range(2):
        for h in range(OWN_HEADS):
            u = q_all[sq * TOK:(sq + 1) * TOK, h * HEAD:(h + 1) * HEAD]
            qbuf[sq, h * TOK:(h + 1) * TOK, :] = rope(u).astype(BF16)

    for sq in range(2):
        mbuf[sq] = jnp.full((OWN_HEADS * TOK, HEAD), masked_score, F32)
        lbuf[sq] = jnp.zeros((OWN_HEADS * TOK, HEAD), F32)
        accbuf[sq] = jnp.zeros((OWN_HEADS * TOK, HEAD), F32)

    def attend(sq, yks, zk, diagonal):
        pairs = [kv[sq, yk, zk] for yk in yks]
        kb_ = jnp.concatenate([p[:, :, 0:HEAD].reshape(2 * TOK, HEAD) for p in pairs], axis=0)
        vb_ = jnp.concatenate([p[:, :, HEAD:2 * HEAD].reshape(2 * TOK, HEAD) for p in pairs], axis=0)
        sc = lax.dot_general(qbuf[sq], kb_, (((1,), (1,)), ((), ())), preferred_element_type=F32)
        if diagonal:
            row = lax.rem(lax.broadcasted_iota(jnp.int32, sc.shape, 0), TOK) + c * TOK
            col = lax.broadcasted_iota(jnp.int32, sc.shape, 1)
            sc = jnp.where(col <= row, sc, masked_score)
        m_old = mbuf[sq]
        m_new = jnp.maximum(m_old, jnp.max(sc, axis=1, keepdims=True))
        p = jnp.exp2((sc - jnp.concatenate([m_new] * (2 * len(yks)), axis=1)) * EXP2_SCALE)
        alpha = jnp.exp2((m_old - m_new) * EXP2_SCALE)
        mbuf[sq] = m_new
        lbuf[sq] = lbuf[sq] * alpha + jnp.sum(p, axis=1, keepdims=True)
        accbuf[sq] = accbuf[sq] * alpha + jnp.dot(p.astype(BF16), vb_, preferred_element_type=F32)

    def attend_round(sq, k):
        zk = wrap(zk_of(k), NZ)

        @pl.when(k == 0)
        def _():
            attend(sq, (y,), zk, True)

        n = y + jnp.where(zk < z, 1, 0)

        def step(i, _):
            attend(sq, (2 * i, 2 * i + 1), zk, False)
            return 0

        lax.fori_loop(0, n // 2, step, 0)

        @pl.when(lax.rem(n, 2) == 1)
        def _():
            attend(sq, (n - 1,), zk, False)

    def seq_rows(sq):
        return pl.ds(sq * TOK, TOK)

    def rs1_send(sq, j):
        return rcx(stage1.at[sq, j], rs1.at[m, seq_rows(sq)], x_send.at[0, sq, j],
                   x_recv.at[0, sq, j], wrap(m + j, MP))

    def rs1_recv(sq, j):
        ref = rs1.at[wrap(m - j, MP), seq_rows(sq)]
        return rcx(ref, ref, x_send.at[0, sq, j], x_recv.at[0, sq, j], wrap(m - j, MP))

    def o_project(sq):
        if sq == 0:
            for q in range(MP):
                loads[8 + q].wait()
        for h in range(OWN_HEADS):
            r = slice(h * TOK, (h + 1) * TOK)
            attn[sq * TOK:(sq + 1) * TOK, h * HEAD:(h + 1) * HEAD] = (
                accbuf[sq, r, :] / lbuf[sq, r, :]
            ).astype(BF16)
        here = attn[sq * TOK:(sq + 1) * TOK, :]
        for j in (2, 1, 3, 0):
            part = jnp.dot(here, ow[wrap(m + j, MP)], preferred_element_type=F32).astype(BF16)
            if j == 0:
                rs1[m, seq_rows(sq), :] = part
            else:
                stage1[sq, j] = part
        for j in (2, 1, 3):
            rs1_send(sq, j).start()

    def ag_send(sq, j):
        ref = resid.at[m, seq_rows(sq)]
        return rcx(ref, ref, x_send.at[1, sq, j], x_recv.at[1, sq, j], wrap(m + j, MP))

    def ag_recv(sq, j):
        ref = resid.at[wrap(m - j, MP), seq_rows(sq)]
        return rcx(ref, ref, x_send.at[1, sq, j], x_recv.at[1, sq, j], wrap(m - j, MP))

    def residual(sq):
        if sq == 0:
            loads[7].wait()
        for j in (1, 3, 2):
            rs1_recv(sq, j).wait_recv()
        r = seq_rows(sq)
        add = rs1[0, r, :].astype(F32)
        for q in range(1, MP):
            add = add + rs1[q, r, :].astype(F32)
        resid[m, r, :] = (hidq[r, :].astype(F32) + add).astype(BF16)
        for j in (2, 1, 3):
            ag_send(sq, j).start()

    def second_norm(sq):
        for j in (1, 3, 2):
            ag_recv(sq, j).wait_recv()

        def norm2_rows(i, _):
            r = pl.ds(pl.multiple_of(sq * TOK + i * 16, 16), 16)
            xs = [resid[q, r, :].astype(F32) for q in range(MP)]
            part = None
            for x in xs:
                sqr = x * x
                for j in range(QUART // HEAD):
                    t = sqr[:, j * HEAD:(j + 1) * HEAD]
                    part = t if part is None else part + t
            factor = lax.rsqrt(jnp.sum(part, axis=-1, keepdims=True) * (1.0 / D) + norm_eps)
            for q in range(MP):
                cols = slice(q * QUART, (q + 1) * QUART)
                mlp_in[r, cols] = (xs[q] * factor * mg_ref[:, cols]).astype(BF16)
            return 0

        lax.fori_loop(0, TOK // 16, norm2_rows, 0, unroll=4)

    def gate_dot():
        for k in range(NZ):
            a_wait(1, k)
        gbuf[...] = jnp.dot(mlp_in[...], gate[...].reshape(D, FFP), preferred_element_type=F32)

    def up_dot():
        for k in range(NZ):
            b_wait(1, k)
        up_sum = jnp.dot(mlp_in[...], up[...].reshape(D, FFP), preferred_element_type=F32)
        g = gbuf[...]
        act[...] = (g / (1.0 + jnp.exp(-g)) * up_sum).astype(BF16)

    odd = lax.rem(z, 2)

    def z_pair(i):
        turn = (0, 2 * odd - 1, 1 - 2 * odd, 2)[i]
        return wrap(z // 2 + turn, NZ // 2)

    def rs2_send(i, j):
        q = wrap(m + j, MP)
        return rcx(stage2.at[i, q], rs2.at[i, m], r_send.at[i, j], r_recv.at[i, j], q)

    def rs2_recv(i, j):
        ref = rs2.at[i, wrap(m - j, MP)]
        return rcx(ref, ref, r_send.at[i, j], r_recv.at[i, j], wrap(m - j, MP))

    def down_stage(i):
        for k in ((0, 1, 2), (3, 4), (5, 6), (7,))[i]:
            a_wait(2, k)
        p = z_pair(i)
        for q0 in (0, 2):
            rows = down[q0:q0 + 2, pl.ds(2 * p, 2)].reshape(2 * HEAD, FFP)
            part = lax.dot_general(
                act[...], rows, (((1,), (1,)), ((), ())), preferred_element_type=F32
            ).astype(BF16)
            stage2[i, q0] = part[:, 0:HEAD]
            stage2[i, q0 + 1] = part[:, HEAD:2 * HEAD]
        for j in (2, 1, 3):
            rs2_send(i, j).start()

    def layer_stage(i, so_far):
        for j in (1, 3, 2):
            rs2_recv(i, j).wait_recv()
        cols = pl.ds(pl.multiple_of(z_pair(i) * HEAD, HEAD), HEAD)
        add = stage2[i, m].astype(F32)
        for j in range(1, MP):
            add = add + rs2[i, wrap(m - j, MP)].astype(F32)
        layer = (resid[m, :, cols].astype(F32) + add).astype(BF16)
        layer_v[:, cols] = layer
        wide = layer.astype(F32)
        cp, op = hidq[:, cols].astype(F32) * wide, wide * wide
        return (cp, op) if so_far is None else (so_far[0] + cp, so_far[1] + op)

    plan = []

    def at(time, act_, *args):
        plan.append((time, len(plan), act_, args))

    def kv_start():
        z_start(0)
        y_send(0, 0)
        by_start(0)
        loads[2].wait()
        z_start(2)

    at(3.2, kv_start)
    at(3.5, by_pass, 1)
    at(4.0, z_hop, 1, 1)
    at(6.5, z_hop, 0, 1, True)
    at(7.0, by_pass, 0)
    at(8.0, y_pass, 0, 0)
    at(9.5, z_hop, 0, 2, True)
    at(9.7, by_last, 0)
    at(9.71, bz_start, 0)
    at(9.72, bd_start, 0, 0)
    at(10.0, z_hop, 2, 1)
    at(10.1, z_hop, 1, 2)
    at(10.2, y_last, 0, 0)
    at(11.0, y_pass, 0, 1)
    at(11.1, y_pass, 0, 2)
    at(13.0, z_hop, 0, 3, True)
    at(13.5, y_last, 0, 1)
    at(13.6, y_last, 0, 2)
    at(14.0, y_pass, 0, 3)
    at(14.1, y_pass, 0, 4)
    at(16.0, b_hop, 0, 1, 0)
    at(16.5, z_hop, 0, 4, True)
    at(17.0, y_last, 0, 3)
    at(17.1, y_last, 0, 4)
    at(17.2, y_pass, 0, 5)
    at(17.3, y_pass, 0, 6)
    at(18.5, b_hop, 0, 1, 1)
    at(19.5, by_last, 1)
    at(19.6, bd_start, 1, 0)
    at(20.0, z_hop, 1, 3)
    at(20.1, z_hop, 2, 2)
    at(20.5, y_last, 0, 5)
    at(20.6, y_last, 0, 6)
    at(20.7, y_pass, 0, 7)
    at(21.5, b_hop, 0, 2, 0)
    for k in range(5):
        at(21.6 + k / 100, y_send, 1, k)
    at(22.0, y_last, 0, 7)
    at(24.0, b_hop, 0, 2, 1)
    at(26.6, o_project, 0)
    at(27.0, b_hop, 0, 3, 0)
    at(27.1, bz_start, 1)
    at(28.0, z_hop, 1, 4)
    for k in range(5, NZ):
        at(28.1 + k / 100, y_send, 1, k)
    at(29.5, b_hop, 0, 3, 1)
    at(30.0, z_hop, 2, 3)
    at(32.0, b_hop, 0, 4, 0)
    at(32.1, b_hop, 0, 4, 1)
    for i, (time, sq, k) in enumerate((
        (11.5, 0, 0), (12.0, 1, 0), (15.0, 0, 1), (15.1, 0, 2), (18.0, 0, 3), (18.1, 0, 4),
        (21.0, 1, 1), (21.1, 1, 2), (22.5, 0, 5), (22.6, 0, 6), (22.7, 0, 7),
        (26.0, 1, 3), (26.1, 1, 4), (31.0, 1, 5), (31.1, 1, 6), (34.0, 1, 7),
    )):
        at(time, "attend", sq, k)
    for k in range(NZ):
        at(27.5 + 2.6 * k, y_pass, 1, k)
        at(31.5 + 2.6 * k, y_last, 1, k)
    at(34.5, residual, 0)
    at(35.0, b_hop, 1, 1, 0)
    at(36.0, o_project, 1)
    at(37.0, z_hop, 2, 4)
    at(39.0, b_hop, 1, 1, 1)
    for k in range(NZ):
        at(39.0 + 1.5 * k, y_send, 2, k)
        at(49.0 + 2.6 * k, y_pass, 2, k)
        at(52.0 + 2.6 * k, y_last, 2, k)
    at(42.5, b_hop, 1, 2, 0)
    at(45.0, second_norm, 0)
    at(46.4, b_hop, 1, 2, 1)
    at(48.5, residual, 1)
    at(50.0, b_hop, 1, 3, 0)
    at(54.0, b_hop, 1, 3, 1)
    at(56.5, second_norm, 1)
    at(57.0, gate_dot)
    at(58.0, b_hop, 1, 4, 0)
    at(58.1, b_hop, 1, 4, 1)
    at(60.0, up_dot)
    at(60.5, down_stage, 0)
    at(63.0, down_stage, 1)
    at(68.6, down_stage, 2)
    at(72.0, down_stage, 3)

    plan.sort(key=lambda e: e[:2])
    items, before, after = [], [], []
    for _, _, act_, args in plan:
        if act_ == "attend":
            items.append(args)
            before.append(after)
            after = []
        else:
            after.append((act_, args))

    def run(events):
        for act_, args in events:
            act_(*args)

    def pick(t, values):
        total = 0
        for i, v in enumerate(values):
            if v:
                total = total + jnp.where(t == i, v, 0)
        return total

    def item(t, _):
        for i, events in enumerate(before):
            if events:
                pl.when(t == i)(lambda events=events: run(events))
        sq = pick(t, [e[0] for e in items])
        k = pick(t, [e[1] for e in items])

        @pl.when(sq == 0)
        def _():
            a_wait(0, k)

        @pl.when(sq == 1)
        def _():
            b_wait(0, k)

        attend_round(sq, k)
        return 0

    lax.fori_loop(0, len(items), item, 0)
    run(after)

    def sent(k, _):
        for st in range(3):
            ref = block(st, y, zk_of(k))
            a_copy(ref, st, YPS, k, yp).wait_send()
            a_copy(ref, st, YMS, k, ym).wait_send()
            a_copy(half(st, ref, 0), st, HPS, k, yp).wait_send()
            a_copy(half(st, ref, 1), st, HMS, k, ym).wait_send()
            a_copy(a_ref(st, ALL, wrap(zk_of(k), NZ), c), st, DS, k, partner).wait_send()
        for st in range(2):
            b_copy(st, b_ref(st, ALL, wrap(zk_of(k), NZ), c), DZ + k, partner).wait_send()
        return 0

    lax.fori_loop(0, NZ, sent, 0)
    for st in range(3):
        for k in range(1, NZ):
            z_copy(st, k, z, True).wait_send()
    for st in range(2):
        b_copy(st, b_block(st, y), BYP, yp).wait_send()
        b_copy(st, b_block(st, y), BYM, ym).wait_send()
        b_copy(st, b_block(st, y, 0), BHP, yp).wait_send()
        b_copy(st, b_block(st, y, 1), BHM, ym).wait_send()
        for w in range(2):
            for i in range(1, r_steps(w) + 1):
                r_copy(st, i, w).wait_send()
            for i in range(1, l_steps(w) + 1):
                l_copy(st, i, w).wait_send()
    for sq in range(2):
        for j in (1, 2, 3):
            rs1_send(sq, j).wait_send()
            ag_send(sq, j).wait_send()

    def lane_sums(part):
        return jnp.sum(part.T, axis=0, keepdims=True)

    in_norm = lane_sums(innp[...])

    so_far = None
    for i in range(4):
        so_far = layer_stage(i, so_far)
    out_copy = pltpu.make_async_copy(layer_v, out_hbm, osem.at[0])
    rowi = lax.broadcasted_iota(jnp.int32, (8, ROWS), 0)
    sums[m] = jnp.where(rowi == 0, lane_sums(so_far[0]), lane_sums(so_far[1]))

    def s_copy(j):
        return rcx(sums.at[m], sums.at[m], s_send.at[j], s_recv.at[j], wrap(m + j, MP))

    def s_from(j):
        src = wrap(m - j, MP)
        return rcx(sums.at[src], sums.at[src], s_send.at[j], s_recv.at[j], src)

    for j in (2, 1, 3):
        s_copy(j).start()
    out_copy.start()
    for j in (1, 3, 2):
        s_from(j).wait_recv()
    both = sums[0] + sums[1] + sums[2] + sums[3]
    cross, out_norm = both[0:1, :], both[1:2, :]
    cosine = cross / jnp.sqrt((in_norm + norm_eps) * (out_norm + norm_eps))
    lane = lax.broadcasted_iota(jnp.int32, (1, ROWS), 1)
    pos = s * TOK + lax.rem(lane, TOK)
    limit = jnp.where(lane < TOK, len_ref[0], len_ref[1])
    influence = jnp.where(pos < limit, 1.0 - cosine, 0.0)
    infl_ref[0:1, :] = influence[:, 0:TOK]
    infl_ref[1:2, :] = influence[:, TOK:2 * TOK]
    t0 = jnp.sum(influence[:, 0:TOK], axis=1, keepdims=True)
    t1 = jnp.sum(influence[:, TOK:2 * TOK], axis=1, keepdims=True)
    lane = lax.broadcasted_iota(jnp.int32, (1, HEAD), 1)
    one = pl.ds(0, 1)
    tot[s, one, :] = jnp.where(lane < HEAD // 2, t0, t1)

    def t_copy(i):
        ref = tot.at[s, one]
        return rc(ref, ref, t_send.at[0], t_recv.at[0], lax.rem(s + i, NS))

    def t_start(i, _):
        t_copy(i).start()
        return 0

    lax.fori_loop(1, NS, t_start, 0)
    every = tot.at[pl.ds(0, NS - 1), one]
    rc(every, every, t_send.at[0], t_recv.at[0], partner).wait()
    total = jnp.sum(tot[:, 0, :], axis=0, keepdims=True)
    tokens = jnp.where(lane < HEAD // 2, len_ref[0], len_ref[1]).astype(F32)
    score = total / tokens
    score_ref[0] = jnp.sum(jnp.where(lane == 0, score, 0.0))
    score_ref[1] = jnp.sum(jnp.where(lane == HEAD - 1, score, 0.0))

    for i in range(4):
        for j in (1, 2, 3):
            rs2_send(i, j).wait_send()
    for j in (1, 2, 3):
        s_copy(j).wait_send()
    out_copy.wait()


def finish_kernel(layer_hbm, infl_ref, score_ref, out_hbm, infl_out, score_out, buf, sem):
    into = pltpu.make_async_copy(layer_hbm, buf, sem.at[0])
    into.start()
    infl_out[...] = infl_ref[...]
    score_out[0] = score_ref[0]
    score_out[1] = score_ref[1]
    into.wait()
    out = pltpu.make_async_copy(buf, out_hbm, sem.at[1])
    out.start()
    out.wait()


def local(
    hidden_in, attn_gain, q_weight, q_bias, k_weight, k_bias, v_weight, v_bias, o_weight,
    mlp_gain, gate_weight, up_weight, down_weight, lengths,
):
    seqs_n, tok_n, width = hidden_in.shape
    seq_rank = lax.axis_index("seq")
    positions = seq_rank * tok_n + jnp.arange(tok_n, dtype=jnp.int32)
    half_width = HEAD // 2
    inv_freq = rope_base ** (-(jnp.arange(half_width, dtype=jnp.float32) * 2.0) / HEAD)
    angles = positions.astype(jnp.float32)[:, None] * inv_freq[None, :]
    cos = jnp.cos(angles)
    sin = jnp.sin(angles)
    cos_t = jnp.concatenate([cos, cos], axis=-1)
    sin_t = jnp.concatenate([-sin, sin], axis=-1)

    hbm = pl.BlockSpec(memory_space=pltpu.HBM)
    vmem = pl.BlockSpec(memory_space=pltpu.VMEM)
    smem = pl.BlockSpec(memory_space=pltpu.SMEM)
    dma = pltpu.SemaphoreType.DMA
    results = (
        jax.ShapeDtypeStruct((ROWS, QUART), BF16),
        jax.ShapeDtypeStruct((2, TOK), F32),
        jax.ShapeDtypeStruct((2,), F32),
    )
    layer_part, influence, score = pl.pallas_call(
        layer_kernel,
        out_shape=results,
        in_specs=[
            hbm, vmem, hbm, vmem, hbm, vmem, hbm, vmem, hbm, vmem,
            hbm, hbm, hbm, vmem, vmem, smem,
        ],
        out_specs=(hbm, vmem, smem),
        scratch_shapes=[
            pltpu.VMEM((ROWS, D), BF16),
            pltpu.VMEM((ROWS, QUART), BF16),
            pltpu.VMEM((ROWS, D), BF16),
            pltpu.VMEM((D, QCOLS), BF16),
            pltpu.VMEM((D, 2 * HEAD), BF16),
            pltpu.VMEM((MP, QCOLS, QUART), BF16),
            pltpu.VMEM((2, OWN_HEADS * TOK, HEAD), BF16),
            pltpu.VMEM((2, NY, NZ, 2, TOK, 2 * HEAD), BF16),
            pltpu.VMEM((NY, NZ, 2, WR, FFP), BF16),
            pltpu.VMEM((NY, NZ, 2, WR, FFP), BF16),
            pltpu.VMEM((NY, NZ, 2, WR, FFP), BF16),
            pltpu.VMEM((2, OWN_HEADS * TOK, HEAD), F32),
            pltpu.VMEM((2, OWN_HEADS * TOK, HEAD), F32),
            pltpu.VMEM((2, OWN_HEADS * TOK, HEAD), F32),
            pltpu.VMEM((ROWS, QCOLS), BF16),
            pltpu.VMEM((2, MP, TOK, QUART), BF16),
            pltpu.VMEM((MP, ROWS, QUART), BF16),
            pltpu.VMEM((MP, ROWS, QUART), BF16),
            pltpu.VMEM((4, MP, ROWS, HEAD), BF16),
            pltpu.VMEM((4, MP, ROWS, HEAD), BF16),
            pltpu.VMEM((ROWS, D), BF16),
            pltpu.VMEM((ROWS, FFP), BF16),
            pltpu.VMEM((ROWS, HEAD), F32),
            pltpu.VMEM((MP, 8, ROWS), F32),
            pltpu.VMEM((NS, 8, HEAD), F32),
            pltpu.VMEM((ROWS, FFP), F32),
            pltpu.VMEM((ROWS, QUART), BF16),
            dma((12,)),
            dma((1,)),
            dma((3, 6, NZ)),
            dma((3, 6, NZ)),
            dma((2, 28)),
            dma((2, 28)),
            dma((2, 2, MP)),
            dma((2, 2, MP)),
            dma((4, MP)),
            dma((4, MP)),
            dma((MP,)),
            dma((MP,)),
            dma((1,)),
            dma((1,)),
        ],
        compiler_params=pltpu.CompilerParams(
            collective_id=0, has_side_effects=True, vmem_limit_bytes=62 * 1024 * 1024
        ),
        name="layer",
    )(
        hidden_in.reshape(ROWS, width), attn_gain.reshape(1, width), q_weight,
        q_bias.reshape(1, QCOLS), k_weight, k_bias.reshape(KV_HEADS, HEAD), v_weight,
        v_bias.reshape(KV_HEADS, HEAD), o_weight, mlp_gain.reshape(1, width), gate_weight,
        up_weight, down_weight, cos_t, sin_t, lengths,
    )
    layer_part, influence, score = pl.pallas_call(
        finish_kernel,
        out_shape=results,
        in_specs=[hbm, vmem, smem],
        out_specs=(hbm, vmem, smem),
        scratch_shapes=[pltpu.VMEM((ROWS, QUART), BF16), dma((2,))],
        name="finish",
    )(layer_part, influence, score)
    return layer_part.reshape(seqs_n, tok_n, QUART), influence, score


def solution(mesh):
    placed = (
        P(None, "seq", None), P(), P(None, "mp"), P("mp"), P(), P(), P(), P(),
        P("mp", None), P(), P("seq", "mp"), P("seq", "mp"), P("seq", "mp"), P(),
    )
    return jax.shard_map(
        local, mesh=mesh, in_specs=placed,
        out_specs=(P(None, "seq", "mp"), P(None, "seq"), P()), check_vma=False,
    )
```

```python
import jax
import jax.numpy as jnp
from jax import lax
from jax.experimental import pallas as pl
from jax.experimental.pallas import tpu as pltpu
from jax.sharding import PartitionSpec as P

HEADS = 16
KV_HEADS = 2
HEAD = 128
D = 2048
NY, NZ = 4, 8
MP = 4
TOK = 128
ROWS = 2 * TOK
OWN_HEADS = HEADS // MP
QCOLS = OWN_HEADS * HEAD
QUART = D // MP
FFP = 1408
WR = 32
GU_CUT = 2048
DN_CUT = 640
NS = NY * NZ * 2

rope_base = 1000000.0
norm_eps = 1e-06
masked_score = -1e30
EXP2_SCALE = HEAD ** (-0.5) * 1.4426950408889634

MESH = pl.DeviceIdType.MESH
F32, BF16 = jnp.float32, jnp.bfloat16

Z_OFF = (0, -1, 1, -2, 2, -3, 3, -4)

FAR_RIGHT = (True, True, True)

EARLY = (
    ("bs", 1), ("bs", 2), ("zs", 1),
)
LATER = (
    ("zs", 0), ("bs", 0), ("ys", 0, 0), ("bp", 1), ("zs", 2), ("ys", 1, 0), ("bp", 2), ("zh", 1, 1),
    ("bp", 0), ("zh", 0, 1), ("yp", 0, 0), ("bl", 1), ("zh", 2, 1), ("zh", 1, 2), ("yp", 1, 0), ("bl", 2),
    ("zh", 0, 2), ("bl", 0), ("bz", 0), ("yp", 0, 1), ("at", 1, 0), ("yl", 0, 0), ("yp", 0, 2), ("yl", 1, 0),
    ("zh", 0, 3), ("at", 0, 0), ("yp", 0, 3), ("yp", 0, 4), ("bh", 0, 1, 0), ("yl", 0, 1), ("yl", 0, 2),
    ("ys", 1, 1), ("at", 0, 1), ("bh", 0, 1, 1), ("yp", 0, 5), ("at", 0, 2), ("zh", 0, 4), ("yp", 0, 6),
    ("yl", 0, 3), ("yl", 0, 4), ("at", 1, 1), ("bh", 0, 2, 0), ("at", 1, 2), ("ys", 1, 2), ("yp", 1, 1),
    ("at", 0, 3), ("yl", 0, 5), ("bh", 0, 2, 1), ("at", 0, 4), ("yl", 0, 6), ("yp", 0, 7), ("zh", 1, 3),
    ("at", 0, 5), ("bh", 0, 3, 0), ("ys", 1, 3), ("at", 1, 3), ("at", 0, 6), ("yl", 0, 7), ("bh", 0, 3, 1),
    ("yl", 1, 1), ("yp", 1, 2), ("at", 1, 4), ("ys", 1, 4), ("at", 0, 7), ("bz", 1), ("yp", 1, 3),
    ("zh", 1, 4), ("op", 0), ("at", 1, 5), ("bh", 0, 4, 0), ("bh", 0, 4, 1), ("yl", 1, 2), ("ys", 1, 5),
    ("at", 1, 6), ("yp", 1, 4), ("zh", 2, 2), ("at", 1, 7), ("bh", 1, 1, 0), ("yl", 1, 3), ("op", 1),
    ("ys", 1, 6), ("bh", 1, 1, 1), ("yp", 1, 5), ("re", 0), ("zh", 2, 3), ("yl", 1, 4), ("bh", 1, 2, 0),
    ("ys", 1, 7), ("bh", 1, 2, 1), ("yp", 1, 6), ("zh", 2, 4), ("yl", 1, 5), ("re", 1), ("ys", 2, 0),
    ("bz", 2), ("bh", 1, 3, 0), ("ys", 2, 1), ("ys", 2, 2), ("yp", 1, 7), ("bh", 1, 3, 1), ("yl", 1, 6),
    ("ys", 2, 3), ("yp", 2, 0), ("bh", 2, 1, 0), ("sn", 0), ("ys", 2, 4), ("yp", 2, 1), ("yp", 2, 2),
    ("bh", 2, 1, 1), ("ys", 2, 5), ("yl", 1, 7), ("ys", 2, 6), ("yp", 2, 3), ("bh", 1, 4, 0), ("bh", 1, 4, 1),
    ("yl", 2, 0), ("ys", 2, 7), ("yp", 2, 4), ("yl", 2, 1), ("yl", 2, 2), ("sn", 1), ("bh", 2, 2, 0), ("gd",),
    ("bh", 2, 2, 1), ("ud",), ("ds", 0), ("bh", 2, 3, 0), ("yl", 2, 3), ("yl", 2, 4), ("yp", 2, 5),
    ("yp", 2, 6), ("yp", 2, 7), ("bh", 2, 3, 1), ("ds", 1), ("yl", 2, 5), ("yl", 2, 6), ("yl", 2, 7),
    ("bh", 2, 4, 0), ("ds", 2), ("bh", 2, 4, 1), ("ds", 3),
)


def layer_kernel(
    hid_hbm, ag_ref, qw_hbm, qb_ref, kw_hbm, kb_ref, vw_hbm, vb_ref, ow_hbm, mg_ref,
    gate_hbm, up_hbm, down_hbm, cos_ref, sin_ref, len_ref,
    out_hbm, infl_ref, score_ref,
    hid, hidq, normed, qw, kvw, ow, qbuf, kv, gu, down, mbuf, lbuf, accbuf, attn,
    stage1, rs1, resid, stage2, rs2, mlp_in, act, innp, sums, tot, gbuf, layer_v,
    lsem, osem, a_send, a_recv, b_send, b_recv, x_send, x_recv, r_send, r_recv,
    s_sem, t_sem,
):
    s = lax.axis_index("seq")
    m = lax.axis_index("mp")
    y = s // (2 * NZ)
    z = lax.rem(s // 2, NZ)
    c = lax.rem(s, 2)
    kvi = m // 2

    def wrap(v, n):
        return lax.rem(v + 2 * n, n)

    def dev(yy, zz, cc):
        return (wrap(yy, NY) * NZ + wrap(zz, NZ)) * 2 + cc

    zp, zm = dev(y, z + 1, c), dev(y, z - 1, c)
    yp, ym = dev(y + 1, z, c), dev(y - 1, z, c)
    partner = dev(y, z, 1 - c)

    def rc(src, dst, ssem, rsem, sdev):
        return pltpu.make_async_remote_copy(
            src_ref=src, dst_ref=dst, send_sem=ssem, recv_sem=rsem,
            device_id={"seq": sdev, "mp": m}, device_id_type=MESH,
        )

    def rcx(src, dst, ssem, rsem, mdev):
        return pltpu.make_async_remote_copy(
            src_ref=src, dst_ref=dst, send_sem=ssem, recv_sem=rsem,
            device_id={"seq": s, "mp": mdev}, device_id_type=MESH,
        )

    kv_cols = pl.ds(pl.multiple_of(kvi * HEAD, HEAD), HEAD)
    own = gu.at[y, z, c]
    loads = {
        "up": [pltpu.make_async_copy(up_hbm, own.at[:, pl.ds(FFP, FFP)], lsem.at[0])],
        "gate": [pltpu.make_async_copy(gate_hbm, own.at[:, pl.ds(0, FFP)], lsem.at[1])],
        "hid": [pltpu.make_async_copy(hid_hbm, hid, lsem.at[3])],
        "kv": [
            pltpu.make_async_copy(kw_hbm.at[:, kv_cols], kvw.at[:, pl.ds(0, HEAD)], lsem.at[4]),
            pltpu.make_async_copy(vw_hbm.at[:, kv_cols], kvw.at[:, pl.ds(HEAD, HEAD)], lsem.at[8]),
        ],
        "q": [pltpu.make_async_copy(qw_hbm, qw, lsem.at[5])],
        "down": [pltpu.make_async_copy(down_hbm, down.at[y, z, c], lsem.at[2])],
        "hidq": [pltpu.make_async_copy(
            hid_hbm.at[:, pl.ds(pl.multiple_of(m * QUART, QUART), QUART)], hidq, lsem.at[6])],
        "ow": [
            pltpu.make_async_copy(ow_hbm.at[:, pl.ds(q * QUART, QUART)], ow.at[q], lsem.at[9 + q])
            for q in range(MP)
        ],
    }
    for copies in loads.values():
        for copy in copies:
            copy.start()

    def need(name):
        for copy in loads.pop(name, ()):
            copy.wait()

    bar = pltpu.get_barrier_semaphore()
    for peer in (zp, zm, yp, ym, partner):
        pl.semaphore_signal(bar, inc=1, device_id={"seq": peer, "mp": m}, device_id_type=MESH)
    for i in range(1, MP):
        pl.semaphore_signal(bar, inc=1, device_id={"seq": s, "mp": wrap(m + i, MP)}, device_id_type=MESH)
    pl.semaphore_wait(bar, 5 + MP - 1)

    ALL = slice(None)
    ZR, YR, HR, DR = 0, 4, 12, 20
    A_HALF = (TOK // 2, WR // 2, WR // 2)
    WGU, WDN = ("gate", "up"), ("down",)

    def a_ref(st, yy, zz, cc):
        if st == 0:
            return kv.at[0, yy, zz, cc]
        if st == 1:
            return gu.at[yy, zz, cc, :, pl.ds(0, GU_CUT)]
        return down.at[yy, zz, cc, :, pl.ds(0, DN_CUT)]

    def load_of(st):
        for name in ((), WGU, WDN)[st]:
            need(name)

    def block(st, yy, zz):
        return a_ref(st, wrap(yy, NY), wrap(zz, NZ), c)

    def half(st, ref, i):
        return ref.at[pl.ds(i * A_HALF[st], A_HALF[st])]

    def a_copy(ref, st, ssem, rsem, d):
        return rc(ref, ref, a_send.at[st, ssem], a_recv.at[st, rsem], d)

    def a_wait_recv(st, rsem, *size):
        a_copy(a_ref(st, *size), st, 0, rsem, partner).wait_recv()

    def zk_of(k):
        if isinstance(k, int):
            return z + Z_OFF[k]
        return z + jnp.where(lax.rem(k, 2) == 1, -((k + 1) // 2), k // 2)

    def z_copy(st, k_to, zz, right):
        return a_copy(block(st, y, zz), st, 0, ZR + (k_to - 1) // 2, zp if right else zm)

    def y_send(st, k):
        load_of(st)
        ref = block(st, y, zk_of(k))
        a_copy(ref, st, 1, YR + k, yp).start()
        a_copy(ref, st, 1, YR + k, ym).start()

    TWO = pl.ds(0, 2)

    def y_pass(st, k):
        zz = zk_of(k)
        a_wait_recv(st, YR + k, TWO, 0, 0)
        a_copy(half(st, block(st, y - 1, zz), 0), st, 1, HR + k, yp).start()
        a_copy(half(st, block(st, y + 1, zz), 1), st, 1, HR + k, ym).start()

    def d_index(st, k):
        return DR + (k, 0, max(0, (k - 1) // 2))[st]

    def y_last(st, k):
        a_wait_recv(st, HR + k, 0, 0, 0)
        a_copy(a_ref(st, ALL, wrap(zk_of(k), NZ), c), st, 1, d_index(st, k), partner).start()

    def z_start(st):
        load_of(st)
        z_copy(st, 1, z, True).start()
        z_copy(st, 2, z, False).start()

    def z_hop(st, h):
        far_right = FAR_RIGHT[st]
        a_wait_recv(st, ZR + h - 1, TWO if h < 4 else 0, 0, 0)
        for k in (2 * h - 1, 2 * h):
            if k >= NZ:
                continue
            right = far_right if k == 7 else k % 2 == 1
            if k + 2 < NZ - 1:
                z_copy(st, k + 2, zk_of(k), right).start()
            if k == (5 if far_right else 6):
                z_copy(st, 7, zk_of(k), far_right).start()
            if st == 0:
                y_send(st, k)

    BY, BH, BZ, BD = 0, 1, 2, 10
    B_HALF = (TOK // 2, WR // 2, WR // 2)

    def b_ref(st, yy, zz, cc):
        if st == 0:
            return kv.at[1, yy, zz, cc]
        if st == 1:
            return gu.at[yy, zz, cc, :, pl.ds(GU_CUT, 2 * FFP - GU_CUT)]
        return down.at[yy, zz, cc, :, pl.ds(DN_CUT, FFP - DN_CUT)]

    def b_copy(st, ref, ssem, rsem, d):
        return rc(ref, ref, b_send.at[st, ssem], b_recv.at[st, rsem], d)

    def b_wait_recv(st, rsem, *size):
        b_copy(st, b_ref(st, *size), 0, rsem, partner).wait_recv()

    def b_block(st, yy, w=None):
        ref = b_ref(st, wrap(yy, NY), z, c)
        return ref if w is None else ref.at[pl.ds(w * B_HALF[st], B_HALF[st])]

    def group(st, zz, w):
        rows = pl.ds(w * B_HALF[st], B_HALF[st])
        zz = wrap(zz, NZ)
        if st == 0:
            return kv.at[1, :, zz, c, rows]
        if st == 1:
            return gu.at[:, zz, c, rows, pl.ds(GU_CUT, 2 * FFP - GU_CUT)]
        return down.at[:, zz, c, rows, pl.ds(DN_CUT, FFP - DN_CUT)]

    def r_copy(st, i, w):
        return b_copy(st, group(st, z - (i - 1), w), 1, BZ + 2 * (i - 1) + w, zp)

    def l_copy(st, i, w):
        return b_copy(st, group(st, z + (i - 1), w), 1, BZ + 2 * (i - 1) + w, zm)

    def r_steps(w):
        return 4 if w == 0 else 3

    def l_steps(w):
        return 3 if w == 0 else 4

    def by_start(st):
        for name in ((), WGU[1:], WDN)[st]:
            need(name)
        b_copy(st, b_block(st, y), 0, BY, yp).start()
        b_copy(st, b_block(st, y), 0, BY, ym).start()

    def by_pass(st):
        b_wait_recv(st, BY, TWO, 0, 0)
        b_copy(st, b_block(st, y - 1, 0), 0, BH, yp).start()
        b_copy(st, b_block(st, y + 1, 1), 0, BH, ym).start()

    def bd_start(st, k):
        b_copy(st, b_ref(st, ALL, wrap(zk_of(k), NZ), c), 2,
               BD + (k, 0, max(0, (k - 1) // 2))[st], partner).start()

    def by_last(st):
        b_wait_recv(st, BH, 0, 0, 0)
        bd_start(st, 0)

    def bz_start(st):
        for w in range(2):
            r_copy(st, 1, w).start()
            l_copy(st, 1, w).start()

    def b_hop(st, h, w):
        b_wait_recv(st, BZ + 2 * (h - 1) + w, ALL if h < 4 else TWO, 0, 0)
        if h + 1 <= r_steps(w):
            r_copy(st, h + 1, w).start()
        if h + 1 <= l_steps(w):
            l_copy(st, h + 1, w).start()
        if w == 1:
            for k in (2 * h - 1, 2 * h):
                if k < NZ:
                    bd_start(st, k)

    TASKS = {
        "zs": z_start, "zh": z_hop, "ys": y_send, "yp": y_pass, "yl": y_last,
        "bs": by_start, "bp": by_pass, "bl": by_last, "bz": bz_start, "bh": b_hop,
    }
    for name, *args in EARLY:
        TASKS[name](*args)

    need("hid")

    def norm_rows(i, _):
        r = pl.ds(pl.multiple_of(i * 16, 16), 16)
        x = hid[r, :].astype(F32)
        sq = x * x
        part = sq[:, 0:HEAD]
        for j in range(1, D // HEAD):
            part = part + sq[:, j * HEAD:(j + 1) * HEAD]
        innp[r, :] = part
        factor = lax.rsqrt(jnp.sum(part, axis=-1, keepdims=True) * (1.0 / D) + norm_eps)
        normed[r, :] = (x * factor * ag_ref[...]).astype(BF16)
        return 0

    lax.fori_loop(0, ROWS // 16, norm_rows, 0, unroll=4)

    cos = cos_ref[...]
    sin = sin_ref[...]

    def rope(u):
        return u * cos + pltpu.roll(u, HEAD // 2, 1) * sin

    need("kv")
    kv_all = jnp.dot(normed[...], kvw[...], preferred_element_type=F32)
    kb = kb_ref[pl.ds(kvi, 1), :]
    vb = vb_ref[pl.ds(kvi, 1), :]
    for sq in range(2):
        kk = kv_all[sq * TOK:(sq + 1) * TOK, 0:HEAD] + kb
        vv = kv_all[sq * TOK:(sq + 1) * TOK, HEAD:2 * HEAD] + vb
        kv[sq, y, z, c, :, 0:HEAD] = rope(kk).astype(BF16)
        kv[sq, y, z, c, :, HEAD:2 * HEAD] = vv.astype(BF16)

    need("q")
    q_all = jnp.dot(normed[...], qw[...], preferred_element_type=F32) + qb_ref[...]
    for sq in range(2):
        for h in range(OWN_HEADS):
            u = q_all[sq * TOK:(sq + 1) * TOK, h * HEAD:(h + 1) * HEAD]
            qbuf[sq, h * TOK:(h + 1) * TOK, :] = rope(u).astype(BF16)

    for sq in range(2):
        mbuf[sq] = jnp.full((OWN_HEADS * TOK, HEAD), masked_score, F32)
        lbuf[sq] = jnp.zeros((OWN_HEADS * TOK, HEAD), F32)
        accbuf[sq] = jnp.zeros((OWN_HEADS * TOK, HEAD), F32)

    def attend(sq, yks, zk, diagonal):
        pairs = [kv[sq, yk, zk] for yk in yks]
        kb_ = jnp.concatenate([p[:, :, 0:HEAD].reshape(2 * TOK, HEAD) for p in pairs], axis=0)
        vb_ = jnp.concatenate([p[:, :, HEAD:2 * HEAD].reshape(2 * TOK, HEAD) for p in pairs], axis=0)
        sc = lax.dot_general(qbuf[sq], kb_, (((1,), (1,)), ((), ())), preferred_element_type=F32)
        if diagonal:
            row = lax.rem(lax.broadcasted_iota(jnp.int32, sc.shape, 0), TOK) + c * TOK
            col = lax.broadcasted_iota(jnp.int32, sc.shape, 1)
            sc = jnp.where(col <= row, sc, masked_score)
        m_old = mbuf[sq]
        m_new = jnp.maximum(m_old, jnp.max(sc, axis=1, keepdims=True))
        p = jnp.exp2((sc - jnp.concatenate([m_new] * (2 * len(yks)), axis=1)) * EXP2_SCALE)
        alpha = jnp.exp2((m_old - m_new) * EXP2_SCALE)
        mbuf[sq] = m_new
        lbuf[sq] = lbuf[sq] * alpha + jnp.sum(p, axis=1, keepdims=True)
        accbuf[sq] = accbuf[sq] * alpha + jnp.dot(p.astype(BF16), vb_, preferred_element_type=F32)

    def attend_round(sq, k):
        zk = wrap(zk_of(k), NZ)

        @pl.when(k == 0)
        def _():
            attend(sq, (y,), zk, True)

        n = y + jnp.where(zk < z, 1, 0)

        def step(i, _):
            attend(sq, (2 * i, 2 * i + 1), zk, False)
            return 0

        lax.fori_loop(0, n // 2, step, 0)

        @pl.when(lax.rem(n, 2) == 1)
        def _():
            attend(sq, (n - 1,), zk, False)

    def seq_rows(sq):
        return pl.ds(sq * TOK, TOK)

    def rs1_send(sq, j):
        return rcx(stage1.at[sq, j], rs1.at[m, seq_rows(sq)], x_send.at[0], x_recv.at[0, sq],
                   wrap(m + j, MP))

    def three(buf, sq):
        return buf.at[pl.ds(0, MP - 1), seq_rows(sq)]

    def o_project(sq):
        need("ow")
        for h in range(OWN_HEADS):
            r = slice(h * TOK, (h + 1) * TOK)
            attn[sq * TOK:(sq + 1) * TOK, h * HEAD:(h + 1) * HEAD] = (
                accbuf[sq, r, :] / lbuf[sq, r, :]
            ).astype(BF16)
        here = attn[sq * TOK:(sq + 1) * TOK, :]
        for j in (2, 1, 3, 0):
            part = jnp.dot(here, ow[wrap(m + j, MP)], preferred_element_type=F32).astype(BF16)
            if j == 0:
                rs1[m, seq_rows(sq), :] = part
            else:
                stage1[sq, j] = part
        for j in (2, 1, 3):
            rs1_send(sq, j).start()

    def ag_send(sq, j):
        ref = resid.at[m, seq_rows(sq)]
        return rcx(ref, ref, x_send.at[1], x_recv.at[1, sq], wrap(m + j, MP))

    def residual(sq):
        need("hidq")
        rcx(three(rs1, sq), three(rs1, sq), x_send.at[0], x_recv.at[0, sq], wrap(m + 1, MP)).wait_recv()
        r = seq_rows(sq)
        add = rs1[0, r, :].astype(F32)
        for q in range(1, MP):
            add = add + rs1[q, r, :].astype(F32)
        resid[m, r, :] = (hidq[r, :].astype(F32) + add).astype(BF16)
        for j in (2, 1, 3):
            ag_send(sq, j).start()

    def second_norm(sq):
        rcx(three(resid, sq), three(resid, sq), x_send.at[1], x_recv.at[1, sq], wrap(m + 1, MP)).wait_recv()

        def norm2_rows(i, _):
            r = pl.ds(pl.multiple_of(sq * TOK + i * 16, 16), 16)
            xs = [resid[q, r, :].astype(F32) for q in range(MP)]
            part = None
            for x in xs:
                sqr = x * x
                for j in range(QUART // HEAD):
                    t = sqr[:, j * HEAD:(j + 1) * HEAD]
                    part = t if part is None else part + t
            factor = lax.rsqrt(jnp.sum(part, axis=-1, keepdims=True) * (1.0 / D) + norm_eps)
            for q in range(MP):
                cols = slice(q * QUART, (q + 1) * QUART)
                mlp_in[r, cols] = (xs[q] * factor * mg_ref[:, cols]).astype(BF16)
            return 0

        lax.fori_loop(0, TOK // 16, norm2_rows, 0, unroll=4)

    def gate_dot():
        a_wait_recv(1, DR, ALL, ALL, 0)
        rows = gu[:, :, :, :, 0:FFP].reshape(D, FFP)
        gbuf[...] = jnp.dot(mlp_in[...], rows, preferred_element_type=F32)

    def up_dot():
        b_wait_recv(1, BD, ALL, ALL, 0)
        rows = gu[:, :, :, :, FFP:2 * FFP].reshape(D, FFP)
        up_sum = jnp.dot(mlp_in[...], rows, preferred_element_type=F32)
        g = gbuf[...]
        act[...] = (g / (1.0 + jnp.exp(-g)) * up_sum).astype(BF16)

    odd = lax.rem(z, 2)

    def z_pair(i):
        turn = (0, 2 * odd - 1, 1 - 2 * odd, 2)[i]
        return wrap(z // 2 + turn, NZ // 2)

    def rs2_send(i, j):
        q = wrap(m + j, MP)
        return rcx(stage2.at[i, q], rs2.at[i, m], r_send.at[0], r_recv.at[i], q)

    def down_stage(i):
        rounds = pl.ds(0, (3, 2, 2, 1)[i])
        a_wait_recv(2, DR + i, ALL, rounds, 0)
        b_wait_recv(2, BD + i, ALL, rounds, 0)
        p = z_pair(i)
        for q0 in (0, 2):
            rows = down[q0:q0 + 2, pl.ds(2 * p, 2)].reshape(2 * HEAD, FFP)
            part = lax.dot_general(
                act[...], rows, (((1,), (1,)), ((), ())), preferred_element_type=F32
            ).astype(BF16)
            stage2[i, q0] = part[:, 0:HEAD]
            stage2[i, q0 + 1] = part[:, HEAD:2 * HEAD]
        for j in (2, 1, 3):
            rs2_send(i, j).start()

    def layer_stage(i, so_far):
        came = rs2.at[i, pl.ds(0, MP - 1)]
        rcx(came, came, r_send.at[0], r_recv.at[i], wrap(m + 1, MP)).wait_recv()
        cols = pl.ds(pl.multiple_of(z_pair(i) * HEAD, HEAD), HEAD)
        add = stage2[i, m].astype(F32)
        for j in range(1, MP):
            add = add + rs2[i, wrap(m - j, MP)].astype(F32)
        layer = (resid[m, :, cols].astype(F32) + add).astype(BF16)
        layer_v[:, cols] = layer
        wide = layer.astype(F32)
        cp, op = hidq[:, cols].astype(F32) * wide, wide * wide
        return (cp, op) if so_far is None else (so_far[0] + cp, so_far[1] + op)

    TASKS.update(
        op=o_project, re=residual, sn=second_norm, gd=gate_dot, ud=up_dot, ds=down_stage,
    )
    items, before, after = [], [], []
    for name, *args in LATER:
        if name == "at":
            items.append(args)
            before.append(after)
            after = []
        else:
            after.append((TASKS[name], args))

    def run(events):
        for act_, args in events:
            act_(*args)

    def pick(t, values):
        total = 0
        for i, v in enumerate(values):
            if v:
                total = total + jnp.where(t == i, v, 0)
        return total

    def item(t, _):
        for i, events in enumerate(before):
            if events:
                pl.when(t == i)(lambda events=events: run(events))
        sq = pick(t, [e[0] for e in items])
        k = pick(t, [e[1] for e in items])

        @pl.when(sq == 0)
        def _():
            a_wait_recv(0, DR + k, ALL, 0, 0)

        @pl.when(sq == 1)
        def _():
            b_wait_recv(0, BD + k, ALL, 0, 0)

        attend_round(sq, k)
        return 0

    lax.fori_loop(0, len(items), item, 0)
    run(after)

    seven = pl.ds(0, NZ - 1)
    for st in range(3):
        a_copy(a_ref(st, 0, seven, 0), st, 0, 0, partner).wait_send()
        a_copy(a_ref(st, ALL, seven, ALL), st, 1, 0, partner).wait_send()
        b_copy(st, b_ref(st, 0, pl.ds(0, 3), 0), 0, 0, partner).wait_send()
        b_copy(st, b_ref(st, ALL, seven, 0), 1, 0, partner).wait_send()
        b_copy(st, b_ref(st, ALL, ALL, 0), 2, 0, partner).wait_send()
    six = rs1.at[pl.ds(0, MP - 1)]
    for phase in range(2):
        rcx(six, six, x_send.at[phase], x_recv.at[0, 0], wrap(m + 1, MP)).wait_send()

    def lane_sums(part):
        return jnp.sum(part.T, axis=0, keepdims=True)

    in_norm = lane_sums(innp[...])

    so_far = None
    for i in range(4):
        so_far = layer_stage(i, so_far)
    out_copy = pltpu.make_async_copy(layer_v, out_hbm, osem.at[0])
    rowi = lax.broadcasted_iota(jnp.int32, (8, ROWS), 0)
    sums[m] = jnp.where(rowi == 0, lane_sums(so_far[0]), lane_sums(so_far[1]))

    def s_copy(j):
        return rcx(sums.at[m], sums.at[m], s_sem.at[0], s_sem.at[1], wrap(m + j, MP))

    for j in (2, 1, 3):
        s_copy(j).start()
    out_copy.start()
    came = sums.at[pl.ds(0, MP - 1)]
    rcx(came, came, s_sem.at[0], s_sem.at[1], wrap(m + 1, MP)).wait()
    both = sums[0] + sums[1] + sums[2] + sums[3]
    cross, out_norm = both[0:1, :], both[1:2, :]
    cosine = cross / jnp.sqrt((in_norm + norm_eps) * (out_norm + norm_eps))
    lane = lax.broadcasted_iota(jnp.int32, (1, ROWS), 1)
    pos = s * TOK + lax.rem(lane, TOK)
    limit = jnp.where(lane < TOK, len_ref[0], len_ref[1])
    influence = jnp.where(pos < limit, 1.0 - cosine, 0.0)
    infl_ref[0:1, :] = influence[:, 0:TOK]
    infl_ref[1:2, :] = influence[:, TOK:2 * TOK]
    t0 = jnp.sum(influence[:, 0:TOK], axis=1, keepdims=True)
    t1 = jnp.sum(influence[:, TOK:2 * TOK], axis=1, keepdims=True)
    lane = lax.broadcasted_iota(jnp.int32, (1, HEAD), 1)
    one = pl.ds(0, 1)
    tot[s, one, :] = jnp.where(lane < HEAD // 2, t0, t1)

    def t_copy(i):
        ref = tot.at[s, one]
        return rc(ref, ref, t_sem.at[0], t_sem.at[1], lax.rem(s + i, NS))

    def t_start(i, _):
        t_copy(i).start()
        return 0

    lax.fori_loop(1, NS, t_start, 0)
    every = tot.at[pl.ds(0, NS - 1), one]
    rc(every, every, t_sem.at[0], t_sem.at[1], partner).wait()
    total = jnp.sum(tot[:, 0, :], axis=0, keepdims=True)
    tokens = jnp.where(lane < HEAD // 2, len_ref[0], len_ref[1]).astype(F32)
    score = total / tokens
    score_ref[0] = jnp.sum(jnp.where(lane == 0, score, 0.0))
    score_ref[1] = jnp.sum(jnp.where(lane == HEAD - 1, score, 0.0))

    gone = rs2.at[pl.ds(0, MP - 1)]
    rcx(gone, gone, r_send.at[0], r_recv.at[0], wrap(m + 1, MP)).wait_send()
    out_copy.wait()


def finish_kernel(layer_hbm, infl_hbm, score_hbm, out_hbm, infl_out, score_out, buf, sem):
    into = pltpu.make_async_copy(layer_hbm, buf, sem.at[0])
    small = [
        pltpu.make_async_copy(infl_hbm, infl_out, sem.at[1]),
        pltpu.make_async_copy(score_hbm, score_out, sem.at[2]),
    ]
    into.start()
    for copy in small:
        copy.start()
    into.wait()
    out = pltpu.make_async_copy(buf, out_hbm, sem.at[3])
    out.start()
    for copy in small:
        copy.wait()
    out.wait()


def local(
    hidden_in, attn_gain, q_weight, q_bias, k_weight, k_bias, v_weight, v_bias, o_weight,
    mlp_gain, gate_weight, up_weight, down_weight, lengths,
):
    seqs_n, tok_n, width = hidden_in.shape
    seq_rank = lax.axis_index("seq")
    positions = seq_rank * tok_n + jnp.arange(tok_n, dtype=jnp.int32)
    half_width = HEAD // 2
    inv_freq = rope_base ** (-(jnp.arange(half_width, dtype=jnp.float32) * 2.0) / HEAD)
    angles = positions.astype(jnp.float32)[:, None] * inv_freq[None, :]
    cos = jnp.cos(angles)
    sin = jnp.sin(angles)
    cos_t = jnp.concatenate([cos, cos], axis=-1)
    sin_t = jnp.concatenate([-sin, sin], axis=-1)

    hbm = pl.BlockSpec(memory_space=pltpu.HBM)
    vmem = pl.BlockSpec(memory_space=pltpu.VMEM)
    smem = pl.BlockSpec(memory_space=pltpu.SMEM)
    dma = pltpu.SemaphoreType.DMA
    results = (
        jax.ShapeDtypeStruct((ROWS, QUART), BF16),
        jax.ShapeDtypeStruct((2, TOK), F32),
        jax.ShapeDtypeStruct((2,), F32),
    )
    layer_part, influence, score = pl.pallas_call(
        layer_kernel,
        out_shape=results,
        in_specs=[
            hbm, vmem, hbm, vmem, hbm, vmem, hbm, vmem, hbm, vmem,
            hbm, hbm, hbm, vmem, vmem, smem,
        ],
        out_specs=(hbm, vmem, smem),
        scratch_shapes=[
            pltpu.VMEM((ROWS, D), BF16),
            pltpu.VMEM((ROWS, QUART), BF16),
            pltpu.VMEM((ROWS, D), BF16),
            pltpu.VMEM((D, QCOLS), BF16),
            pltpu.VMEM((D, 2 * HEAD), BF16),
            pltpu.VMEM((MP, QCOLS, QUART), BF16),
            pltpu.VMEM((2, OWN_HEADS * TOK, HEAD), BF16),
            pltpu.VMEM((2, NY, NZ, 2, TOK, 2 * HEAD), BF16),
            pltpu.VMEM((NY, NZ, 2, WR, 2 * FFP), BF16),
            pltpu.VMEM((NY, NZ, 2, WR, FFP), BF16),
            pltpu.VMEM((2, OWN_HEADS * TOK, HEAD), F32),
            pltpu.VMEM((2, OWN_HEADS * TOK, HEAD), F32),
            pltpu.VMEM((2, OWN_HEADS * TOK, HEAD), F32),
            pltpu.VMEM((ROWS, QCOLS), BF16),
            pltpu.VMEM((2, MP, TOK, QUART), BF16),
            pltpu.VMEM((MP, ROWS, QUART), BF16),
            pltpu.VMEM((MP, ROWS, QUART), BF16),
            pltpu.VMEM((4, MP, ROWS, HEAD), BF16),
            pltpu.VMEM((4, MP, ROWS, HEAD), BF16),
            pltpu.VMEM((ROWS, D), BF16),
            pltpu.VMEM((ROWS, FFP), BF16),
            pltpu.VMEM((ROWS, HEAD), F32),
            pltpu.VMEM((MP, 8, ROWS), F32),
            pltpu.VMEM((NS, 8, HEAD), F32),
            pltpu.VMEM((ROWS, FFP), F32),
            pltpu.VMEM((ROWS, QUART), BF16),
            dma((13,)),
            dma((1,)),
            dma((3, 2)),
            dma((3, 28)),
            dma((3, 3)),
            dma((3, 18)),
            dma((2,)),
            dma((2, 2)),
            dma((1,)),
            dma((4,)),
            dma((2,)),
            dma((2,)),
        ],
        compiler_params=pltpu.CompilerParams(
            collective_id=0, has_side_effects=True, vmem_limit_bytes=62 * 1024 * 1024
        ),
        name="layer",
    )(
        hidden_in.reshape(ROWS, width), attn_gain.reshape(1, width), q_weight,
        q_bias.reshape(1, QCOLS), k_weight, k_bias.reshape(KV_HEADS, HEAD), v_weight,
        v_bias.reshape(KV_HEADS, HEAD), o_weight, mlp_gain.reshape(1, width), gate_weight,
        up_weight, down_weight, cos_t, sin_t, lengths,
    )
    layer_part, influence, score = pl.pallas_call(
        finish_kernel,
        out_shape=results,
        in_specs=[hbm, hbm, hbm],
        out_specs=(hbm, hbm, hbm),
        scratch_shapes=[pltpu.VMEM((ROWS, QUART), BF16), dma((4,))],
        name="finish",
    )(layer_part, influence, score)
    return layer_part.reshape(seqs_n, tok_n, QUART), influence, score


def solution(mesh):
    placed = (
        P(None, "seq", None), P(), P(None, "mp"), P("mp"), P(), P(), P(), P(),
        P("mp", None), P(), P("seq", "mp"), P("seq", "mp"), P("seq", "mp"), P(),
    )
    return jax.shard_map(
        local, mesh=mesh, in_specs=placed,
        out_specs=(P(None, "seq", "mp"), P(None, "seq"), P()), check_vma=False,
    )
```

```python
import jax
import jax.numpy as jnp
import numpy as np
from jax import lax
from jax.experimental import pallas as pl
from jax.experimental.pallas import tpu as pltpu
from jax.sharding import PartitionSpec as P

HEADS = 16
KV_HEADS = 2
HEAD = 128
D = 2048
NY, NZ = 4, 8
MP = 4
TOK = 128
ROWS = 2 * TOK
OWN_HEADS = HEADS // MP
QCOLS = OWN_HEADS * HEAD
QUART = D // MP
FFP = 1408
WR = 32
GU_CUT = 1792
DN_CUT = 640
NS = NY * NZ * 2

rope_base = 1000000.0
norm_eps = 1e-06
masked_score = -1e30
EXP2_SCALE = HEAD ** (-0.5) * 1.4426950408889634


def rotation_tables():
    freq = rope_base ** (-2.0 * np.arange(HEAD // 2) / HEAD)
    freq = np.concatenate([freq, freq])
    near = np.arange(TOK)[:, None] * freq
    far = TOK * np.arange(NS)[:, None] * freq
    return np.stack([np.cos(near), np.sin(near)]).astype(np.float32), np.stack(
        [np.cos(far), np.sin(far)]).astype(np.float32)


MESH = pl.DeviceIdType.MESH
F32, BF16 = jnp.float32, jnp.bfloat16

Z_OFF = (0, -1, 1, -2, 2, -3, 3, -4)

FAR_RIGHT = (False, True, True)

EARLY = (
    ("bs", 2), ("zs", 2), ("zs", 1), ("bs", 1),
)
LATER = (
    ("ys", 2, 0), ("bs", 0), ("zs", 0), ("ys", 0, 0), ("zh", 2, 1), ("bp", 2), ("bp", 1), ("zh", 1, 1),
    ("yp", 2, 0), ("bp", 0), ("zh", 0, 1), ("yp", 0, 0), ("zh", 2, 2), ("bl", 2), ("bl", 1), ("yl", 2, 0),
    ("bl", 0), ("bz", 0), ("ys", 1, 0), ("yp", 0, 1), ("zh", 0, 2), ("yp", 0, 2), ("zh", 2, 3), ("yl", 0, 0),
    ("xl", 0), ("bh", 0, 1, 0), ("at", 0, 0), ("bh", 0, 1, 1), ("yl", 0, 1), ("yp", 1, 0), ("at", 1, 0),
    ("zh", 1, 2), ("zh", 2, 4), ("zh", 0, 3), ("yp", 0, 3), ("at", 0, 1), ("bh", 0, 2, 0), ("yp", 0, 4),
    ("yl", 0, 2), ("bh", 0, 2, 1), ("yl", 1, 0), ("xl", 1), ("at", 0, 2), ("yp", 0, 5), ("ys", 1, 1),
    ("zh", 1, 3), ("at", 1, 1), ("xl", 2), ("zh", 0, 4), ("yp", 0, 6), ("yl", 0, 3), ("yl", 0, 4),
    ("bh", 0, 3, 0), ("yl", 0, 5), ("xl", 3), ("bh", 0, 3, 1), ("at", 1, 2), ("ys", 1, 2), ("bz", 1),
    ("at", 0, 3), ("zh", 1, 4), ("yp", 1, 1), ("at", 0, 4), ("bh", 0, 4, 0), ("xl", 4), ("yl", 0, 6),
    ("bh", 0, 4, 1), ("yp", 0, 7), ("at", 1, 3), ("at", 0, 5), ("xl", 5), ("ys", 1, 3), ("yp", 1, 2),
    ("bh", 1, 1, 0), ("at", 1, 4), ("yl", 1, 1), ("yl", 0, 7), ("at", 0, 6), ("xl", 6), ("bh", 1, 1, 1),
    ("ys", 1, 4), ("at", 1, 5), ("at", 0, 7), ("yp", 1, 3), ("xl", 7), ("yl", 1, 2), ("op", 0), ("bz", 2),
    ("at", 1, 6), ("ys", 1, 5), ("at", 1, 7), ("yp", 1, 4), ("op", 1), ("bh", 1, 2, 0), ("yl", 1, 3),
    ("bh", 1, 2, 1), ("rm", 0), ("bh", 2, 1, 0), ("ys", 1, 6), ("yp", 1, 5), ("bh", 2, 1, 1), ("rm", 1),
    ("yl", 1, 4), ("ys", 1, 7), ("bh", 1, 3, 0), ("re", 0), ("yp", 1, 6), ("yl", 1, 5), ("bh", 1, 3, 1),
    ("ys", 2, 1), ("re", 1), ("ys", 2, 2), ("yp", 1, 7), ("bh", 2, 2, 0), ("yl", 1, 6), ("ap", 0),
    ("ys", 2, 3), ("yp", 2, 1), ("bh", 2, 2, 1), ("yp", 2, 2), ("ys", 2, 4), ("yl", 1, 7), ("ys", 2, 5),
    ("ap", 1), ("yp", 2, 3), ("yl", 2, 1), ("bh", 1, 4, 0), ("bh", 1, 4, 1), ("ys", 2, 6), ("sn", 0),
    ("yl", 2, 2), ("ys", 2, 7), ("yp", 2, 4), ("yp", 2, 5), ("bh", 2, 3, 0), ("sn", 1), ("gd",),
    ("bh", 2, 3, 1), ("yp", 2, 6), ("yl", 2, 3), ("yp", 2, 7), ("ud",), ("bh", 2, 4, 0), ("yl", 2, 4),
    ("yl", 2, 5), ("ds", 0), ("yl", 2, 6), ("yl", 2, 7), ("ds", 1), ("bh", 2, 4, 1), ("ds", 2), ("dm", 0),
    ("ds", 3), ("dm", 1), ("dm", 2), ("dm", 3),
)


def layer_kernel(
    hid_hbm, ag_hbm, qw_hbm, qb_hbm, kw_hbm, kb_hbm, vw_hbm, vb_hbm, ow_hbm, mg_hbm,
    gate_hbm, up_hbm, down_hbm, near_hbm, far_hbm, len_ref,
    out_hbm, infl_ref, score_ref,
    hid, hidq, normed, qw, kvw, ow, qbuf, kv, gu, down, mbuf, accbuf, attn,
    stage1, tr1, rs1, resid, stage2, tr2, rs2, mlp_in, act, innp, sums, tot, gbuf, layer_v,
    ag_ref, mg_ref, qb_ref, kb_ref, vb_ref, near_ref, far_ref,
    lsem, osem, a_send, a_recv, b_send, b_recv, k_send, k_recv, x_send, x_recv, r_send, r_recv,
    s_sem, t_sem,
):
    s = lax.axis_index("seq")
    m = lax.axis_index("mp")
    y = s // (2 * NZ)
    z = lax.rem(s // 2, NZ)
    c = lax.rem(s, 2)
    kvi = m // 2

    def wrap(v, n):
        return lax.rem(v + 2 * n, n)

    def dev(yy, zz, cc):
        return (wrap(yy, NY) * NZ + wrap(zz, NZ)) * 2 + cc

    zp, zm = dev(y, z + 1, c), dev(y, z - 1, c)
    yp, ym = dev(y + 1, z, c), dev(y - 1, z, c)
    partner = dev(y, z, 1 - c)

    def rc(src, dst, ssem, rsem, sdev):
        return pltpu.make_async_remote_copy(
            src_ref=src, dst_ref=dst, send_sem=ssem, recv_sem=rsem,
            device_id={"seq": sdev, "mp": m}, device_id_type=MESH,
        )

    def rcx(src, dst, ssem, rsem, mdev):
        return pltpu.make_async_remote_copy(
            src_ref=src, dst_ref=dst, send_sem=ssem, recv_sem=rsem,
            device_id={"seq": s, "mp": mdev}, device_id_type=MESH,
        )

    kv_cols = pl.ds(pl.multiple_of(kvi * HEAD, HEAD), HEAD)
    own = gu.at[y, z, c]

    def group_of(index, *pairs):
        return [pltpu.make_async_copy(a, b, lsem.at[index + i]) for i, (a, b) in enumerate(pairs)]

    loads = {
        "up": group_of(0, (up_hbm, own.at[:, pl.ds(FFP, FFP)])),
        "gate": group_of(1, (gate_hbm, own.at[:, pl.ds(0, FFP)])),
        "hid": group_of(2, (hid_hbm, hid), (ag_hbm, ag_ref)),
        "kv": group_of(
            4, (kw_hbm.at[:, kv_cols], kvw.at[:, pl.ds(0, HEAD)]),
            (vw_hbm.at[:, kv_cols], kvw.at[:, pl.ds(HEAD, HEAD)]),
            (kb_hbm, kb_ref), (vb_hbm, vb_ref), (near_hbm, near_ref), (far_hbm, far_ref)),
        "q": group_of(10, (qw_hbm, qw), (qb_hbm, qb_ref)),
        "down": group_of(12, (down_hbm, down.at[y, z, c])),
        "hidq": group_of(
            13, (hid_hbm.at[:, pl.ds(pl.multiple_of(m * QUART, QUART), QUART)], hidq), (mg_hbm, mg_ref)),
        "ow": group_of(15, *((ow_hbm.at[:, pl.ds(q * QUART, QUART)], ow.at[q]) for q in range(MP))),
    }
    for copies in loads.values():
        for copy in copies:
            copy.start()

    def need(name):
        for copy in loads.pop(name, ()):
            copy.wait()

    bar = pltpu.get_barrier_semaphore()
    for peer in (zp, zm, yp, ym, partner):
        pl.semaphore_signal(bar, inc=1, device_id={"seq": peer, "mp": m}, device_id_type=MESH)
    for i in range(1, MP):
        pl.semaphore_signal(bar, inc=1, device_id={"seq": s, "mp": wrap(m + i, MP)}, device_id_type=MESH)
    pl.semaphore_wait(bar, 5 + MP - 1)

    ALL = slice(None)
    ZR, YR, HR, DR = 0, 4, 12, 20
    A_HALF = (TOK // 2, WR // 2, WR // 2)
    WGU, WDN = ("gate", "up"), ("down",)

    def a_ref(st, yy, zz, cc):
        if st == 0:
            return kv.at[0, yy, zz, cc]
        if st == 1:
            return gu.at[yy, zz, cc, :, pl.ds(0, GU_CUT)]
        return down.at[yy, zz, cc, :, pl.ds(0, DN_CUT)]

    def load_of(st):
        for name in ((), WGU, WDN)[st]:
            need(name)

    def block(st, yy, zz):
        return a_ref(st, wrap(yy, NY), wrap(zz, NZ), c)

    def half(st, ref, i):
        return ref.at[pl.ds(i * A_HALF[st], A_HALF[st])]

    def a_copy(ref, st, ssem, rsem, d):
        return rc(ref, ref, a_send.at[st, ssem], a_recv.at[st, rsem], d)

    def a_wait_recv(st, rsem, *size):
        a_copy(a_ref(st, *size), st, 0, rsem, partner).wait_recv()

    def zk_of(k):
        if isinstance(k, int):
            return z + Z_OFF[k]
        return z + jnp.where(lax.rem(k, 2) == 1, -((k + 1) // 2), k // 2)

    def z_copy(st, k_to, zz, right):
        return a_copy(block(st, y, zz), st, 0, ZR + (k_to - 1) // 2, zp if right else zm)

    def y_send(st, k):
        load_of(st)
        ref = block(st, y, zk_of(k))
        a_copy(ref, st, 1, YR + k, yp).start()
        a_copy(ref, st, 1, YR + k, ym).start()

    TWO = pl.ds(0, 2)

    def y_pass(st, k):
        zz = zk_of(k)
        a_wait_recv(st, YR + k, TWO, 0, 0)
        a_copy(half(st, block(st, y - 1, zz), 0), st, 1, HR + k, yp).start()
        a_copy(half(st, block(st, y + 1, zz), 1), st, 1, HR + k, ym).start()

    def d_index(st, k):
        return DR + (k, 0, max(0, (k - 1) // 2))[st]

    def y_last(st, k):
        a_wait_recv(st, HR + k, 0, 0, 0)
        a_copy(a_ref(st, ALL, wrap(zk_of(k), NZ), c), st, 1, d_index(st, k), partner).start()

    def z_start(st):
        load_of(st)
        z_copy(st, 1, z, True).start()
        z_copy(st, 2, z, False).start()

    def z_hop(st, h):
        far_right = FAR_RIGHT[st]
        a_wait_recv(st, ZR + h - 1, TWO if h < 4 else 0, 0, 0)
        for k in (2 * h - 1, 2 * h):
            if k >= NZ:
                continue
            right = far_right if k == 7 else k % 2 == 1
            if k + 2 < NZ - 1:
                z_copy(st, k + 2, zk_of(k), right).start()
            if k == (5 if far_right else 6):
                z_copy(st, 7, zk_of(k), far_right).start()
            if st == 0:
                y_send(st, k)

    BY, BH, BZ, BD = 0, 1, 2, 10
    B_HALF = (TOK // 4, WR // 2, WR // 2)
    mine = pl.multiple_of(lax.rem(m, 2) * (TOK // 2), TOK // 2)
    other = pl.multiple_of(TOK // 2 - mine, TOK // 2)

    def b_full(st, yy, zz, cc):
        if st == 0:
            return kv.at[1, yy, zz, cc]
        if st == 1:
            return gu.at[yy, zz, cc, :, pl.ds(GU_CUT, 2 * FFP - GU_CUT)]
        return down.at[yy, zz, cc, :, pl.ds(DN_CUT, FFP - DN_CUT)]

    def b_ref(st, yy, zz, cc):
        if st == 0:
            return kv.at[1, yy, zz, cc, pl.ds(mine, TOK // 2)]
        return b_full(st, yy, zz, cc)

    def b_copy(st, ref, ssem, rsem, d):
        return rc(ref, ref, b_send.at[st, ssem], b_recv.at[st, rsem], d)

    def b_wait_recv(st, rsem, *size):
        b_copy(st, b_ref(st, *size), 0, rsem, partner).wait_recv()

    def b_block(st, yy, w=None):
        ref = b_ref(st, wrap(yy, NY), z, c)
        return ref if w is None else ref.at[pl.ds(w * B_HALF[st], B_HALF[st])]

    def group(st, zz, w):
        rows = pl.ds(w * B_HALF[st], B_HALF[st])
        zz = wrap(zz, NZ)
        if st == 0:
            rows = pl.ds(pl.multiple_of(mine + w * B_HALF[st], B_HALF[st]), B_HALF[st])
            return kv.at[1, :, zz, c, rows]
        if st == 1:
            return gu.at[:, zz, c, rows, pl.ds(GU_CUT, 2 * FFP - GU_CUT)]
        return down.at[:, zz, c, rows, pl.ds(DN_CUT, FFP - DN_CUT)]

    def r_copy(st, i, w):
        return b_copy(st, group(st, z - (i - 1), w), 1, BZ + 2 * (i - 1) + w, zp)

    def l_copy(st, i, w):
        return b_copy(st, group(st, z + (i - 1), w), 1, BZ + 2 * (i - 1) + w, zm)

    def r_steps(w):
        return 4 if w == 0 else 3

    def l_steps(w):
        return 3 if w == 0 else 4

    def by_start(st):
        for name in ((), WGU[1:], WDN)[st]:
            need(name)
        b_copy(st, b_block(st, y), 0, BY, yp).start()
        b_copy(st, b_block(st, y), 0, BY, ym).start()

    def by_pass(st):
        b_wait_recv(st, BY, TWO, 0, 0)
        b_copy(st, b_block(st, y - 1, 0), 0, BH, yp).start()
        b_copy(st, b_block(st, y + 1, 1), 0, BH, ym).start()

    def b_all_wait(st, rsem, *size):
        ref = b_full(st, *size)
        rc(ref, ref, b_send.at[st, 2], b_recv.at[st, rsem], partner).wait_recv()

    def bd_start(st, k):
        b_copy(st, b_full(st, ALL, wrap(zk_of(k), NZ), c), 2,
               BD + (k, 0, max(0, (k - 1) // 2))[st], partner).start()

    pair = m + 1 - 2 * lax.rem(m, 2)

    def k_copy(ref, k):
        return rcx(ref, ref, k_send.at[min(k, 1)], k_recv.at[k], pair)

    def swap_start(k):
        zz = wrap(zk_of(k), NZ)
        rows = pl.ds(mine, TOK // 2)
        if k == 0:
            for i in range(1, NY):
                k_copy(kv.at[1, wrap(y + i, NY), zz, c, rows], k).start()
        else:
            k_copy(kv.at[1, :, zz, c, rows], k).start()

    def swap_last(k):
        some = kv.at[1, pl.ds(0, NY - 1) if k == 0 else ALL, 0, 0, pl.ds(0, TOK // 2)]
        k_copy(some, k).wait_recv()
        bd_start(0, k)

    def b_done(st, k):
        if st == 0:
            swap_start(k)
        else:
            bd_start(st, k)

    def by_last(st):
        b_wait_recv(st, BH, 0, 0, 0)
        b_done(st, 0)

    def bz_start(st):
        for w in range(2):
            r_copy(st, 1, w).start()
            l_copy(st, 1, w).start()

    def b_hop(st, h, w):
        b_wait_recv(st, BZ + 2 * (h - 1) + w, ALL if h < 4 else TWO, 0, 0)
        if h + 1 <= r_steps(w):
            r_copy(st, h + 1, w).start()
        if h + 1 <= l_steps(w):
            l_copy(st, h + 1, w).start()
        if w == 1:
            for k in (2 * h - 1, 2 * h):
                if k < NZ:
                    b_done(st, k)

    TASKS = {
        "zs": z_start, "zh": z_hop, "ys": y_send, "yp": y_pass, "yl": y_last,
        "bs": by_start, "bp": by_pass, "bl": by_last, "bz": bz_start, "bh": b_hop,
    }
    for name, *args in EARLY:
        TASKS[name](*args)

    need("hid")

    def norm_rows(i, _):
        r = pl.ds(pl.multiple_of(i * 16, 16), 16)
        x = hid[r, :].astype(F32)
        sq = x * x
        part = sq[:, 0:HEAD]
        for j in range(1, D // HEAD):
            part = part + sq[:, j * HEAD:(j + 1) * HEAD]
        innp[r, :] = part
        factor = lax.rsqrt(jnp.sum(part, axis=-1, keepdims=True) * (1.0 / D) + norm_eps)
        normed[r, :] = (x * factor * ag_ref[...]).astype(BF16)
        return 0

    lax.fori_loop(0, ROWS // 16, norm_rows, 0, unroll=4)

    need("kv")
    far_cos, far_sin = far_ref[0, pl.ds(s, 1), :], far_ref[1, pl.ds(s, 1), :]
    near_cos, near_sin = near_ref[0], near_ref[1]
    cos = near_cos * far_cos - near_sin * far_sin
    sin = near_sin * far_cos + near_cos * far_sin
    first = lax.broadcasted_iota(jnp.int32, sin.shape, 1) < HEAD // 2
    sin = jnp.where(first, -sin, sin)

    def rope(u):
        return u * cos + pltpu.roll(u, HEAD // 2, 1) * sin

    kv_all = jnp.dot(normed[...], kvw[...], preferred_element_type=F32)
    kb = kb_ref[pl.ds(kvi, 1), :]
    vb = vb_ref[pl.ds(kvi, 1), :]
    for sq in range(2):
        kk = kv_all[sq * TOK:(sq + 1) * TOK, 0:HEAD] + kb
        vv = kv_all[sq * TOK:(sq + 1) * TOK, HEAD:2 * HEAD] + vb
        kv[sq, y, z, c, :, 0:HEAD] = rope(kk).astype(BF16)
        kv[sq, y, z, c, :, HEAD:2 * HEAD] = vv.astype(BF16)

    need("q")
    q_all = jnp.dot(normed[...], qw[...], preferred_element_type=F32) + qb_ref[...]
    for sq in range(2):
        for h in range(OWN_HEADS):
            u = q_all[sq * TOK:(sq + 1) * TOK, h * HEAD:(h + 1) * HEAD]
            qbuf[sq, h * TOK:(h + 1) * TOK, :] = rope(u).astype(BF16)

    for sq in range(2):
        mbuf[sq] = jnp.full((OWN_HEADS * TOK, HEAD), masked_score, F32)
        accbuf[sq] = jnp.zeros((OWN_HEADS * TOK, 2 * HEAD), F32)

    def attend(sq, yks, zk, diagonal):
        pairs = [kv[sq, yk, zk] for yk in yks]
        kb_ = jnp.concatenate([p[:, :, 0:HEAD].reshape(2 * TOK, HEAD) for p in pairs], axis=0)
        vb_ = jnp.concatenate([p[:, :, HEAD:2 * HEAD].reshape(2 * TOK, HEAD) for p in pairs], axis=0)
        vb_ = jnp.concatenate([vb_, jnp.ones_like(vb_)], axis=1)
        sc = lax.dot_general(qbuf[sq], kb_, (((1,), (1,)), ((), ())), preferred_element_type=F32)
        if diagonal:
            row = lax.rem(lax.broadcasted_iota(jnp.int32, sc.shape, 0), TOK) + c * TOK
            col = lax.broadcasted_iota(jnp.int32, sc.shape, 1)
            sc = jnp.where(col <= row, sc, masked_score)
        m_old = mbuf[sq]
        m_new = jnp.maximum(m_old, jnp.max(sc, axis=1, keepdims=True))
        p = jnp.exp2((sc - jnp.concatenate([m_new] * (2 * len(yks)), axis=1)) * EXP2_SCALE)
        alpha = jnp.exp2((m_old - m_new) * EXP2_SCALE)
        mbuf[sq] = m_new
        accbuf[sq] = accbuf[sq] * jnp.concatenate([alpha, alpha], axis=1) + jnp.dot(p.astype(BF16), vb_, preferred_element_type=F32)

    def attend_round(sq, k):
        zk = wrap(zk_of(k), NZ)

        @pl.when(k == 0)
        def _():
            attend(sq, (y,), zk, True)

        n = y + jnp.where(zk < z, 1, 0)

        def step(i, _):
            attend(sq, (2 * i, 2 * i + 1), zk, False)
            return 0

        lax.fori_loop(0, n // 2, step, 0)

        @pl.when(lax.rem(n, 2) == 1)
        def _():
            attend(sq, (n - 1,), zk, False)

    def seq_rows(sq):
        return pl.ds(sq * TOK, TOK)

    right, left = wrap(m + 1, MP), wrap(m + MP - 1, MP)
    FROM_LEFT, FROM_RIGHT = 0, 1
    X_TR, X_RS, X_AG, X_AGH = range(4)

    def x_copy(src, dst, phase, sq, to):
        return rcx(src, dst, x_send.at[phase], x_recv.at[phase, sq], to)

    def x_wait(ref, phase, sq):
        x_copy(ref, ref, phase, sq, right).wait_recv()

    def o_project(sq):
        need("ow")
        for h in range(OWN_HEADS):
            r = slice(h * TOK, (h + 1) * TOK)
            attn[sq * TOK:(sq + 1) * TOK, h * HEAD:(h + 1) * HEAD] = (
                accbuf[sq, r, 0:HEAD] / accbuf[sq, r, HEAD:2 * HEAD]
            ).astype(BF16)
        here = attn[sq * TOK:(sq + 1) * TOK, :]
        for j in (2, 1, 3, 0):
            part = jnp.dot(here, ow[wrap(m + j, MP)], preferred_element_type=F32).astype(BF16)
            stage1[sq, j] = part
            if j == 1:
                for i, to in ((FROM_LEFT, right), (FROM_RIGHT, left)):
                    x_copy(stage1.at[sq, 2, pl.ds(i * (TOK // 2), TOK // 2)], tr1.at[sq, i], X_TR, sq, to).start()

    def rs1_mid(sq):
        x_wait(tr1.at[sq], X_TR, sq)
        for i, j, to in ((FROM_LEFT, 1, right), (FROM_RIGHT, 3, left)):
            r = slice(i * (TOK // 2), (i + 1) * (TOK // 2))
            both = stage1[sq, j, r, :].astype(F32) + tr1[sq, i].astype(F32)
            stage1[sq, j, r, :] = both.astype(BF16)
            x_copy(stage1.at[sq, j], rs1.at[i, seq_rows(sq)], X_RS, sq, to).start()

    def residual(sq):
        need("hidq")
        r = seq_rows(sq)
        x_wait(rs1.at[:, r], X_RS, sq)
        add = stage1[sq, 0].astype(F32) + rs1[0, r, :].astype(F32) + rs1[1, r, :].astype(F32)
        resid[m, r, :] = (hidq[r, :].astype(F32) + add).astype(BF16)
        for to in (right, left):
            x_copy(resid.at[m, r], resid.at[m, r], X_AG, sq, to).start()

    def ag_pass(sq):
        x_wait(resid.at[TWO, seq_rows(sq)], X_AG, sq)
        for i, src, to in ((0, left, right), (1, right, left)):
            ref = resid.at[src, pl.ds(sq * TOK + i * (TOK // 2), TOK // 2)]
            x_copy(ref, ref, X_AGH, sq, to).start()

    def second_norm(sq):
        x_wait(resid.at[0, seq_rows(sq)], X_AGH, sq)

        def norm2_rows(i, _):
            r = pl.ds(pl.multiple_of(sq * TOK + i * 16, 16), 16)
            xs = [resid[q, r, :].astype(F32) for q in range(MP)]
            part = None
            for x in xs:
                sqr = x * x
                for j in range(QUART // HEAD):
                    t = sqr[:, j * HEAD:(j + 1) * HEAD]
                    part = t if part is None else part + t
            factor = lax.rsqrt(jnp.sum(part, axis=-1, keepdims=True) * (1.0 / D) + norm_eps)
            for q in range(MP):
                cols = slice(q * QUART, (q + 1) * QUART)
                mlp_in[r, cols] = (xs[q] * factor * mg_ref[:, cols]).astype(BF16)
            return 0

        lax.fori_loop(0, TOK // 16, norm2_rows, 0, unroll=4)

    def gate_dot():
        a_wait_recv(1, DR, ALL, ALL, 0)
        rows = gu[:, :, :, :, 0:FFP].reshape(D, FFP)
        gbuf[...] = jnp.dot(mlp_in[...], rows, preferred_element_type=F32)

    def up_dot():
        b_wait_recv(1, BD, ALL, ALL, 0)
        rows = gu[:, :, :, :, FFP:2 * FFP].reshape(D, FFP)
        up_sum = jnp.dot(mlp_in[...], rows, preferred_element_type=F32)
        g = gbuf[...]
        act[...] = (g / (1.0 + jnp.exp(-g)) * up_sum).astype(BF16)

    odd = lax.rem(z, 2)

    def z_pair(i):
        turn = (0, 2 * odd - 1, 1 - 2 * odd, 2)[i]
        return wrap(z // 2 + turn, NZ // 2)

    def r_copy2(src, dst, ssem, rsem, to):
        return rcx(src, dst, r_send.at[ssem], r_recv.at[rsem], to)

    def down_stage(i):
        rounds = pl.ds(0, (3, 2, 2, 1)[i])
        a_wait_recv(2, DR + i, ALL, rounds, 0)
        b_wait_recv(2, BD + i, ALL, rounds, 0)
        p = z_pair(i)
        for q0 in (0, 2):
            rows = down[q0:q0 + 2, pl.ds(2 * p, 2)].reshape(2 * HEAD, FFP)
            part = lax.dot_general(
                act[...], rows, (((1,), (1,)), ((), ())), preferred_element_type=F32
            ).astype(BF16)
            stage2[i, q0] = part[:, 0:HEAD]
            stage2[i, q0 + 1] = part[:, HEAD:2 * HEAD]
        far_q = wrap(m + 2, MP)
        for w, to in ((FROM_LEFT, right), (FROM_RIGHT, left)):
            r_copy2(stage2.at[i, far_q, pl.ds(w * TOK, TOK)], tr2.at[i, w], 0, i, to).start()

    def rs2_mid(i):
        r_copy2(tr2.at[i], tr2.at[i], 0, i, right).wait_recv()
        for w, q in ((FROM_LEFT, right), (FROM_RIGHT, left)):
            r = slice(w * TOK, (w + 1) * TOK)
            both_ = stage2[i, q, r, :].astype(F32) + tr2[i, w].astype(F32)
            stage2[i, q, r, :] = both_.astype(BF16)
            r_copy2(stage2.at[i, q], rs2.at[i, w], 1, 4 + i, q).start()

    def layer_stage(i, so_far):
        r_copy2(rs2.at[i], rs2.at[i], 1, 4 + i, right).wait_recv()
        cols = pl.ds(pl.multiple_of(z_pair(i) * HEAD, HEAD), HEAD)
        add = stage2[i, m].astype(F32) + rs2[i, 0].astype(F32) + rs2[i, 1].astype(F32)
        layer = (resid[m, :, cols].astype(F32) + add).astype(BF16)
        layer_v[:, cols] = layer
        wide = layer.astype(F32)
        cp, op = hidq[:, cols].astype(F32) * wide, wide * wide
        return (cp, op) if so_far is None else (so_far[0] + cp, so_far[1] + op)

    TASKS.update(
        op=o_project, rm=rs1_mid, re=residual, ap=ag_pass, sn=second_norm, xl=swap_last, dm=rs2_mid, gd=gate_dot, ud=up_dot, ds=down_stage,
    )
    items, before, after = [], [], []
    for name, *args in LATER:
        if name == "at":
            items.append(args)
            before.append(after)
            after = []
        else:
            after.append((TASKS[name], args))

    def run(events):
        for act_, args in events:
            act_(*args)

    def pick(t, values):
        total = 0
        for i, v in enumerate(values):
            if v:
                total = total + jnp.where(t == i, v, 0)
        return total

    def item(t, _):
        for i, events in enumerate(before):
            if events:
                pl.when(t == i)(lambda events=events: run(events))
        sq = pick(t, [e[0] for e in items])
        k = pick(t, [e[1] for e in items])

        @pl.when(sq == 0)
        def _():
            a_wait_recv(0, DR + k, ALL, 0, 0)

        @pl.when(sq == 1)
        def _():
            b_all_wait(0, BD + k, ALL, 0, 0)

        attend_round(sq, k)
        return 0

    lax.fori_loop(0, len(items), item, 0)
    run(after)

    seven = pl.ds(0, NZ - 1)
    for st in range(3):
        a_copy(a_ref(st, 0, seven, 0), st, 0, 0, partner).wait_send()
        a_copy(a_ref(st, ALL, seven, ALL), st, 1, 0, partner).wait_send()
        b_copy(st, b_ref(st, 0, pl.ds(0, 3), 0), 0, 0, partner).wait_send()
        b_copy(st, b_ref(st, ALL, seven, 0), 1, 0, partner).wait_send()
        b_copy(st, b_full(st, ALL, ALL, 0), 2, 0, partner).wait_send()
    x_copy(rs1.at[0], rs1.at[0], X_TR, 0, right).wait_send()
    x_copy(rs1, rs1, X_RS, 0, right).wait_send()
    x_copy(rs1, rs1, X_AG, 0, right).wait_send()
    x_copy(rs1.at[0], rs1.at[0], X_AGH, 0, right).wait_send()
    k_copy(kv.at[1, pl.ds(0, NY - 1), 0, 0, pl.ds(0, TOK // 2)], 0).wait_send()
    k_copy(kv.at[1, :, seven, 0, pl.ds(0, TOK // 2)], 1).wait_send()

    def lane_sums(part):
        return jnp.sum(part.T, axis=0, keepdims=True)

    in_norm = lane_sums(innp[...])

    so_far = None
    for i in range(4):
        so_far = layer_stage(i, so_far)
    out_copy = pltpu.make_async_copy(layer_v, out_hbm, osem.at[0])
    rowi = lax.broadcasted_iota(jnp.int32, (8, ROWS), 0)
    sums[m] = jnp.where(rowi == 0, lane_sums(so_far[0]), lane_sums(so_far[1]))

    def s_copy(j):
        return rcx(sums.at[m], sums.at[m], s_sem.at[0], s_sem.at[1], wrap(m + j, MP))

    for j in (2, 1, 3):
        s_copy(j).start()
    out_copy.start()
    came = sums.at[pl.ds(0, MP - 1)]
    rcx(came, came, s_sem.at[0], s_sem.at[1], wrap(m + 1, MP)).wait()
    both = sums[0] + sums[1] + sums[2] + sums[3]
    cross, out_norm = both[0:1, :], both[1:2, :]
    cosine = cross / jnp.sqrt((in_norm + norm_eps) * (out_norm + norm_eps))
    lane = lax.broadcasted_iota(jnp.int32, (1, ROWS), 1)
    pos = s * TOK + lax.rem(lane, TOK)
    limit = jnp.where(lane < TOK, len_ref[0], len_ref[1])
    influence = jnp.where(pos < limit, 1.0 - cosine, 0.0)
    infl_ref[0:1, :] = influence[:, 0:TOK]
    infl_ref[1:2, :] = influence[:, TOK:2 * TOK]
    t0 = jnp.sum(influence[:, 0:TOK], axis=1, keepdims=True)
    t1 = jnp.sum(influence[:, TOK:2 * TOK], axis=1, keepdims=True)
    lane = lax.broadcasted_iota(jnp.int32, (1, HEAD), 1)
    one = pl.ds(0, 1)
    tot[s, one, :] = jnp.where(lane < HEAD // 2, t0, t1)

    for dy in (2, 1, 3, 0):
        for dz in (4, 3, 5, 2, 6, 1, 7, 0):
            for cc in (c, 1 - c):
                if dy == 0 and dz == 0 and cc is c:
                    continue
                ref = tot.at[s, one]
                rc(ref, ref, t_sem.at[0], t_sem.at[1], dev(y + dy, z + dz, cc)).start()
    every = tot.at[pl.ds(0, NS - 1), one]
    rc(every, every, t_sem.at[0], t_sem.at[1], partner).wait()
    total = jnp.sum(tot[:, 0, :], axis=0, keepdims=True)
    tokens = jnp.where(lane < HEAD // 2, len_ref[0], len_ref[1]).astype(F32)
    score = total / tokens
    score_ref[0] = jnp.sum(jnp.where(lane == 0, score, 0.0))
    score_ref[1] = jnp.sum(jnp.where(lane == HEAD - 1, score, 0.0))

    r_copy2(tr2, tr2, 0, 0, right).wait_send()
    r_copy2(rs2, rs2, 1, 0, right).wait_send()
    out_copy.wait()


def finish_kernel(layer_hbm, infl_hbm, score_hbm, out_hbm, infl_out, score_out, buf, sem):
    into = pltpu.make_async_copy(layer_hbm, buf, sem.at[0])
    small = [
        pltpu.make_async_copy(infl_hbm, infl_out, sem.at[1]),
        pltpu.make_async_copy(score_hbm, score_out, sem.at[2]),
    ]
    into.start()
    for copy in small:
        copy.start()
    into.wait()
    out = pltpu.make_async_copy(buf, out_hbm, sem.at[3])
    out.start()
    for copy in small:
        copy.wait()
    out.wait()


def local(
    hidden_in, attn_gain, q_weight, q_bias, k_weight, k_bias, v_weight, v_bias, o_weight,
    mlp_gain, gate_weight, up_weight, down_weight, lengths,
):
    seqs_n, tok_n, width = hidden_in.shape
    near, far = rotation_tables()

    hbm = pl.BlockSpec(memory_space=pltpu.HBM)
    vmem = pl.BlockSpec(memory_space=pltpu.VMEM)
    smem = pl.BlockSpec(memory_space=pltpu.SMEM)
    dma = pltpu.SemaphoreType.DMA
    results = (
        jax.ShapeDtypeStruct((ROWS, QUART), BF16),
        jax.ShapeDtypeStruct((2, TOK), F32),
        jax.ShapeDtypeStruct((2,), F32),
    )
    layer_part, influence, score = pl.pallas_call(
        layer_kernel,
        out_shape=results,
        in_specs=[hbm] * 15 + [smem],
        out_specs=(hbm, vmem, smem),
        scratch_shapes=[
            pltpu.VMEM((ROWS, D), BF16),
            pltpu.VMEM((ROWS, QUART), BF16),
            pltpu.VMEM((ROWS, D), BF16),
            pltpu.VMEM((D, QCOLS), BF16),
            pltpu.VMEM((D, 2 * HEAD), BF16),
            pltpu.VMEM((MP, QCOLS, QUART), BF16),
            pltpu.VMEM((2, OWN_HEADS * TOK, HEAD), BF16),
            pltpu.VMEM((2, NY, NZ, 2, TOK, 2 * HEAD), BF16),
            pltpu.VMEM((NY, NZ, 2, WR, 2 * FFP), BF16),
            pltpu.VMEM((NY, NZ, 2, WR, FFP), BF16),
            pltpu.VMEM((2, OWN_HEADS * TOK, HEAD), F32),
            pltpu.VMEM((2, OWN_HEADS * TOK, 2 * HEAD), F32),
            pltpu.VMEM((ROWS, QCOLS), BF16),
            pltpu.VMEM((2, MP, TOK, QUART), BF16),
            pltpu.VMEM((2, 2, TOK // 2, QUART), BF16),
            pltpu.VMEM((2, ROWS, QUART), BF16),
            pltpu.VMEM((MP, ROWS, QUART), BF16),
            pltpu.VMEM((4, MP, ROWS, HEAD), BF16),
            pltpu.VMEM((4, 2, TOK, HEAD), BF16),
            pltpu.VMEM((4, 2, ROWS, HEAD), BF16),
            pltpu.VMEM((ROWS, D), BF16),
            pltpu.VMEM((ROWS, FFP), BF16),
            pltpu.VMEM((ROWS, HEAD), F32),
            pltpu.VMEM((MP, 8, ROWS), F32),
            pltpu.VMEM((NS, 8, HEAD), F32),
            pltpu.VMEM((ROWS, FFP), F32),
            pltpu.VMEM((ROWS, QUART), BF16),
            pltpu.VMEM((1, D), F32),
            pltpu.VMEM((1, D), F32),
            pltpu.VMEM((1, QCOLS), F32),
            pltpu.VMEM((KV_HEADS, HEAD), F32),
            pltpu.VMEM((KV_HEADS, HEAD), F32),
            pltpu.VMEM((2, TOK, HEAD), F32),
            pltpu.VMEM((2, NS, HEAD), F32),
            dma((19,)),
            dma((1,)),
            dma((3, 2)),
            dma((3, 28)),
            dma((3, 3)),
            dma((3, 18)),
            dma((2,)),
            dma((NZ,)),
            dma((4,)),
            dma((4, 2)),
            dma((2,)),
            dma((8,)),
            dma((2,)),
            dma((2,)),
        ],
        compiler_params=pltpu.CompilerParams(
            collective_id=0, has_side_effects=True, vmem_limit_bytes=62 * 1024 * 1024
        ),
        name="layer",
    )(
        hidden_in.reshape(ROWS, width), attn_gain.reshape(1, width), q_weight,
        q_bias.reshape(1, QCOLS), k_weight, k_bias.reshape(KV_HEADS, HEAD), v_weight,
        v_bias.reshape(KV_HEADS, HEAD), o_weight, mlp_gain.reshape(1, width), gate_weight,
        up_weight, down_weight, near, far, lengths,
    )
    layer_part, influence, score = pl.pallas_call(
        finish_kernel,
        out_shape=results,
        in_specs=[hbm, hbm, hbm],
        out_specs=(hbm, hbm, hbm),
        scratch_shapes=[pltpu.VMEM((ROWS, QUART), BF16), dma((4,))],
        name="finish",
    )(layer_part, influence, score)
    return layer_part.reshape(seqs_n, tok_n, QUART), influence, score


def solution(mesh):
    placed = (
        P(None, "seq", None), P(), P(None, "mp"), P("mp"), P(), P(), P(), P(),
        P("mp", None), P(), P("seq", "mp"), P("seq", "mp"), P("seq", "mp"), P(),
    )
    return jax.shard_map(
        local, mesh=mesh, in_specs=placed,
        out_specs=(P(None, "seq", "mp"), P(None, "seq"), P()), check_vma=False,
    )
```

```python
import jax
import jax.numpy as jnp
import numpy as np
from jax import lax
from jax.experimental import pallas as pl
from jax.experimental.pallas import tpu as pltpu
from jax.sharding import PartitionSpec as P

HEADS = 16
KV_HEADS = 2
HEAD = 128
D = 2048
NY, NZ = 4, 8
MP = 4
TOK = 128
ROWS = 2 * TOK
OWN_HEADS = HEADS // MP
QCOLS = OWN_HEADS * HEAD
QUART = D // MP
FFP = 1408
WR = 32
GU_CUT = 1792
DN_CUT = 640
NS = NY * NZ * 2

rope_base = 1000000.0
norm_eps = 1e-06
masked_score = -1e30
EXP2_SCALE = HEAD ** (-0.5) * 1.4426950408889634


def rotation_tables():
    freq = rope_base ** (-2.0 * np.arange(HEAD // 2) / HEAD)
    freq = np.concatenate([freq, freq])
    near = np.arange(TOK)[:, None] * freq
    far = TOK * np.arange(NS)[:, None] * freq
    return np.stack([np.cos(near), np.sin(near)]).astype(np.float32), np.stack(
        [np.cos(far), np.sin(far)]).astype(np.float32)


MESH = pl.DeviceIdType.MESH
F32, BF16 = jnp.float32, jnp.bfloat16

Z_OFF = (0, -1, 1, -2, 2, -3, 3, -4)

FAR_RIGHT = (True, False, True)

EARLY = (
    ("zs", 1), ("bs", 1), ("bs", 2),
)
LATER = (
    ("bs", 0), ("zs", 0), ("ys", 0, 0), ("qp",), ("bp", 1), ("zs", 2), ("zh", 1, 1), ("bp", 2), ("bp", 0),
    ("zh", 0, 1), ("yp", 0, 0), ("bl", 1), ("bl", 2), ("bl", 0), ("bz", 0), ("ys", 1, 0), ("yp", 0, 1),
    ("zh", 0, 2), ("yp", 0, 2), ("yl", 0, 0), ("bh", 0, 1, 0), ("xl", 0), ("bh", 0, 1, 1), ("at", 0, 0),
    ("zh", 1, 2), ("yp", 1, 0), ("zh", 0, 3), ("yl", 0, 1), ("at", 1, 0), ("bh", 0, 2, 0), ("yp", 0, 3),
    ("at", 0, 1), ("bh", 0, 2, 1), ("xl", 1), ("yp", 0, 4), ("yl", 0, 2), ("yl", 1, 0), ("at", 1, 1),
    ("xl", 2), ("yp", 0, 5), ("at", 0, 2), ("bz", 1), ("ys", 1, 1), ("zh", 0, 4), ("yp", 0, 6),
    ("bh", 0, 3, 0), ("yl", 0, 3), ("at", 1, 2), ("xl", 3), ("yl", 0, 4), ("bh", 0, 3, 1), ("yl", 0, 5),
    ("at", 0, 3), ("at", 1, 3), ("xl", 4), ("yp", 1, 1), ("bh", 1, 1, 0), ("at", 0, 4), ("ys", 1, 2),
    ("yp", 0, 7), ("at", 0, 5), ("xl", 5), ("yl", 0, 6), ("at", 1, 4), ("bh", 1, 1, 1), ("yl", 1, 1),
    ("ys", 1, 3), ("bh", 0, 4, 0), ("bh", 0, 4, 1), ("at", 1, 5), ("xl", 6), ("at", 0, 6), ("ys", 1, 4),
    ("yp", 1, 2), ("yl", 0, 7), ("bh", 1, 2, 0), ("at", 1, 6), ("xl", 7), ("bh", 1, 2, 1), ("yp", 1, 3),
    ("at", 0, 7), ("op", 0), ("yp", 1, 4), ("at", 1, 7), ("zh", 1, 3), ("ys", 1, 5), ("yl", 1, 2),
    ("bh", 1, 3, 0), ("op", 1), ("yl", 1, 3), ("rm", 0), ("yl", 1, 4), ("ys", 1, 6), ("bh", 1, 3, 1),
    ("rm", 1), ("yp", 1, 5), ("zh", 1, 4), ("zh", 2, 1), ("bh", 1, 4, 0), ("ys", 1, 7), ("bz", 2), ("re", 0),
    ("yp", 1, 6), ("bh", 1, 4, 1), ("yl", 1, 5), ("re", 1), ("ys", 2, 0), ("zh", 2, 2), ("ys", 2, 1),
    ("yp", 1, 7), ("bh", 2, 1, 0), ("yl", 1, 6), ("ap", 0), ("ys", 2, 2), ("yp", 2, 0), ("bh", 2, 1, 1),
    ("yp", 2, 1), ("ys", 2, 3), ("yl", 1, 7), ("ap", 1), ("ys", 2, 4), ("zh", 2, 3), ("yp", 2, 2),
    ("bh", 2, 2, 0), ("yl", 2, 0), ("sn", 0), ("ys", 2, 5), ("yl", 2, 1), ("yp", 2, 3), ("bh", 2, 2, 1),
    ("ys", 2, 6), ("sn", 1), ("zh", 2, 4), ("yp", 2, 4), ("gd",), ("ys", 2, 7), ("yl", 2, 2), ("yl", 2, 3),
    ("yp", 2, 5), ("bh", 2, 3, 0), ("ud",), ("yl", 2, 4), ("yp", 2, 6), ("bh", 2, 3, 1), ("ds", 0),
    ("yp", 2, 7), ("yl", 2, 5), ("ds", 1), ("bh", 2, 4, 0), ("yl", 2, 6), ("yl", 2, 7), ("dm", 0), ("ds", 2),
    ("bh", 2, 4, 1), ("dm", 1), ("ds", 3), ("dm", 2), ("dm", 3),
)


def layer_kernel(
    hid_hbm, ag_hbm, qw_hbm, qb_hbm, kw_hbm, kb_hbm, vw_hbm, vb_hbm, ow_hbm, mg_hbm,
    gate_hbm, up_hbm, down_hbm, near_hbm, far_hbm, len_ref,
    out_hbm, infl_ref, score_ref,
    hid, hidq, normed, qw, kvw, ow, qbuf, kv, gu, down, mbuf, lbuf, accbuf, attn,
    stage1, tr1, rs1, resid, stage2, tr2, rs2, mlp_in, act, innp, sums, tot, gbuf, layer_v,
    ag_ref, mg_ref, qb_ref, kb_ref, vb_ref, near_ref, far_ref,
    lsem, osem, a_send, a_recv, b_send, b_recv, k_send, k_recv, x_send, x_recv, r_send, r_recv,
    s_sem, t_sem,
):
    s = lax.axis_index("seq")
    m = lax.axis_index("mp")
    y = s // (2 * NZ)
    z = lax.rem(s // 2, NZ)
    c = lax.rem(s, 2)
    kvi = m // 2

    def wrap(v, n):
        return lax.rem(v + 2 * n, n)

    def dev(yy, zz, cc):
        return (wrap(yy, NY) * NZ + wrap(zz, NZ)) * 2 + cc

    zp, zm = dev(y, z + 1, c), dev(y, z - 1, c)
    yp, ym = dev(y + 1, z, c), dev(y - 1, z, c)
    partner = dev(y, z, 1 - c)

    def rc(src, dst, ssem, rsem, sdev):
        return pltpu.make_async_remote_copy(
            src_ref=src, dst_ref=dst, send_sem=ssem, recv_sem=rsem,
            device_id={"seq": sdev, "mp": m}, device_id_type=MESH,
        )

    def rcx(src, dst, ssem, rsem, mdev):
        return pltpu.make_async_remote_copy(
            src_ref=src, dst_ref=dst, send_sem=ssem, recv_sem=rsem,
            device_id={"seq": s, "mp": mdev}, device_id_type=MESH,
        )

    kv_cols = pl.ds(pl.multiple_of(kvi * HEAD, HEAD), HEAD)
    own = gu.at[y, z, c]
    ow_here = []

    def group_of(index, *pairs):
        return [pltpu.make_async_copy(a, b, lsem.at[index + i]) for i, (a, b) in enumerate(pairs)]

    loads = {
        "up": group_of(0, (up_hbm, own.at[:, pl.ds(FFP, FFP)])),
        "gate": group_of(1, (gate_hbm, own.at[:, pl.ds(0, FFP)])),
        "hid": group_of(2, (hid_hbm, hid), (ag_hbm, ag_ref)),
        "kv": group_of(
            4, (kw_hbm.at[:, kv_cols], kvw.at[:, pl.ds(0, HEAD)]),
            (vw_hbm.at[:, kv_cols], kvw.at[:, pl.ds(HEAD, HEAD)]),
            (kb_hbm, kb_ref), (vb_hbm, vb_ref), (near_hbm, near_ref), (far_hbm, far_ref)),
        "q": group_of(10, (qw_hbm, qw), (qb_hbm, qb_ref)),
        "down": group_of(12, (down_hbm, down.at[y, z, c])),
        "hidq": group_of(
            13, (hid_hbm.at[:, pl.ds(pl.multiple_of(m * QUART, QUART), QUART)], hidq), (mg_hbm, mg_ref)),
    }
    for copies in loads.values():
        for copy in copies:
            copy.start()

    for q in range(MP):
        pltpu.make_async_copy(ow_hbm.at[:, pl.ds(q * QUART, QUART)], ow.at[q], lsem.at[15]).start()

    def need(name):
        if name == "ow":
            if not ow_here:
                pltpu.make_async_copy(ow, ow, lsem.at[15]).wait()
                ow_here.append(True)
        for copy in loads.pop(name, ()):
            copy.wait()

    bar = pltpu.get_barrier_semaphore()
    for peer in (zp, zm, yp, ym, partner):
        pl.semaphore_signal(bar, inc=1, device_id={"seq": peer, "mp": m}, device_id_type=MESH)
    for i in range(1, MP):
        pl.semaphore_signal(bar, inc=1, device_id={"seq": s, "mp": wrap(m + i, MP)}, device_id_type=MESH)
    pl.semaphore_wait(bar, 5 + MP - 1)

    ALL = slice(None)
    ZR, YR, HR, DR = 0, 4, 12, 20
    A_HALF = (TOK // 2, WR // 2, WR // 2)
    WGU, WDN = ("gate", "up"), ("down",)

    def a_ref(st, yy, zz, cc):
        if st == 0:
            return kv.at[0, yy, zz, cc]
        if st == 1:
            return gu.at[yy, zz, cc, :, pl.ds(0, GU_CUT)]
        return down.at[yy, zz, cc, :, pl.ds(0, DN_CUT)]

    def load_of(st):
        for name in ((), WGU, WDN)[st]:
            need(name)

    def block(st, yy, zz):
        return a_ref(st, wrap(yy, NY), wrap(zz, NZ), c)

    def half(st, ref, i):
        return ref.at[pl.ds(i * A_HALF[st], A_HALF[st])]

    def a_copy(ref, st, ssem, rsem, d):
        return rc(ref, ref, a_send.at[st, ssem], a_recv.at[(0, 28, 49)[st] + rsem], d)

    def a_wait_recv(st, rsem, *size):
        a_copy(a_ref(st, *size), st, 0, rsem, partner).wait_recv()

    def zk_of(k):
        if isinstance(k, int):
            return z + Z_OFF[k]
        return z + jnp.where(lax.rem(k, 2) == 1, -((k + 1) // 2), k // 2)

    def z_copy(st, k_to, zz, right):
        return a_copy(block(st, y, zz), st, 0, ZR + (k_to - 1) // 2, zp if right else zm)

    def y_send(st, k):
        load_of(st)
        ref = block(st, y, zk_of(k))
        a_copy(ref, st, 1, YR + k, yp).start()
        a_copy(ref, st, 1, YR + k, ym).start()

    TWO = pl.ds(0, 2)

    def y_pass(st, k):
        zz = zk_of(k)
        a_wait_recv(st, YR + k, TWO, 0, 0)
        a_copy(half(st, block(st, y - 1, zz), 0), st, 1, HR + k, yp).start()
        a_copy(half(st, block(st, y + 1, zz), 1), st, 1, HR + k, ym).start()

    def d_index(st, k):
        return DR + (k, 0, max(0, (k - 1) // 2))[st]

    def y_last(st, k):
        a_wait_recv(st, HR + k, 0, 0, 0)
        a_copy(a_ref(st, ALL, wrap(zk_of(k), NZ), c), st, 1, d_index(st, k), partner).start()

    def z_start(st):
        load_of(st)
        z_copy(st, 1, z, True).start()
        z_copy(st, 2, z, False).start()

    def z_hop(st, h):
        far_right = FAR_RIGHT[st]
        a_wait_recv(st, ZR + h - 1, TWO if h < 4 else 0, 0, 0)
        for k in (2 * h - 1, 2 * h):
            if k >= NZ:
                continue
            right = far_right if k == 7 else k % 2 == 1
            if k + 2 < NZ - 1:
                z_copy(st, k + 2, zk_of(k), right).start()
            if k == (5 if far_right else 6):
                z_copy(st, 7, zk_of(k), far_right).start()
            if st == 0:
                y_send(st, k)

    BY, BH, BZ, BD = 0, 1, 2, 10
    B_HALF = (TOK // 4, WR // 2, WR // 2)
    mine = pl.multiple_of(lax.rem(m, 2) * (TOK // 2), TOK // 2)
    other = pl.multiple_of(TOK // 2 - mine, TOK // 2)

    def b_full(st, yy, zz, cc):
        if st == 0:
            return kv.at[1, yy, zz, cc]
        if st == 1:
            return gu.at[yy, zz, cc, :, pl.ds(GU_CUT, 2 * FFP - GU_CUT)]
        return down.at[yy, zz, cc, :, pl.ds(DN_CUT, FFP - DN_CUT)]

    def b_ref(st, yy, zz, cc):
        if st == 0:
            return kv.at[1, yy, zz, cc, pl.ds(mine, TOK // 2)]
        return b_full(st, yy, zz, cc)

    def b_copy(st, ref, ssem, rsem, d):
        return rc(ref, ref, b_send.at[st, ssem], b_recv.at[(0, 18, 29)[st] + rsem], d)

    def b_wait_recv(st, rsem, *size):
        b_copy(st, b_ref(st, *size), 0, rsem, partner).wait_recv()

    def b_block(st, yy, w=None):
        ref = b_ref(st, wrap(yy, NY), z, c)
        return ref if w is None else ref.at[pl.ds(w * B_HALF[st], B_HALF[st])]

    def group(st, zz, w):
        rows = pl.ds(w * B_HALF[st], B_HALF[st])
        zz = wrap(zz, NZ)
        if st == 0:
            rows = pl.ds(pl.multiple_of(mine + w * B_HALF[st], B_HALF[st]), B_HALF[st])
            return kv.at[1, :, zz, c, rows]
        if st == 1:
            return gu.at[:, zz, c, rows, pl.ds(GU_CUT, 2 * FFP - GU_CUT)]
        return down.at[:, zz, c, rows, pl.ds(DN_CUT, FFP - DN_CUT)]

    def r_copy(st, i, w):
        return b_copy(st, group(st, z - (i - 1), w), 1, BZ + 2 * (i - 1) + w, zp)

    def l_copy(st, i, w):
        return b_copy(st, group(st, z + (i - 1), w), 1, BZ + 2 * (i - 1) + w, zm)

    def r_steps(w):
        return 4 if w == 0 else 3

    def l_steps(w):
        return 3 if w == 0 else 4

    def by_start(st):
        for name in ((), WGU[1:], WDN)[st]:
            need(name)
        b_copy(st, b_block(st, y), 0, BY, yp).start()
        b_copy(st, b_block(st, y), 0, BY, ym).start()

    def by_pass(st):
        b_wait_recv(st, BY, TWO, 0, 0)
        b_copy(st, b_block(st, y - 1, 0), 0, BH, yp).start()
        b_copy(st, b_block(st, y + 1, 1), 0, BH, ym).start()

    def b_all_wait(st, rsem, *size):
        ref = b_full(st, *size)
        rc(ref, ref, b_send.at[st, 2], b_recv.at[(0, 18, 29)[st] + rsem], partner).wait_recv()

    def bd_start(st, k):
        b_copy(st, b_full(st, ALL, wrap(zk_of(k), NZ), c), 2,
               BD + (k, 0, max(0, (k - 1) // 2))[st], partner).start()

    pair = m + 1 - 2 * lax.rem(m, 2)

    def k_copy(ref, k):
        return rcx(ref, ref, k_send.at[min(k, 1)], k_recv.at[k], pair)

    def swap_start(k):
        zz = wrap(zk_of(k), NZ)
        rows = pl.ds(mine, TOK // 2)
        if k == 0:
            for i in range(1, NY):
                k_copy(kv.at[1, wrap(y + i, NY), zz, c, rows], k).start()
        else:
            k_copy(kv.at[1, :, zz, c, rows], k).start()

    def swap_last(k):
        some = kv.at[1, pl.ds(0, NY - 1) if k == 0 else ALL, 0, 0, pl.ds(0, TOK // 2)]
        k_copy(some, k).wait_recv()
        bd_start(0, k)

    def b_done(st, k):
        if st == 0:
            swap_start(k)
        else:
            bd_start(st, k)

    def by_last(st):
        b_wait_recv(st, BH, 0, 0, 0)
        b_done(st, 0)

    def bz_start(st):
        for w in range(2):
            r_copy(st, 1, w).start()
            l_copy(st, 1, w).start()

    def b_hop(st, h, w):
        b_wait_recv(st, BZ + 2 * (h - 1) + w, ALL if h < 4 else TWO, 0, 0)
        if h + 1 <= r_steps(w):
            r_copy(st, h + 1, w).start()
        if h + 1 <= l_steps(w):
            l_copy(st, h + 1, w).start()
        if w == 1:
            for k in (2 * h - 1, 2 * h):
                if k < NZ:
                    b_done(st, k)

    TASKS = {
        "zs": z_start, "zh": z_hop, "ys": y_send, "yp": y_pass, "yl": y_last,
        "bs": by_start, "bp": by_pass, "bl": by_last, "bz": bz_start, "bh": b_hop,
    }
    for name, *args in EARLY:
        TASKS[name](*args)

    need("hid")

    def norm_rows(i, _):
        r = pl.ds(pl.multiple_of(i * 16, 16), 16)
        x = hid[r, :].astype(F32)
        sq = x * x
        part = sq[:, 0:HEAD]
        for j in range(1, D // HEAD):
            part = part + sq[:, j * HEAD:(j + 1) * HEAD]
        innp[r, :] = part
        factor = lax.rsqrt(jnp.sum(part, axis=-1, keepdims=True) * (1.0 / D) + norm_eps)
        normed[r, :] = (x * factor * ag_ref[...]).astype(BF16)
        return 0

    lax.fori_loop(0, ROWS // 16, norm_rows, 0, unroll=4)

    need("kv")
    far_cos, far_sin = far_ref[0, pl.ds(s, 1), :], far_ref[1, pl.ds(s, 1), :]
    near_cos, near_sin = near_ref[0], near_ref[1]
    cos = near_cos * far_cos - near_sin * far_sin
    sin = near_sin * far_cos + near_cos * far_sin
    first = lax.broadcasted_iota(jnp.int32, sin.shape, 1) < HEAD // 2
    sin = jnp.where(first, -sin, sin)

    def rope(u):
        return u * cos + pltpu.roll(u, HEAD // 2, 1) * sin

    kv_all = jnp.dot(normed[...], kvw[...], preferred_element_type=F32)
    kb = kb_ref[pl.ds(kvi, 1), :]
    vb = vb_ref[pl.ds(kvi, 1), :]
    for sq in range(2):
        kk = kv_all[sq * TOK:(sq + 1) * TOK, 0:HEAD] + kb
        vv = kv_all[sq * TOK:(sq + 1) * TOK, HEAD:2 * HEAD] + vb
        kv[sq, y, z, c, :, 0:HEAD] = rope(kk).astype(BF16)
        kv[sq, y, z, c, :, HEAD:2 * HEAD] = vv.astype(BF16)

    for sq in range(2):
        mbuf[sq] = jnp.full((OWN_HEADS * TOK, HEAD), masked_score, F32)
        lbuf[sq] = jnp.zeros((OWN_HEADS * TOK, HEAD), F32)
        accbuf[sq] = jnp.zeros((OWN_HEADS * TOK, HEAD), F32)

    def queries():
        need("q")
        q_all = jnp.dot(normed[...], qw[...], preferred_element_type=F32) + qb_ref[...]
        for sq in range(2):
            for h in range(OWN_HEADS):
                u = q_all[sq * TOK:(sq + 1) * TOK, h * HEAD:(h + 1) * HEAD]
                qbuf[sq, h * TOK:(h + 1) * TOK, :] = rope(u).astype(BF16)

    def attend(sq, yks, zk, diagonal):
        pairs = [kv[sq, yk, zk] for yk in yks]
        kb_ = jnp.concatenate([p[:, :, 0:HEAD].reshape(2 * TOK, HEAD) for p in pairs], axis=0)
        vb_ = jnp.concatenate([p[:, :, HEAD:2 * HEAD].reshape(2 * TOK, HEAD) for p in pairs], axis=0)
        sc = lax.dot_general(qbuf[sq], kb_, (((1,), (1,)), ((), ())), preferred_element_type=F32)
        if diagonal:
            row = lax.rem(lax.broadcasted_iota(jnp.int32, sc.shape, 0), TOK) + c * TOK
            col = lax.broadcasted_iota(jnp.int32, sc.shape, 1)
            sc = jnp.where(col <= row, sc, masked_score)
        m_old = mbuf[sq]
        m_new = jnp.maximum(m_old, jnp.max(sc, axis=1, keepdims=True))
        p = jnp.exp2((sc - jnp.concatenate([m_new] * (2 * len(yks)), axis=1)) * EXP2_SCALE)
        alpha = jnp.exp2((m_old - m_new) * EXP2_SCALE)
        mbuf[sq] = m_new
        part = p[:, 0:HEAD]
        for i in range(1, 2 * len(yks)):
            part = part + p[:, i * HEAD:(i + 1) * HEAD]
        lbuf[sq] = lbuf[sq] * alpha + part
        accbuf[sq] = accbuf[sq] * alpha + jnp.dot(p.astype(BF16), vb_, preferred_element_type=F32)

    def attend_round(sq, k):
        zk = wrap(zk_of(k), NZ)

        @pl.when(k == 0)
        def _():
            attend(sq, (y,), zk, True)

        n = y + jnp.where(zk < z, 1, 0)

        for count in range(1, NY + 1):
            @pl.when(n == count)
            def _():
                attend(sq, tuple(range(count)), zk, False)

    def seq_rows(sq):
        return pl.ds(sq * TOK, TOK)

    right, left = wrap(m + 1, MP), wrap(m + MP - 1, MP)
    FROM_LEFT, FROM_RIGHT = 0, 1
    X_TR, X_RS, X_AG, X_AGH = range(4)

    def x_copy(src, dst, phase, sq, to):
        return rcx(src, dst, x_send.at[phase], x_recv.at[phase, sq], to)

    def x_wait(ref, phase, sq):
        x_copy(ref, ref, phase, sq, right).wait_recv()

    def o_project(sq):
        need("ow")
        for h in range(OWN_HEADS):
            r = slice(h * TOK, (h + 1) * TOK)
            attn[sq * TOK:(sq + 1) * TOK, h * HEAD:(h + 1) * HEAD] = (
                accbuf[sq, r, :] / jnp.sum(lbuf[sq, r, :], axis=1, keepdims=True)
            ).astype(BF16)
        here = attn[sq * TOK:(sq + 1) * TOK, :]
        for j in (2, 1, 3, 0):
            part = jnp.dot(here, ow[wrap(m + j, MP)], preferred_element_type=F32).astype(BF16)
            stage1[sq, j] = part
            if j == 1:
                for i, to in ((FROM_LEFT, right), (FROM_RIGHT, left)):
                    x_copy(stage1.at[sq, 2, pl.ds(i * (TOK // 2), TOK // 2)], tr1.at[sq, i], X_TR, sq, to).start()

    def rs1_mid(sq):
        x_wait(tr1.at[sq], X_TR, sq)
        for i, j, to in ((FROM_LEFT, 1, right), (FROM_RIGHT, 3, left)):
            r = slice(i * (TOK // 2), (i + 1) * (TOK // 2))
            both = stage1[sq, j, r, :].astype(F32) + tr1[sq, i].astype(F32)
            stage1[sq, j, r, :] = both.astype(BF16)
            x_copy(stage1.at[sq, j], rs1.at[i, seq_rows(sq)], X_RS, sq, to).start()

    def residual(sq):
        need("hidq")
        r = seq_rows(sq)
        x_wait(rs1.at[:, r], X_RS, sq)
        add = stage1[sq, 0].astype(F32) + rs1[0, r, :].astype(F32) + rs1[1, r, :].astype(F32)
        resid[m, r, :] = (hidq[r, :].astype(F32) + add).astype(BF16)
        for to in (right, left):
            x_copy(resid.at[m, r], resid.at[m, r], X_AG, sq, to).start()

    def ag_pass(sq):
        x_wait(resid.at[TWO, seq_rows(sq)], X_AG, sq)
        for i, src, to in ((0, left, right), (1, right, left)):
            ref = resid.at[src, pl.ds(sq * TOK + i * (TOK // 2), TOK // 2)]
            x_copy(ref, ref, X_AGH, sq, to).start()

    def second_norm(sq):
        x_wait(resid.at[0, seq_rows(sq)], X_AGH, sq)

        def norm2_rows(i, _):
            r = pl.ds(pl.multiple_of(sq * TOK + i * 16, 16), 16)
            xs = [resid[q, r, :].astype(F32) for q in range(MP)]
            part = None
            for x in xs:
                sqr = x * x
                for j in range(QUART // HEAD):
                    t = sqr[:, j * HEAD:(j + 1) * HEAD]
                    part = t if part is None else part + t
            factor = lax.rsqrt(jnp.sum(part, axis=-1, keepdims=True) * (1.0 / D) + norm_eps)
            for q in range(MP):
                cols = slice(q * QUART, (q + 1) * QUART)
                mlp_in[r, cols] = (xs[q] * factor * mg_ref[:, cols]).astype(BF16)
            return 0

        lax.fori_loop(0, TOK // 16, norm2_rows, 0, unroll=4)

    def gate_dot():
        a_wait_recv(1, DR, ALL, ALL, 0)
        rows = gu[:, :, :, :, 0:FFP].reshape(D, FFP)
        gbuf[...] = jnp.dot(mlp_in[...], rows, preferred_element_type=F32)

    def up_dot():
        b_wait_recv(1, BD, ALL, ALL, 0)
        rows = gu[:, :, :, :, FFP:2 * FFP].reshape(D, FFP)
        up_sum = jnp.dot(mlp_in[...], rows, preferred_element_type=F32)
        g = gbuf[...]
        act[...] = (g / (1.0 + jnp.exp(-g)) * up_sum).astype(BF16)

    odd = lax.rem(z, 2)

    def z_pair(i):
        turn = (0, 2 * odd - 1, 1 - 2 * odd, 2)[i]
        return wrap(z // 2 + turn, NZ // 2)

    def r_copy2(src, dst, ssem, rsem, to):
        return rcx(src, dst, r_send.at[ssem], r_recv.at[rsem], to)

    def down_stage(i):
        rounds = pl.ds(0, (3, 2, 2, 1)[i])
        a_wait_recv(2, DR + i, ALL, rounds, 0)
        b_wait_recv(2, BD + i, ALL, rounds, 0)
        p = z_pair(i)
        for q0 in (0, 2):
            rows = down[q0:q0 + 2, pl.ds(2 * p, 2)].reshape(2 * HEAD, FFP)
            part = lax.dot_general(
                act[...], rows, (((1,), (1,)), ((), ())), preferred_element_type=F32
            ).astype(BF16)
            stage2[i, q0] = part[:, 0:HEAD]
            stage2[i, q0 + 1] = part[:, HEAD:2 * HEAD]
        far_q = wrap(m + 2, MP)
        for w, to in ((FROM_LEFT, right), (FROM_RIGHT, left)):
            r_copy2(stage2.at[i, far_q, pl.ds(w * TOK, TOK)], tr2.at[i, w], 0, i, to).start()

    def rs2_mid(i):
        r_copy2(tr2.at[i], tr2.at[i], 0, i, right).wait_recv()
        for w, q in ((FROM_LEFT, right), (FROM_RIGHT, left)):
            r = slice(w * TOK, (w + 1) * TOK)
            both_ = stage2[i, q, r, :].astype(F32) + tr2[i, w].astype(F32)
            stage2[i, q, r, :] = both_.astype(BF16)
            r_copy2(stage2.at[i, q], rs2.at[i, w], 1, 4 + i, q).start()

    def layer_stage(i, so_far):
        r_copy2(rs2.at[i], rs2.at[i], 1, 4 + i, right).wait_recv()
        cols = pl.ds(pl.multiple_of(z_pair(i) * HEAD, HEAD), HEAD)
        add = stage2[i, m].astype(F32) + rs2[i, 0].astype(F32) + rs2[i, 1].astype(F32)
        layer = (resid[m, :, cols].astype(F32) + add).astype(BF16)
        layer_v[:, cols] = layer
        wide = layer.astype(F32)
        cp, op = hidq[:, cols].astype(F32) * wide, wide * wide
        return (cp, op) if so_far is None else (so_far[0] + cp, so_far[1] + op)

    TASKS.update(
        qp=queries, op=o_project, rm=rs1_mid, re=residual, ap=ag_pass, sn=second_norm, xl=swap_last, dm=rs2_mid, gd=gate_dot, ud=up_dot, ds=down_stage,
    )
    items, before, after = [], [], []
    for name, *args in LATER:
        if name == "at":
            items.append(args)
            before.append(after)
            after = []
        else:
            after.append((TASKS[name], args))

    def run(events):
        for act_, args in events:
            act_(*args)

    def pick(t, values):
        total = 0
        for i, v in enumerate(values):
            if v:
                total = total + jnp.where(t == i, v, 0)
        return total

    def item(t, _):
        for i, events in enumerate(before):
            if events:
                pl.when(t == i)(lambda events=events: run(events))
        sq = pick(t, [e[0] for e in items])
        k = pick(t, [e[1] for e in items])

        @pl.when(sq == 0)
        def _():
            a_wait_recv(0, DR + k, ALL, 0, 0)

        @pl.when(sq == 1)
        def _():
            b_all_wait(0, BD + k, ALL, 0, 0)

        attend_round(sq, k)
        return 0

    lax.fori_loop(0, len(items), item, 0)
    run(after)

    seven = pl.ds(0, NZ - 1)
    for st in range(3):
        a_copy(a_ref(st, 0, seven, 0), st, 0, 0, partner).wait_send()
        a_copy(a_ref(st, ALL, seven, ALL), st, 1, 0, partner).wait_send()
        b_copy(st, b_ref(st, 0, pl.ds(0, 3), 0), 0, 0, partner).wait_send()
        b_copy(st, b_ref(st, ALL, seven, 0), 1, 0, partner).wait_send()
        b_copy(st, b_full(st, ALL, ALL, 0), 2, 0, partner).wait_send()
    x_copy(rs1.at[0], rs1.at[0], X_TR, 0, right).wait_send()
    x_copy(rs1, rs1, X_RS, 0, right).wait_send()
    x_copy(rs1, rs1, X_AG, 0, right).wait_send()
    x_copy(rs1.at[0], rs1.at[0], X_AGH, 0, right).wait_send()
    k_copy(kv.at[1, pl.ds(0, NY - 1), 0, 0, pl.ds(0, TOK // 2)], 0).wait_send()
    k_copy(kv.at[1, :, seven, 0, pl.ds(0, TOK // 2)], 1).wait_send()

    def lane_sums(part):
        return jnp.sum(part.T, axis=0, keepdims=True)

    in_norm = lane_sums(innp[...])

    so_far = None
    for i in range(4):
        so_far = layer_stage(i, so_far)
    out_copy = pltpu.make_async_copy(layer_v, out_hbm, osem.at[0])
    rowi = lax.broadcasted_iota(jnp.int32, (8, ROWS), 0)
    sums[m] = jnp.where(rowi == 0, lane_sums(so_far[0]), lane_sums(so_far[1]))

    def s_copy(j):
        return rcx(sums.at[m], sums.at[m], s_sem.at[0], s_sem.at[1], wrap(m + j, MP))

    for j in (2, 1, 3):
        s_copy(j).start()
    out_copy.start()
    came = sums.at[pl.ds(0, MP - 1)]
    rcx(came, came, s_sem.at[0], s_sem.at[1], wrap(m + 1, MP)).wait()
    both = sums[0] + sums[1] + sums[2] + sums[3]
    cross, out_norm = both[0:1, :], both[1:2, :]
    cosine = cross / jnp.sqrt((in_norm + norm_eps) * (out_norm + norm_eps))
    lane = lax.broadcasted_iota(jnp.int32, (1, ROWS), 1)
    pos = s * TOK + lax.rem(lane, TOK)
    limit = jnp.where(lane < TOK, len_ref[0], len_ref[1])
    influence = jnp.where(pos < limit, 1.0 - cosine, 0.0)
    infl_ref[0:1, :] = influence[:, 0:TOK]
    infl_ref[1:2, :] = influence[:, TOK:2 * TOK]
    t0 = jnp.sum(influence[:, 0:TOK], axis=1, keepdims=True)
    t1 = jnp.sum(influence[:, TOK:2 * TOK], axis=1, keepdims=True)
    lane = lax.broadcasted_iota(jnp.int32, (1, HEAD), 1)
    one = pl.ds(0, 1)
    tot[s, one, :] = jnp.where(lane < HEAD // 2, t0, t1)

    for dy in (2, 1, 3, 0):
        for dz in (4, 3, 5, 2, 6, 1, 7, 0):
            for cc in (c, 1 - c):
                if dy == 0 and dz == 0 and cc is c:
                    continue
                ref = tot.at[s, one]
                rc(ref, ref, t_sem.at[0], t_sem.at[1], dev(y + dy, z + dz, cc)).start()
    every = tot.at[pl.ds(0, NS - 1), one]
    rc(every, every, t_sem.at[0], t_sem.at[1], partner).wait()
    total = jnp.sum(tot[:, 0, :], axis=0, keepdims=True)
    tokens = jnp.where(lane < HEAD // 2, len_ref[0], len_ref[1]).astype(F32)
    score = total / tokens
    score_ref[0] = jnp.sum(jnp.where(lane == 0, score, 0.0))
    score_ref[1] = jnp.sum(jnp.where(lane == HEAD - 1, score, 0.0))

    r_copy2(tr2, tr2, 0, 0, right).wait_send()
    r_copy2(rs2, rs2, 1, 0, right).wait_send()
    out_copy.wait()


def finish_kernel(layer_hbm, infl_hbm, score_hbm, out_hbm, infl_out, score_out, buf, sem):
    into = pltpu.make_async_copy(layer_hbm, buf, sem.at[0])
    small = [
        pltpu.make_async_copy(infl_hbm, infl_out, sem.at[1]),
        pltpu.make_async_copy(score_hbm, score_out, sem.at[2]),
    ]
    into.start()
    for copy in small:
        copy.start()
    into.wait()
    out = pltpu.make_async_copy(buf, out_hbm, sem.at[3])
    out.start()
    for copy in small:
        copy.wait()
    out.wait()


def local(
    hidden_in, attn_gain, q_weight, q_bias, k_weight, k_bias, v_weight, v_bias, o_weight,
    mlp_gain, gate_weight, up_weight, down_weight, lengths,
):
    seqs_n, tok_n, width = hidden_in.shape
    near, far = rotation_tables()

    hbm = pl.BlockSpec(memory_space=pltpu.HBM)
    vmem = pl.BlockSpec(memory_space=pltpu.VMEM)
    smem = pl.BlockSpec(memory_space=pltpu.SMEM)
    dma = pltpu.SemaphoreType.DMA
    results = (
        jax.ShapeDtypeStruct((ROWS, QUART), BF16),
        jax.ShapeDtypeStruct((2, TOK), F32),
        jax.ShapeDtypeStruct((2,), F32),
    )
    layer_part, influence, score = pl.pallas_call(
        layer_kernel,
        out_shape=results,
        in_specs=[hbm] * 15 + [smem],
        out_specs=(hbm, vmem, smem),
        scratch_shapes=[
            pltpu.VMEM((ROWS, D), BF16),
            pltpu.VMEM((ROWS, QUART), BF16),
            pltpu.VMEM((ROWS, D), BF16),
            pltpu.VMEM((D, QCOLS), BF16),
            pltpu.VMEM((D, 2 * HEAD), BF16),
            pltpu.VMEM((MP, QCOLS, QUART), BF16),
            pltpu.VMEM((2, OWN_HEADS * TOK, HEAD), BF16),
            pltpu.VMEM((2, NY, NZ, 2, TOK, 2 * HEAD), BF16),
            pltpu.VMEM((NY, NZ, 2, WR, 2 * FFP), BF16),
            pltpu.VMEM((NY, NZ, 2, WR, FFP), BF16),
            pltpu.VMEM((2, OWN_HEADS * TOK, HEAD), F32),
            pltpu.VMEM((2, OWN_HEADS * TOK, HEAD), F32),
            pltpu.VMEM((2, OWN_HEADS * TOK, HEAD), F32),
            pltpu.VMEM((ROWS, QCOLS), BF16),
            pltpu.VMEM((2, MP, TOK, QUART), BF16),
            pltpu.VMEM((2, 2, TOK // 2, QUART), BF16),
            pltpu.VMEM((2, ROWS, QUART), BF16),
            pltpu.VMEM((MP, ROWS, QUART), BF16),
            pltpu.VMEM((4, MP, ROWS, HEAD), BF16),
            pltpu.VMEM((4, 2, TOK, HEAD), BF16),
            pltpu.VMEM((4, 2, ROWS, HEAD), BF16),
            pltpu.VMEM((ROWS, D), BF16),
            pltpu.VMEM((ROWS, FFP), BF16),
            pltpu.VMEM((ROWS, HEAD), F32),
            pltpu.VMEM((MP, 8, ROWS), F32),
            pltpu.VMEM((NS, 8, HEAD), F32),
            pltpu.VMEM((ROWS, FFP), F32),
            pltpu.VMEM((ROWS, QUART), BF16),
            pltpu.VMEM((1, D), F32),
            pltpu.VMEM((1, D), F32),
            pltpu.VMEM((1, QCOLS), F32),
            pltpu.VMEM((KV_HEADS, HEAD), F32),
            pltpu.VMEM((KV_HEADS, HEAD), F32),
            pltpu.VMEM((2, TOK, HEAD), F32),
            pltpu.VMEM((2, NS, HEAD), F32),
            dma((16,)),
            dma((1,)),
            dma((3, 2)),
            dma((73,)),
            dma((3, 3)),
            dma((43,)),
            dma((2,)),
            dma((NZ,)),
            dma((4,)),
            dma((4, 2)),
            dma((2,)),
            dma((8,)),
            dma((2,)),
            dma((2,)),
        ],
        compiler_params=pltpu.CompilerParams(
            collective_id=0, has_side_effects=True, vmem_limit_bytes=62 * 1024 * 1024
        ),
        name="layer",
    )(
        hidden_in.reshape(ROWS, width), attn_gain.reshape(1, width), q_weight,
        q_bias.reshape(1, QCOLS), k_weight, k_bias.reshape(KV_HEADS, HEAD), v_weight,
        v_bias.reshape(KV_HEADS, HEAD), o_weight, mlp_gain.reshape(1, width), gate_weight,
        up_weight, down_weight, near, far, lengths,
    )
    layer_part, influence, score = pl.pallas_call(
        finish_kernel,
        out_shape=results,
        in_specs=[hbm, hbm, hbm],
        out_specs=(hbm, hbm, hbm),
        scratch_shapes=[pltpu.VMEM((ROWS, QUART), BF16), dma((4,))],
        name="finish",
    )(layer_part, influence, score)
    return layer_part.reshape(seqs_n, tok_n, QUART), influence, score


def solution(mesh):
    placed = (
        P(None, "seq", None), P(), P(None, "mp"), P("mp"), P(), P(), P(), P(),
        P("mp", None), P(), P("seq", "mp"), P("seq", "mp"), P("seq", "mp"), P(),
    )
    return jax.shard_map(
        local, mesh=mesh, in_specs=placed,
        out_specs=(P(None, "seq", "mp"), P(None, "seq"), P()), check_vma=False,
    )
```

```python
import jax
import jax.numpy as jnp
import numpy as np
from jax import lax
from jax.experimental import pallas as pl
from jax.experimental.pallas import tpu as pltpu
from jax.sharding import PartitionSpec as P

HEADS = 16
KV_HEADS = 2
HEAD = 128
D = 2048
NY, NZ = 4, 8
MP = 4
TOK = 128
ROWS = 2 * TOK
OWN_HEADS = HEADS // MP
QCOLS = OWN_HEADS * HEAD
QUART = D // MP
FFP = 1408
WR = 32
GU_CUT = 1792
DN_CUT = 640
NS = NY * NZ * 2

rope_base = 1000000.0
norm_eps = 1e-06
masked_score = -1e30
EXP2_SCALE = HEAD ** (-0.5) * 1.4426950408889634


def rotation_tables():
    freq = rope_base ** (-2.0 * np.arange(HEAD // 2) / HEAD)
    freq = np.concatenate([freq, freq])
    near = np.arange(TOK)[:, None] * freq
    far = TOK * np.arange(NS)[:, None] * freq
    return np.stack([np.cos(near), np.sin(near)]).astype(np.float32), np.stack(
        [np.cos(far), np.sin(far)]).astype(np.float32)


MESH = pl.DeviceIdType.MESH
F32, BF16 = jnp.float32, jnp.bfloat16

Z_OFF = (0, -1, 1, -2, 2, -3, 3, -4)

FAR_RIGHT = (False, True, True)

EARLY = (
    ("zs", 1), ("bs", 1), ("bs", 2),
)
LATER = (
    ("bs", 0), ("qp",), ("zs", 2), ("zs", 0), ("ys", 0, 0), ("bp", 1), ("zh", 1, 1), ("bp", 2), ("bp", 0),
    ("ys", 1, 0), ("zh", 2, 1), ("yp", 0, 0), ("zh", 0, 1), ("bl", 1), ("bl", 2), ("bl", 0), ("bz", 0),
    ("yp", 1, 0), ("zh", 1, 2), ("yl", 0, 0), ("zh", 0, 2), ("xl", 0), ("yp", 0, 1), ("bh", 0, 1, 0),
    ("at", 0, 0), ("bh", 0, 1, 1), ("yp", 0, 2), ("at", 1, 0), ("yl", 1, 0), ("yp", 0, 3), ("ys", 1, 1),
    ("zh", 1, 3), ("yp", 0, 4), ("zh", 0, 3), ("yl", 0, 1), ("yl", 0, 2), ("bh", 0, 2, 0), ("xl", 1),
    ("yl", 0, 3), ("at", 0, 1), ("bh", 0, 2, 1), ("at", 0, 2), ("xl", 2), ("yp", 1, 1), ("at", 0, 3),
    ("bz", 1), ("zh", 1, 4), ("yl", 0, 4), ("zh", 0, 4), ("at", 1, 1), ("bh", 0, 3, 0), ("yp", 0, 5),
    ("at", 1, 2), ("bh", 0, 3, 1), ("at", 0, 4), ("yl", 1, 1), ("ys", 1, 2), ("xl", 3), ("yp", 0, 6),
    ("yp", 0, 7), ("bh", 1, 1, 0), ("yl", 0, 5), ("xl", 4), ("at", 1, 3), ("bh", 1, 1, 1), ("ys", 1, 3),
    ("at", 0, 5), ("xl", 5), ("yp", 1, 2), ("bh", 0, 4, 0), ("bh", 0, 4, 1), ("yl", 0, 6), ("at", 1, 4),
    ("yl", 0, 7), ("xl", 6), ("ys", 1, 4), ("at", 1, 5), ("bh", 1, 2, 0), ("at", 0, 6), ("yp", 1, 3),
    ("at", 0, 7), ("xl", 7), ("bh", 1, 2, 1), ("yl", 1, 2), ("ys", 1, 5), ("op", 0), ("at", 1, 6),
    ("yp", 1, 4), ("at", 1, 7), ("yl", 1, 3), ("zh", 2, 2), ("bh", 1, 3, 0), ("op", 1), ("ys", 1, 6),
    ("rm", 0), ("yp", 1, 5), ("bh", 1, 3, 1), ("yl", 1, 4), ("rm", 1), ("ys", 1, 7), ("bz", 2), ("yp", 1, 6),
    ("bh", 1, 4, 0), ("re", 0), ("yl", 1, 5), ("bh", 1, 4, 1), ("ys", 2, 0), ("zh", 2, 3), ("ys", 2, 1),
    ("yp", 1, 7), ("bh", 2, 1, 0), ("re", 1), ("yl", 1, 6), ("ys", 2, 2), ("yp", 2, 0), ("bh", 2, 1, 1),
    ("zh", 2, 4), ("yp", 2, 1), ("ap", 0), ("ys", 2, 3), ("yl", 1, 7), ("bh", 2, 2, 0), ("ys", 2, 4),
    ("yp", 2, 2), ("yl", 2, 0), ("ap", 1), ("ys", 2, 5), ("yl", 2, 1), ("bh", 2, 2, 1), ("ys", 2, 6),
    ("yp", 2, 3), ("sn", 0), ("yp", 2, 4), ("yl", 2, 2), ("ys", 2, 7), ("bh", 2, 3, 0), ("yp", 2, 5),
    ("sn", 1), ("gd",), ("yp", 2, 6), ("yl", 2, 3), ("yl", 2, 4), ("bh", 2, 3, 1), ("yp", 2, 7), ("ud",),
    ("yl", 2, 5), ("bh", 2, 4, 0), ("ds", 0), ("yl", 2, 6), ("ds", 1), ("yl", 2, 7), ("bh", 2, 4, 1),
    ("ds", 2), ("dm", 0), ("ds", 3), ("dm", 1), ("dm", 2), ("dm", 3),
)


def layer_kernel(
    hid_hbm, ag_hbm, qw_hbm, qb_hbm, kw_hbm, kb_hbm, vw_hbm, vb_hbm, ow_hbm, mg_hbm,
    gate_hbm, up_hbm, down_hbm, near_hbm, far_hbm, len_hbm,
    out_hbm, infl_ref, score_ref,
    hid, hidq, normed, qw, kvw, ow, qbuf, kv, gu, down, mbuf, lbuf, accbuf, attn,
    stage1, tr1, rs1, resid, stage2, tr2, rs2, mlp_in, act, innp, sums, tot, gbuf, layer_v,
    ag_ref, mg_ref, qb_ref, kb_ref, vb_ref, near_ref, far_ref, len_ref,
    lsem, osem, a_send, a_recv, b_send, b_recv, k_send, k_recv, x_send, x_recv, r_send, r_recv,
    s_sem, t_sem,
):
    s = lax.axis_index("seq")
    m = lax.axis_index("mp")
    y = s // (2 * NZ)
    z = lax.rem(s // 2, NZ)
    c = lax.rem(s, 2)
    kvi = m // 2

    def wrap(v, n):
        return lax.rem(v + 2 * n, n)

    def dev(yy, zz, cc):
        return (wrap(yy, NY) * NZ + wrap(zz, NZ)) * 2 + cc

    zp, zm = dev(y, z + 1, c), dev(y, z - 1, c)
    yp, ym = dev(y + 1, z, c), dev(y - 1, z, c)
    partner = dev(y, z, 1 - c)

    def rc(src, dst, ssem, rsem, sdev):
        return pltpu.make_async_remote_copy(
            src_ref=src, dst_ref=dst, send_sem=ssem, recv_sem=rsem,
            device_id={"seq": sdev, "mp": m}, device_id_type=MESH,
        )

    def rcx(src, dst, ssem, rsem, mdev):
        return pltpu.make_async_remote_copy(
            src_ref=src, dst_ref=dst, send_sem=ssem, recv_sem=rsem,
            device_id={"seq": s, "mp": mdev}, device_id_type=MESH,
        )

    bar = pltpu.get_barrier_semaphore()
    for peer in (zp, zm, yp, ym, partner):
        pl.semaphore_signal(bar, inc=1, device_id={"seq": peer, "mp": m}, device_id_type=MESH)
    for i in range(1, MP):
        pl.semaphore_signal(bar, inc=1, device_id={"seq": s, "mp": wrap(m + i, MP)}, device_id_type=MESH)

    kv_cols = pl.ds(pl.multiple_of(kvi * HEAD, HEAD), HEAD)
    own = gu.at[y, z, c]
    ow_here = []

    def group_of(index, *pairs):
        return [pltpu.make_async_copy(a, b, lsem.at[index + i]) for i, (a, b) in enumerate(pairs)]

    loads = {
        "up": group_of(0, (up_hbm, own.at[:, pl.ds(FFP, FFP)])),
        "gate": group_of(1, (gate_hbm, own.at[:, pl.ds(0, FFP)])),
        "hid": group_of(2, (hid_hbm, hid), (ag_hbm, ag_ref)),
        "kv": group_of(
            4, (kw_hbm.at[:, kv_cols], kvw.at[:, pl.ds(0, HEAD)]),
            (vw_hbm.at[:, kv_cols], kvw.at[:, pl.ds(HEAD, HEAD)]),
            (kb_hbm, kb_ref), (vb_hbm, vb_ref), (near_hbm, near_ref), (far_hbm, far_ref)),
        "q": group_of(10, (qw_hbm, qw), (qb_hbm, qb_ref)),
        "len": group_of(16, (len_hbm, len_ref)),
        "down": group_of(12, (down_hbm, down.at[y, z, c])),
        "hidq": group_of(
            13, (hid_hbm.at[:, pl.ds(pl.multiple_of(m * QUART, QUART), QUART)], hidq), (mg_hbm, mg_ref)),
    }
    for copies in loads.values():
        for copy in copies:
            copy.start()

    for q in range(MP):
        pltpu.make_async_copy(ow_hbm.at[:, pl.ds(q * QUART, QUART)], ow.at[q], lsem.at[15]).start()

    def need(name):
        if name == "ow":
            if not ow_here:
                pltpu.make_async_copy(ow, ow, lsem.at[15]).wait()
                ow_here.append(True)
        for copy in loads.pop(name, ()):
            copy.wait()

    pl.semaphore_wait(bar, 5 + MP - 1)

    ALL = slice(None)
    ZR, YR, HR, DR = 0, 4, 12, 20
    A_HALF = (TOK // 2, WR // 2, WR // 2)
    WGU, WDN = ("gate", "up"), ("down",)

    def a_ref(st, yy, zz, cc):
        if st == 0:
            return kv.at[0, yy, zz, cc]
        if st == 1:
            return gu.at[yy, zz, cc, :, pl.ds(0, GU_CUT)]
        return down.at[yy, zz, cc, :, pl.ds(0, DN_CUT)]

    def load_of(st):
        for name in ((), WGU, WDN)[st]:
            need(name)

    def block(st, yy, zz):
        return a_ref(st, wrap(yy, NY), wrap(zz, NZ), c)

    def half(st, ref, i):
        return ref.at[pl.ds(i * A_HALF[st], A_HALF[st])]

    def a_copy(ref, st, ssem, rsem, d):
        return rc(ref, ref, a_send.at[st, ssem], a_recv.at[(0, 28, 49)[st] + rsem], d)

    def a_wait_recv(st, rsem, *size):
        a_copy(a_ref(st, *size), st, 0, rsem, partner).wait_recv()

    def zk_of(k):
        if isinstance(k, int):
            return z + Z_OFF[k]
        return z + jnp.where(lax.rem(k, 2) == 1, -((k + 1) // 2), k // 2)

    def z_copy(st, k_to, zz, right):
        return a_copy(block(st, y, zz), st, 0, ZR + (k_to - 1) // 2, zp if right else zm)

    def y_send(st, k):
        load_of(st)
        ref = block(st, y, zk_of(k))
        a_copy(ref, st, 1, YR + k, yp).start()
        a_copy(ref, st, 1, YR + k, ym).start()

    TWO = pl.ds(0, 2)

    def y_pass(st, k):
        zz = zk_of(k)
        a_wait_recv(st, YR + k, TWO, 0, 0)
        a_copy(half(st, block(st, y - 1, zz), 0), st, 1, HR + k, yp).start()
        a_copy(half(st, block(st, y + 1, zz), 1), st, 1, HR + k, ym).start()

    def d_index(st, k):
        return DR + (k, 0, max(0, (k - 1) // 2))[st]

    def y_last(st, k):
        a_wait_recv(st, HR + k, 0, 0, 0)
        a_copy(a_ref(st, ALL, wrap(zk_of(k), NZ), c), st, 1, d_index(st, k), partner).start()

    def z_start(st):
        load_of(st)
        z_copy(st, 1, z, True).start()
        z_copy(st, 2, z, False).start()

    def z_hop(st, h):
        far_right = FAR_RIGHT[st]
        a_wait_recv(st, ZR + h - 1, TWO if h < 4 else 0, 0, 0)
        for k in (2 * h - 1, 2 * h):
            if k >= NZ:
                continue
            right = far_right if k == 7 else k % 2 == 1
            if k + 2 < NZ - 1:
                z_copy(st, k + 2, zk_of(k), right).start()
            if k == (5 if far_right else 6):
                z_copy(st, 7, zk_of(k), far_right).start()
            if st == 0:
                y_send(st, k)

    BY, BH, BZ, BD = 0, 1, 2, 10
    B_HALF = (TOK // 4, WR // 2, WR // 2)
    mine = pl.multiple_of(lax.rem(m, 2) * (TOK // 2), TOK // 2)
    other = pl.multiple_of(TOK // 2 - mine, TOK // 2)

    def b_full(st, yy, zz, cc):
        if st == 0:
            return kv.at[1, yy, zz, cc]
        if st == 1:
            return gu.at[yy, zz, cc, :, pl.ds(GU_CUT, 2 * FFP - GU_CUT)]
        return down.at[yy, zz, cc, :, pl.ds(DN_CUT, FFP - DN_CUT)]

    def b_ref(st, yy, zz, cc):
        if st == 0:
            return kv.at[1, yy, zz, cc, pl.ds(mine, TOK // 2)]
        return b_full(st, yy, zz, cc)

    def b_copy(st, ref, ssem, rsem, d):
        return rc(ref, ref, b_send.at[st, ssem], b_recv.at[(0, 18, 29)[st] + rsem], d)

    def b_wait_recv(st, rsem, *size):
        b_copy(st, b_ref(st, *size), 0, rsem, partner).wait_recv()

    def b_block(st, yy, w=None):
        ref = b_ref(st, wrap(yy, NY), z, c)
        return ref if w is None else ref.at[pl.ds(w * B_HALF[st], B_HALF[st])]

    def group(st, zz, w):
        rows = pl.ds(w * B_HALF[st], B_HALF[st])
        zz = wrap(zz, NZ)
        if st == 0:
            rows = pl.ds(pl.multiple_of(mine + w * B_HALF[st], B_HALF[st]), B_HALF[st])
            return kv.at[1, :, zz, c, rows]
        if st == 1:
            return gu.at[:, zz, c, rows, pl.ds(GU_CUT, 2 * FFP - GU_CUT)]
        return down.at[:, zz, c, rows, pl.ds(DN_CUT, FFP - DN_CUT)]

    def r_copy(st, i, w):
        return b_copy(st, group(st, z - (i - 1), w), 1, BZ + 2 * (i - 1) + w, zp)

    def l_copy(st, i, w):
        return b_copy(st, group(st, z + (i - 1), w), 1, BZ + 2 * (i - 1) + w, zm)

    def r_steps(w):
        return 4 if w == 0 else 3

    def l_steps(w):
        return 3 if w == 0 else 4

    def by_start(st):
        for name in ((), WGU[1:], WDN)[st]:
            need(name)
        b_copy(st, b_block(st, y), 0, BY, yp).start()
        b_copy(st, b_block(st, y), 0, BY, ym).start()

    def by_pass(st):
        b_wait_recv(st, BY, TWO, 0, 0)
        b_copy(st, b_block(st, y - 1, 0), 0, BH, yp).start()
        b_copy(st, b_block(st, y + 1, 1), 0, BH, ym).start()

    def b_all_wait(st, rsem, *size):
        ref = b_full(st, *size)
        rc(ref, ref, b_send.at[st, 2], b_recv.at[(0, 18, 29)[st] + rsem], partner).wait_recv()

    def bd_start(st, k):
        b_copy(st, b_full(st, ALL, wrap(zk_of(k), NZ), c), 2,
               BD + (k, 0, max(0, (k - 1) // 2))[st], partner).start()

    pair = m + 1 - 2 * lax.rem(m, 2)

    def k_copy(ref, k):
        return rcx(ref, ref, k_send.at[min(k, 1)], k_recv.at[k], pair)

    def swap_start(k):
        zz = wrap(zk_of(k), NZ)
        rows = pl.ds(mine, TOK // 2)
        if k == 0:
            for i in range(1, NY):
                k_copy(kv.at[1, wrap(y + i, NY), zz, c, rows], k).start()
        else:
            k_copy(kv.at[1, :, zz, c, rows], k).start()

    def swap_last(k):
        some = kv.at[1, pl.ds(0, NY - 1) if k == 0 else ALL, 0, 0, pl.ds(0, TOK // 2)]
        k_copy(some, k).wait_recv()
        bd_start(0, k)

    def b_done(st, k):
        if st == 0:
            swap_start(k)
        else:
            bd_start(st, k)

    def by_last(st):
        b_wait_recv(st, BH, 0, 0, 0)
        b_done(st, 0)

    def bz_start(st):
        for w in range(2):
            r_copy(st, 1, w).start()
            l_copy(st, 1, w).start()

    def b_hop(st, h, w):
        b_wait_recv(st, BZ + 2 * (h - 1) + w, ALL if h < 4 else TWO, 0, 0)
        if h + 1 <= r_steps(w):
            r_copy(st, h + 1, w).start()
        if h + 1 <= l_steps(w):
            l_copy(st, h + 1, w).start()
        if w == 1:
            for k in (2 * h - 1, 2 * h):
                if k < NZ:
                    b_done(st, k)

    TASKS = {
        "zs": z_start, "zh": z_hop, "ys": y_send, "yp": y_pass, "yl": y_last,
        "bs": by_start, "bp": by_pass, "bl": by_last, "bz": bz_start, "bh": b_hop,
    }
    for name, *args in EARLY:
        TASKS[name](*args)

    need("hid")

    def norm_rows(i, _):
        r = pl.ds(pl.multiple_of(i * 16, 16), 16)
        x = hid[r, :].astype(F32)
        sq = x * x
        part = sq[:, 0:HEAD]
        for j in range(1, D // HEAD):
            part = part + sq[:, j * HEAD:(j + 1) * HEAD]
        innp[r, :] = part
        factor = lax.rsqrt(jnp.sum(part, axis=-1, keepdims=True) * (1.0 / D) + norm_eps)
        normed[r, :] = (x * factor * ag_ref[...]).astype(BF16)
        return 0

    lax.fori_loop(0, ROWS // 16, norm_rows, 0, unroll=4)

    need("kv")
    far_cos, far_sin = far_ref[0, pl.ds(s, 1), :], far_ref[1, pl.ds(s, 1), :]
    near_cos, near_sin = near_ref[0], near_ref[1]
    cos = near_cos * far_cos - near_sin * far_sin
    sin = near_sin * far_cos + near_cos * far_sin
    first = lax.broadcasted_iota(jnp.int32, sin.shape, 1) < HEAD // 2
    sin = jnp.where(first, -sin, sin)

    def rope(u):
        return u * cos + pltpu.roll(u, HEAD // 2, 1) * sin

    kv_all = jnp.dot(normed[...], kvw[...], preferred_element_type=F32)
    kb = kb_ref[pl.ds(kvi, 1), :]
    vb = vb_ref[pl.ds(kvi, 1), :]
    for sq in range(2):
        kk = kv_all[sq * TOK:(sq + 1) * TOK, 0:HEAD] + kb
        vv = kv_all[sq * TOK:(sq + 1) * TOK, HEAD:2 * HEAD] + vb
        kv[sq, y, z, c, :, 0:HEAD] = rope(kk).astype(BF16)
        kv[sq, y, z, c, :, HEAD:2 * HEAD] = vv.astype(BF16)

    for sq in range(2):
        mbuf[sq] = jnp.full((OWN_HEADS * TOK, HEAD), masked_score, F32)
        lbuf[sq] = jnp.zeros((OWN_HEADS * TOK, HEAD), F32)
        accbuf[sq] = jnp.zeros((OWN_HEADS * TOK, HEAD), F32)

    def queries():
        need("q")
        q_all = jnp.dot(normed[...], qw[...], preferred_element_type=F32) + qb_ref[...]
        for sq in range(2):
            for h in range(OWN_HEADS):
                u = q_all[sq * TOK:(sq + 1) * TOK, h * HEAD:(h + 1) * HEAD]
                qbuf[sq, h * TOK:(h + 1) * TOK, :] = rope(u).astype(BF16)

    def attend(sq, yks, zk, diagonal):
        pairs = [kv[sq, yk, zk] for yk in yks]
        kb_ = jnp.concatenate([p[:, :, 0:HEAD].reshape(2 * TOK, HEAD) for p in pairs], axis=0)
        vb_ = jnp.concatenate([p[:, :, HEAD:2 * HEAD].reshape(2 * TOK, HEAD) for p in pairs], axis=0)
        sc = lax.dot_general(qbuf[sq], kb_, (((1,), (1,)), ((), ())), preferred_element_type=F32)
        if diagonal:
            row = lax.rem(lax.broadcasted_iota(jnp.int32, sc.shape, 0), TOK) + c * TOK
            col = lax.broadcasted_iota(jnp.int32, sc.shape, 1)
            sc = jnp.where(col <= row, sc, masked_score)
        m_old = mbuf[sq]
        m_new = jnp.maximum(m_old, jnp.max(sc, axis=1, keepdims=True))
        p = jnp.exp2((sc - jnp.concatenate([m_new] * (2 * len(yks)), axis=1)) * EXP2_SCALE)
        alpha = jnp.exp2((m_old - m_new) * EXP2_SCALE)
        mbuf[sq] = m_new
        part = p[:, 0:HEAD]
        for i in range(1, 2 * len(yks)):
            part = part + p[:, i * HEAD:(i + 1) * HEAD]
        lbuf[sq] = lbuf[sq] * alpha + part
        accbuf[sq] = accbuf[sq] * alpha + jnp.dot(p.astype(BF16), vb_, preferred_element_type=F32)

    def attend_round(sq, k):
        zk = wrap(zk_of(k), NZ)

        @pl.when(k == 0)
        def _():
            attend(sq, (y,), zk, True)

        n = y + jnp.where(zk < z, 1, 0)

        for count in range(1, NY + 1):
            @pl.when(n == count)
            def _():
                attend(sq, tuple(range(count)), zk, False)

    def seq_rows(sq):
        return pl.ds(sq * TOK, TOK)

    right, left = wrap(m + 1, MP), wrap(m + MP - 1, MP)
    FROM_LEFT, FROM_RIGHT = 0, 1
    X_TR, X_RS, X_AG, X_AGH = range(4)

    def x_copy(src, dst, phase, sq, to):
        return rcx(src, dst, x_send.at[phase], x_recv.at[phase, sq], to)

    def x_wait(ref, phase, sq):
        x_copy(ref, ref, phase, sq, right).wait_recv()

    def o_project(sq):
        need("ow")
        for h in range(OWN_HEADS):
            r = slice(h * TOK, (h + 1) * TOK)
            attn[sq * TOK:(sq + 1) * TOK, h * HEAD:(h + 1) * HEAD] = (
                accbuf[sq, r, :] / jnp.sum(lbuf[sq, r, :], axis=1, keepdims=True)
            ).astype(BF16)
        here = attn[sq * TOK:(sq + 1) * TOK, :]
        for j in (2, 1, 3, 0):
            part = jnp.dot(here, ow[wrap(m + j, MP)], preferred_element_type=F32).astype(BF16)
            stage1[sq, j] = part
            if j == 1:
                for i, to in ((FROM_LEFT, right), (FROM_RIGHT, left)):
                    x_copy(stage1.at[sq, 2, pl.ds(i * (TOK // 2), TOK // 2)], tr1.at[sq, i], X_TR, sq, to).start()

    def rs1_mid(sq):
        x_wait(tr1.at[sq], X_TR, sq)
        for i, j, to in ((FROM_LEFT, 1, right), (FROM_RIGHT, 3, left)):
            r = slice(i * (TOK // 2), (i + 1) * (TOK // 2))
            both = stage1[sq, j, r, :].astype(F32) + tr1[sq, i].astype(F32)
            stage1[sq, j, r, :] = both.astype(BF16)
            x_copy(stage1.at[sq, j], rs1.at[i, seq_rows(sq)], X_RS, sq, to).start()

    def residual(sq):
        need("hidq")
        r = seq_rows(sq)
        x_wait(rs1.at[:, r], X_RS, sq)
        add = stage1[sq, 0].astype(F32) + rs1[0, r, :].astype(F32) + rs1[1, r, :].astype(F32)
        resid[m, r, :] = (hidq[r, :].astype(F32) + add).astype(BF16)
        for to in (right, left):
            x_copy(resid.at[m, r], resid.at[m, r], X_AG, sq, to).start()

    def ag_pass(sq):
        x_wait(resid.at[TWO, seq_rows(sq)], X_AG, sq)
        for i, src, to in ((0, left, right), (1, right, left)):
            ref = resid.at[src, pl.ds(sq * TOK + i * (TOK // 2), TOK // 2)]
            x_copy(ref, ref, X_AGH, sq, to).start()

    def second_norm(sq):
        x_wait(resid.at[0, seq_rows(sq)], X_AGH, sq)

        def norm2_rows(i, _):
            r = pl.ds(pl.multiple_of(sq * TOK + i * 16, 16), 16)
            xs = [resid[q, r, :].astype(F32) for q in range(MP)]
            part = None
            for x in xs:
                sqr = x * x
                for j in range(QUART // HEAD):
                    t = sqr[:, j * HEAD:(j + 1) * HEAD]
                    part = t if part is None else part + t
            factor = lax.rsqrt(jnp.sum(part, axis=-1, keepdims=True) * (1.0 / D) + norm_eps)
            for q in range(MP):
                cols = slice(q * QUART, (q + 1) * QUART)
                mlp_in[r, cols] = (xs[q] * factor * mg_ref[:, cols]).astype(BF16)
            return 0

        lax.fori_loop(0, TOK // 16, norm2_rows, 0, unroll=4)

    def gate_dot():
        a_wait_recv(1, DR, ALL, ALL, 0)
        rows = gu[:, :, :, :, 0:FFP].reshape(D, FFP)
        gbuf[...] = jnp.dot(mlp_in[...], rows, preferred_element_type=F32)

    def up_dot():
        b_wait_recv(1, BD, ALL, ALL, 0)
        rows = gu[:, :, :, :, FFP:2 * FFP].reshape(D, FFP)
        up_sum = jnp.dot(mlp_in[...], rows, preferred_element_type=F32)
        g = gbuf[...]
        act[...] = (g / (1.0 + jnp.exp(-g)) * up_sum).astype(BF16)

    odd = lax.rem(z, 2)

    def z_pair(i):
        turn = (0, 2 * odd - 1, 1 - 2 * odd, 2)[i]
        return wrap(z // 2 + turn, NZ // 2)

    def r_copy2(src, dst, ssem, rsem, to):
        return rcx(src, dst, r_send.at[ssem], r_recv.at[rsem], to)

    def down_stage(i):
        rounds = pl.ds(0, (3, 2, 2, 1)[i])
        a_wait_recv(2, DR + i, ALL, rounds, 0)
        b_wait_recv(2, BD + i, ALL, rounds, 0)
        p = z_pair(i)
        for q0 in (0, 2):
            rows = down[q0:q0 + 2, pl.ds(2 * p, 2)].reshape(2 * HEAD, FFP)
            part = lax.dot_general(
                act[...], rows, (((1,), (1,)), ((), ())), preferred_element_type=F32
            ).astype(BF16)
            stage2[i, q0] = part[:, 0:HEAD]
            stage2[i, q0 + 1] = part[:, HEAD:2 * HEAD]
        far_q = wrap(m + 2, MP)
        for w, to in ((FROM_LEFT, right), (FROM_RIGHT, left)):
            r_copy2(stage2.at[i, far_q, pl.ds(w * TOK, TOK)], tr2.at[i, w], 0, i, to).start()

    def rs2_mid(i):
        r_copy2(tr2.at[i], tr2.at[i], 0, i, right).wait_recv()
        for w, q in ((FROM_LEFT, right), (FROM_RIGHT, left)):
            r = slice(w * TOK, (w + 1) * TOK)
            both_ = stage2[i, q, r, :].astype(F32) + tr2[i, w].astype(F32)
            stage2[i, q, r, :] = both_.astype(BF16)
            r_copy2(stage2.at[i, q], rs2.at[i, w], 1, 4 + i, q).start()

    def layer_stage(i, so_far):
        r_copy2(rs2.at[i], rs2.at[i], 1, 4 + i, right).wait_recv()
        cols = pl.ds(pl.multiple_of(z_pair(i) * HEAD, HEAD), HEAD)
        add = stage2[i, m].astype(F32) + rs2[i, 0].astype(F32) + rs2[i, 1].astype(F32)
        layer = (resid[m, :, cols].astype(F32) + add).astype(BF16)
        layer_v[:, cols] = layer
        wide = layer.astype(F32)
        cp, op = hidq[:, cols].astype(F32) * wide, wide * wide
        return (cp, op) if so_far is None else (so_far[0] + cp, so_far[1] + op)

    TASKS.update(
        qp=queries, op=o_project, rm=rs1_mid, re=residual, ap=ag_pass, sn=second_norm, xl=swap_last, dm=rs2_mid, gd=gate_dot, ud=up_dot, ds=down_stage,
    )
    items, before, after = [], [], []
    for name, *args in LATER:
        if name == "at":
            items.append(args)
            before.append(after)
            after = []
        else:
            after.append((TASKS[name], args))

    def run(events):
        for act_, args in events:
            act_(*args)

    def pick(t, values):
        total = 0
        for i, v in enumerate(values):
            if v:
                total = total + jnp.where(t == i, v, 0)
        return total

    def item(t, _):
        for i, events in enumerate(before):
            if events:
                pl.when(t == i)(lambda events=events: run(events))
        sq = pick(t, [e[0] for e in items])
        k = pick(t, [e[1] for e in items])

        @pl.when(sq == 0)
        def _():
            a_wait_recv(0, DR + k, ALL, 0, 0)

        @pl.when(sq == 1)
        def _():
            b_all_wait(0, BD + k, ALL, 0, 0)

        attend_round(sq, k)
        return 0

    lax.fori_loop(0, len(items), item, 0)
    run(after)

    seven = pl.ds(0, NZ - 1)
    for st in range(3):
        a_copy(a_ref(st, 0, seven, 0), st, 0, 0, partner).wait_send()
        a_copy(a_ref(st, ALL, seven, ALL), st, 1, 0, partner).wait_send()
        b_copy(st, b_ref(st, 0, pl.ds(0, 3), 0), 0, 0, partner).wait_send()
        b_copy(st, b_ref(st, ALL, seven, 0), 1, 0, partner).wait_send()
        b_copy(st, b_full(st, ALL, ALL, 0), 2, 0, partner).wait_send()
    x_copy(rs1.at[0], rs1.at[0], X_TR, 0, right).wait_send()
    x_copy(rs1, rs1, X_RS, 0, right).wait_send()
    x_copy(rs1, rs1, X_AG, 0, right).wait_send()
    x_copy(rs1.at[0], rs1.at[0], X_AGH, 0, right).wait_send()
    k_copy(kv.at[1, pl.ds(0, NY - 1), 0, 0, pl.ds(0, TOK // 2)], 0).wait_send()
    k_copy(kv.at[1, :, seven, 0, pl.ds(0, TOK // 2)], 1).wait_send()

    def lane_sums(part):
        return jnp.sum(part.T, axis=0, keepdims=True)

    need("len")
    in_norm = lane_sums(innp[...])

    so_far = None
    for i in range(4):
        so_far = layer_stage(i, so_far)
    out_copy = pltpu.make_async_copy(layer_v, out_hbm, osem.at[0])
    rowi = lax.broadcasted_iota(jnp.int32, (8, ROWS), 0)
    sums[m] = jnp.where(rowi == 0, lane_sums(so_far[0]), lane_sums(so_far[1]))

    def s_copy(j):
        return rcx(sums.at[m], sums.at[m], s_sem.at[0], s_sem.at[1], wrap(m + j, MP))

    for j in (2, 1, 3):
        s_copy(j).start()
    out_copy.start()
    came = sums.at[pl.ds(0, MP - 1)]
    rcx(came, came, s_sem.at[0], s_sem.at[1], wrap(m + 1, MP)).wait()
    both = sums[0] + sums[1] + sums[2] + sums[3]
    cross, out_norm = both[0:1, :], both[1:2, :]
    cosine = cross / jnp.sqrt((in_norm + norm_eps) * (out_norm + norm_eps))
    lane = lax.broadcasted_iota(jnp.int32, (1, ROWS), 1)
    pos = s * TOK + lax.rem(lane, TOK)
    limit = jnp.where(lane < TOK, len_ref[0], len_ref[1])
    influence = jnp.where(pos < limit, 1.0 - cosine, 0.0)
    infl_ref[0:1, :] = influence[:, 0:TOK]
    infl_ref[1:2, :] = influence[:, TOK:2 * TOK]
    t0 = jnp.sum(influence[:, 0:TOK], axis=1, keepdims=True)
    t1 = jnp.sum(influence[:, TOK:2 * TOK], axis=1, keepdims=True)
    lane = lax.broadcasted_iota(jnp.int32, (1, HEAD), 1)
    one = pl.ds(0, 1)
    tot[s, one, :] = jnp.where(lane < HEAD // 2, t0, t1)

    for dy in (2, 1, 3, 0):
        for dz in (4, 3, 5, 2, 6, 1, 7, 0):
            for cc in (c, 1 - c):
                if dy == 0 and dz == 0 and cc is c:
                    continue
                ref = tot.at[s, one]
                rc(ref, ref, t_sem.at[0], t_sem.at[1], dev(y + dy, z + dz, cc)).start()
    every = tot.at[pl.ds(0, NS - 1), one]
    rc(every, every, t_sem.at[0], t_sem.at[1], partner).wait()
    total = jnp.sum(tot[:, 0, :], axis=0, keepdims=True)
    tokens = jnp.where(lane < HEAD // 2, len_ref[0], len_ref[1]).astype(F32)
    score = total / tokens
    score_ref[0] = jnp.sum(jnp.where(lane == 0, score, 0.0))
    score_ref[1] = jnp.sum(jnp.where(lane == HEAD - 1, score, 0.0))

    r_copy2(tr2, tr2, 0, 0, right).wait_send()
    r_copy2(rs2, rs2, 1, 0, right).wait_send()
    out_copy.wait()


def finish_kernel(layer_hbm, infl_hbm, score_hbm, out_hbm, infl_out, score_out, buf, sem):
    into = pltpu.make_async_copy(layer_hbm, buf, sem.at[0])
    small = [
        pltpu.make_async_copy(infl_hbm, infl_out, sem.at[1]),
        pltpu.make_async_copy(score_hbm, score_out, sem.at[2]),
    ]
    into.start()
    for copy in small:
        copy.start()
    into.wait()
    out = pltpu.make_async_copy(buf, out_hbm, sem.at[3])
    out.start()
    for copy in small:
        copy.wait()
    out.wait()


def local(
    hidden_in, attn_gain, q_weight, q_bias, k_weight, k_bias, v_weight, v_bias, o_weight,
    mlp_gain, gate_weight, up_weight, down_weight, lengths,
):
    seqs_n, tok_n, width = hidden_in.shape
    near, far = rotation_tables()

    hbm = pl.BlockSpec(memory_space=pltpu.HBM)
    vmem = pl.BlockSpec(memory_space=pltpu.VMEM)
    smem = pl.BlockSpec(memory_space=pltpu.SMEM)
    dma = pltpu.SemaphoreType.DMA
    results = (
        jax.ShapeDtypeStruct((ROWS, QUART), BF16),
        jax.ShapeDtypeStruct((2, TOK), F32),
        jax.ShapeDtypeStruct((2,), F32),
    )
    layer_part, influence, score = pl.pallas_call(
        layer_kernel,
        out_shape=results,
        in_specs=[hbm] * 16,
        out_specs=(hbm, vmem, smem),
        scratch_shapes=[
            pltpu.VMEM((ROWS, D), BF16),
            pltpu.VMEM((ROWS, QUART), BF16),
            pltpu.VMEM((ROWS, D), BF16),
            pltpu.VMEM((D, QCOLS), BF16),
            pltpu.VMEM((D, 2 * HEAD), BF16),
            pltpu.VMEM((MP, QCOLS, QUART), BF16),
            pltpu.VMEM((2, OWN_HEADS * TOK, HEAD), BF16),
            pltpu.VMEM((2, NY, NZ, 2, TOK, 2 * HEAD), BF16),
            pltpu.VMEM((NY, NZ, 2, WR, 2 * FFP), BF16),
            pltpu.VMEM((NY, NZ, 2, WR, FFP), BF16),
            pltpu.VMEM((2, OWN_HEADS * TOK, HEAD), F32),
            pltpu.VMEM((2, OWN_HEADS * TOK, HEAD), F32),
            pltpu.VMEM((2, OWN_HEADS * TOK, HEAD), F32),
            pltpu.VMEM((ROWS, QCOLS), BF16),
            pltpu.VMEM((2, MP, TOK, QUART), BF16),
            pltpu.VMEM((2, 2, TOK // 2, QUART), BF16),
            pltpu.VMEM((2, ROWS, QUART), BF16),
            pltpu.VMEM((MP, ROWS, QUART), BF16),
            pltpu.VMEM((4, MP, ROWS, HEAD), BF16),
            pltpu.VMEM((4, 2, TOK, HEAD), BF16),
            pltpu.VMEM((4, 2, ROWS, HEAD), BF16),
            pltpu.VMEM((ROWS, D), BF16),
            pltpu.VMEM((ROWS, FFP), BF16),
            pltpu.VMEM((ROWS, HEAD), F32),
            pltpu.VMEM((MP, 8, ROWS), F32),
            pltpu.VMEM((NS, 8, HEAD), F32),
            pltpu.VMEM((ROWS, FFP), F32),
            pltpu.VMEM((ROWS, QUART), BF16),
            pltpu.VMEM((1, D), F32),
            pltpu.VMEM((1, D), F32),
            pltpu.VMEM((1, QCOLS), F32),
            pltpu.VMEM((KV_HEADS, HEAD), F32),
            pltpu.VMEM((KV_HEADS, HEAD), F32),
            pltpu.VMEM((2, TOK, HEAD), F32),
            pltpu.VMEM((2, NS, HEAD), F32),
            pltpu.SMEM((2,), jnp.int32),
            dma((17,)),
            dma((1,)),
            dma((3, 2)),
            dma((73,)),
            dma((3, 3)),
            dma((43,)),
            dma((2,)),
            dma((NZ,)),
            dma((4,)),
            dma((4, 2)),
            dma((2,)),
            dma((8,)),
            dma((2,)),
            dma((2,)),
        ],
        compiler_params=pltpu.CompilerParams(
            collective_id=0, has_side_effects=True, vmem_limit_bytes=62 * 1024 * 1024
        ),
        name="layer",
    )(
        hidden_in.reshape(ROWS, width), attn_gain.reshape(1, width), q_weight,
        q_bias.reshape(1, QCOLS), k_weight, k_bias.reshape(KV_HEADS, HEAD), v_weight,
        v_bias.reshape(KV_HEADS, HEAD), o_weight, mlp_gain.reshape(1, width), gate_weight,
        up_weight, down_weight, near, far, lengths,
    )
    layer_part, influence, score = pl.pallas_call(
        finish_kernel,
        out_shape=results,
        in_specs=[hbm, hbm, hbm],
        out_specs=(hbm, hbm, hbm),
        scratch_shapes=[pltpu.VMEM((ROWS, QUART), BF16), dma((4,))],
        name="finish",
    )(layer_part, influence, score)
    return layer_part.reshape(seqs_n, tok_n, QUART), influence, score


def solution(mesh):
    placed = (
        P(None, "seq", None), P(), P(None, "mp"), P("mp"), P(), P(), P(), P(),
        P("mp", None), P(), P("seq", "mp"), P("seq", "mp"), P("seq", "mp"), P(),
    )
    return jax.shard_map(
        local, mesh=mesh, in_specs=placed,
        out_specs=(P(None, "seq", "mp"), P(None, "seq"), P()), check_vma=False,
    )
```

```python
import jax
import jax.numpy as jnp
import numpy as np
from jax import lax
from jax.experimental import pallas as pl
from jax.experimental.pallas import tpu as pltpu
from jax.sharding import PartitionSpec as P

HEADS = 16
KV_HEADS = 2
HEAD = 128
D = 2048
NY, NZ = 4, 8
MP = 4
TOK = 128
ROWS = 2 * TOK
OWN_HEADS = HEADS // MP
QCOLS = OWN_HEADS * HEAD
QUART = D // MP
FFP = 1408
WR = 32
GU_CUT = 1792
DN_CUT = 640
NS = NY * NZ * 2

rope_base = 1000000.0
norm_eps = 1e-06
masked_score = -1e30
EXP2_SCALE = HEAD ** (-0.5) * 1.4426950408889634


def rotation_tables():
    freq = rope_base ** (-2.0 * np.arange(HEAD // 2) / HEAD)
    freq = np.concatenate([freq, freq])
    near = np.arange(TOK)[:, None] * freq
    far = TOK * np.arange(NS)[:, None] * freq
    return np.stack([np.cos(near), np.sin(near)]).astype(np.float32), np.stack(
        [np.cos(far), np.sin(far)]).astype(np.float32)


MESH = pl.DeviceIdType.MESH
F32, BF16 = jnp.float32, jnp.bfloat16

Z_OFF = (0, -1, 1, -2, 2, -3, 3, -4)

FAR_RIGHT = (True, False, True)

EARLY = (
    ("zs", 1), ("bs", 1), ("bs", 2),
)
LATER = (
    ("bs", 0), ("qp",), ("zs", 2), ("zs", 0), ("ys", 0, 0), ("bp", 1), ("zh", 1, 1), ("bp", 2), ("bp", 0),
    ("ys", 1, 0), ("yp", 0, 0), ("zh", 2, 1), ("zh", 0, 1), ("bl", 1), ("bl", 2), ("bl", 0), ("bz", 0),
    ("zh", 1, 2), ("yp", 1, 0), ("yl", 0, 0), ("zh", 0, 2), ("xl", 0), ("yp", 0, 1), ("bh", 0, 1, 0),
    ("at", 0, 0), ("bh", 0, 1, 1), ("yp", 0, 2), ("at", 1, 0), ("yl", 1, 0), ("yp", 0, 3), ("zh", 1, 3),
    ("ys", 1, 1), ("yp", 0, 4), ("zh", 0, 3), ("yl", 0, 1), ("yl", 0, 2), ("bh", 0, 2, 0), ("xl", 1),
    ("yl", 0, 3), ("at", 0, 1), ("bh", 0, 2, 1), ("at", 0, 2), ("xl", 2), ("yp", 1, 1), ("bz", 1),
    ("at", 0, 3), ("zh", 1, 4), ("yl", 0, 4), ("zh", 0, 4), ("at", 1, 1), ("bh", 0, 3, 0), ("yp", 0, 5),
    ("at", 1, 2), ("bh", 0, 3, 1), ("at", 0, 4), ("yl", 1, 1), ("ys", 1, 2), ("xl", 3), ("yp", 0, 6),
    ("yp", 0, 7), ("bh", 1, 1, 0), ("yl", 0, 5), ("xl", 4), ("at", 1, 3), ("bh", 1, 1, 1), ("ys", 1, 3),
    ("at", 0, 5), ("xl", 5), ("bh", 0, 4, 0), ("bh", 0, 4, 1), ("yp", 1, 2), ("yl", 0, 6), ("at", 1, 4),
    ("yl", 0, 7), ("xl", 6), ("ys", 1, 4), ("at", 1, 5), ("bh", 1, 2, 0), ("at", 0, 6), ("yp", 1, 3),
    ("at", 0, 7), ("xl", 7), ("bh", 1, 2, 1), ("yl", 1, 2), ("ys", 1, 5), ("op", 0), ("at", 1, 6),
    ("yp", 1, 4), ("at", 1, 7), ("yl", 1, 3), ("zh", 2, 2), ("bh", 1, 3, 0), ("op", 1), ("ys", 1, 6),
    ("rm", 0), ("yp", 1, 5), ("bh", 1, 3, 1), ("yl", 1, 4), ("rm", 1), ("ys", 1, 7), ("zh", 2, 3), ("bz", 2),
    ("yp", 1, 6), ("bh", 1, 4, 0), ("re", 0), ("yl", 1, 5), ("bh", 1, 4, 1), ("zh", 2, 4), ("ys", 2, 0),
    ("ys", 2, 1), ("yp", 1, 7), ("re", 1), ("bh", 2, 1, 0), ("yl", 1, 6), ("ys", 2, 2), ("yp", 2, 0),
    ("bh", 2, 1, 1), ("yp", 2, 1), ("ap", 0), ("ys", 2, 3), ("yl", 1, 7), ("ys", 2, 4), ("bh", 2, 2, 0),
    ("yp", 2, 2), ("yl", 2, 0), ("ys", 2, 5), ("ap", 1), ("yl", 2, 1), ("ys", 2, 6), ("bh", 2, 2, 1),
    ("yp", 2, 3), ("sn", 0), ("yp", 2, 4), ("yl", 2, 2), ("ys", 2, 7), ("bh", 2, 3, 0), ("yp", 2, 5),
    ("sn", 1), ("gd",), ("yl", 2, 3), ("yp", 2, 6), ("yl", 2, 4), ("bh", 2, 3, 1), ("yp", 2, 7), ("ud",),
    ("yl", 2, 5), ("ds", 0), ("yl", 2, 6), ("bh", 2, 4, 0), ("ds", 1), ("yl", 2, 7), ("bh", 2, 4, 1),
    ("ds", 2), ("dm", 0), ("ds", 3), ("dm", 1), ("dm", 2), ("dm", 3),
)


def layer_kernel(
    hid_hbm, ag_hbm, qw_hbm, qb_hbm, kw_hbm, kb_hbm, vw_hbm, vb_hbm, ow_hbm, mg_hbm,
    gate_hbm, up_hbm, down_hbm, near_hbm, far_hbm, len_hbm,
    out_hbm, infl_ref, score_ref,
    hid, hidq, normed, qw, kvw, ow, qbuf, kv, gu, down, mbuf, lbuf, accbuf, attn,
    stage1, tr1, rs1, resid, stage2, tr2, rs2, mlp_in, act, innp, sums, tot, gbuf, layer_v,
    ag_ref, mg_ref, qb_ref, kb_ref, vb_ref, near_ref, far_ref, len_ref,
    lsem, osem, a_send, a_recv, b_send, b_recv, k_send, k_recv, x_send, x_recv, r_send, r_recv,
    s_sem, t_sem,
):
    s = lax.axis_index("seq")
    m = lax.axis_index("mp")
    y = s // (2 * NZ)
    z = lax.rem(s // 2, NZ)
    c = lax.rem(s, 2)
    kvi = m // 2

    def wrap(v, n):
        return lax.rem(v + 2 * n, n)

    def dev(yy, zz, cc):
        return (wrap(yy, NY) * NZ + wrap(zz, NZ)) * 2 + cc

    zp, zm = dev(y, z + 1, c), dev(y, z - 1, c)
    yp, ym = dev(y + 1, z, c), dev(y - 1, z, c)
    partner = dev(y, z, 1 - c)

    def rc(src, dst, ssem, rsem, sdev):
        return pltpu.make_async_remote_copy(
            src_ref=src, dst_ref=dst, send_sem=ssem, recv_sem=rsem,
            device_id={"seq": sdev, "mp": m}, device_id_type=MESH,
        )

    def rcx(src, dst, ssem, rsem, mdev):
        return pltpu.make_async_remote_copy(
            src_ref=src, dst_ref=dst, send_sem=ssem, recv_sem=rsem,
            device_id={"seq": s, "mp": mdev}, device_id_type=MESH,
        )

    bar = pltpu.get_barrier_semaphore()
    for peer in (zp, zm, yp, ym, partner):
        pl.semaphore_signal(bar, inc=1, device_id={"seq": peer, "mp": m}, device_id_type=MESH)
    for i in range(1, MP):
        pl.semaphore_signal(bar, inc=1, device_id={"seq": s, "mp": wrap(m + i, MP)}, device_id_type=MESH)

    kv_cols = pl.ds(pl.multiple_of(kvi * HEAD, HEAD), HEAD)
    own = gu.at[y, z, c]
    ow_here = []

    def group_of(index, *pairs):
        return [pltpu.make_async_copy(a, b, lsem.at[index + i]) for i, (a, b) in enumerate(pairs)]

    loads = {
        "up": group_of(0, (up_hbm, own.at[:, pl.ds(FFP, FFP)])),
        "gate": group_of(1, (gate_hbm, own.at[:, pl.ds(0, FFP)])),
        "hid": group_of(2, (hid_hbm, hid), (ag_hbm, ag_ref)),
        "kv": group_of(
            4, (kw_hbm.at[:, kv_cols], kvw.at[:, pl.ds(0, HEAD)]),
            (vw_hbm.at[:, kv_cols], kvw.at[:, pl.ds(HEAD, HEAD)]),
            (kb_hbm, kb_ref), (vb_hbm, vb_ref), (near_hbm, near_ref), (far_hbm, far_ref)),
        "q": group_of(10, (qw_hbm, qw), (qb_hbm, qb_ref)),
        "len": group_of(16, (len_hbm, len_ref)),
        "down": group_of(12, (down_hbm, down.at[y, z, c])),
        "hidq": group_of(
            13, (hid_hbm.at[:, pl.ds(pl.multiple_of(m * QUART, QUART), QUART)], hidq), (mg_hbm, mg_ref)),
    }
    for copies in loads.values():
        for copy in copies:
            copy.start()

    for q in range(MP):
        pltpu.make_async_copy(ow_hbm.at[:, pl.ds(q * QUART, QUART)], ow.at[q], lsem.at[15]).start()

    def need(name):
        if name == "ow":
            if not ow_here:
                pltpu.make_async_copy(ow, ow, lsem.at[15]).wait()
                ow_here.append(True)
        for copy in loads.pop(name, ()):
            copy.wait()

    pl.semaphore_wait(bar, 5 + MP - 1)

    ALL = slice(None)
    ZR, YR, HR, DR = 0, 4, 12, 20
    A_HALF = (TOK // 2, WR // 2, WR // 2)
    WGU, WDN = ("gate", "up"), ("down",)

    def a_ref(st, yy, zz, cc):
        if st == 0:
            return kv.at[0, yy, zz, cc]
        if st == 1:
            return gu.at[yy, zz, cc, :, pl.ds(0, GU_CUT)]
        return down.at[yy, zz, cc, :, pl.ds(0, DN_CUT)]

    def load_of(st):
        for name in ((), WGU, WDN)[st]:
            need(name)

    def block(st, yy, zz):
        return a_ref(st, wrap(yy, NY), wrap(zz, NZ), c)

    def half(st, ref, i):
        return ref.at[pl.ds(i * A_HALF[st], A_HALF[st])]

    def a_copy(ref, st, ssem, rsem, d):
        return rc(ref, ref, a_send.at[st, ssem], a_recv.at[(0, 28, 49)[st] + rsem], d)

    def a_wait_recv(st, rsem, *size):
        a_copy(a_ref(st, *size), st, 0, rsem, partner).wait_recv()

    def zk_of(k):
        if isinstance(k, int):
            return z + Z_OFF[k]
        return z + jnp.where(lax.rem(k, 2) == 1, -((k + 1) // 2), k // 2)

    def z_copy(st, k_to, zz, right):
        return a_copy(block(st, y, zz), st, 0, ZR + (k_to - 1) // 2, zp if right else zm)

    def y_send(st, k):
        load_of(st)
        ref = block(st, y, zk_of(k))
        a_copy(ref, st, 1, YR + k, yp).start()
        a_copy(ref, st, 1, YR + k, ym).start()

    TWO = pl.ds(0, 2)

    def y_pass(st, k):
        zz = zk_of(k)
        a_wait_recv(st, YR + k, TWO, 0, 0)
        a_copy(half(st, block(st, y - 1, zz), 0), st, 1, HR + k, yp).start()
        a_copy(half(st, block(st, y + 1, zz), 1), st, 1, HR + k, ym).start()

    def d_index(st, k):
        return DR + (k, 0, max(0, (k - 1) // 2))[st]

    def y_last(st, k):
        a_wait_recv(st, HR + k, 0, 0, 0)
        a_copy(a_ref(st, ALL, wrap(zk_of(k), NZ), c), st, 1, d_index(st, k), partner).start()

    def z_start(st):
        load_of(st)
        z_copy(st, 1, z, True).start()
        z_copy(st, 2, z, False).start()

    def z_hop(st, h):
        far_right = FAR_RIGHT[st]
        a_wait_recv(st, ZR + h - 1, TWO if h < 4 else 0, 0, 0)
        for k in (2 * h - 1, 2 * h):
            if k >= NZ:
                continue
            right = far_right if k == 7 else k % 2 == 1
            if k + 2 < NZ - 1:
                z_copy(st, k + 2, zk_of(k), right).start()
            if k == (5 if far_right else 6):
                z_copy(st, 7, zk_of(k), far_right).start()
            if st == 0:
                y_send(st, k)

    BY, BH, BZ, BD = 0, 1, 2, 10
    B_HALF = (TOK // 4, WR // 2, WR // 2)
    mine = pl.multiple_of(lax.rem(m, 2) * (TOK // 2), TOK // 2)
    other = pl.multiple_of(TOK // 2 - mine, TOK // 2)

    def b_full(st, yy, zz, cc):
        if st == 0:
            return kv.at[1, yy, zz, cc]
        if st == 1:
            return gu.at[yy, zz, cc, :, pl.ds(GU_CUT, 2 * FFP - GU_CUT)]
        return down.at[yy, zz, cc, :, pl.ds(DN_CUT, FFP - DN_CUT)]

    def b_ref(st, yy, zz, cc):
        if st == 0:
            return kv.at[1, yy, zz, cc, pl.ds(mine, TOK // 2)]
        return b_full(st, yy, zz, cc)

    def b_copy(st, ref, ssem, rsem, d):
        return rc(ref, ref, b_send.at[st, ssem], b_recv.at[(0, 18, 29)[st] + rsem], d)

    def b_wait_recv(st, rsem, *size):
        b_copy(st, b_ref(st, *size), 0, rsem, partner).wait_recv()

    def b_block(st, yy, w=None):
        ref = b_ref(st, wrap(yy, NY), z, c)
        return ref if w is None else ref.at[pl.ds(w * B_HALF[st], B_HALF[st])]

    def group(st, zz, w):
        rows = pl.ds(w * B_HALF[st], B_HALF[st])
        zz = wrap(zz, NZ)
        if st == 0:
            rows = pl.ds(pl.multiple_of(mine + w * B_HALF[st], B_HALF[st]), B_HALF[st])
            return kv.at[1, :, zz, c, rows]
        if st == 1:
            return gu.at[:, zz, c, rows, pl.ds(GU_CUT, 2 * FFP - GU_CUT)]
        return down.at[:, zz, c, rows, pl.ds(DN_CUT, FFP - DN_CUT)]

    def r_copy(st, i, w):
        return b_copy(st, group(st, z - (i - 1), w), 1, BZ + 2 * (i - 1) + w, zp)

    def l_copy(st, i, w):
        return b_copy(st, group(st, z + (i - 1), w), 1, BZ + 2 * (i - 1) + w, zm)

    def r_steps(w):
        return 4 if w == 0 else 3

    def l_steps(w):
        return 3 if w == 0 else 4

    def by_start(st):
        for name in ((), WGU[1:], WDN)[st]:
            need(name)
        b_copy(st, b_block(st, y), 0, BY, yp).start()
        b_copy(st, b_block(st, y), 0, BY, ym).start()

    def by_pass(st):
        b_wait_recv(st, BY, TWO, 0, 0)
        b_copy(st, b_block(st, y - 1, 0), 0, BH, yp).start()
        b_copy(st, b_block(st, y + 1, 1), 0, BH, ym).start()

    def b_all_wait(st, rsem, *size):
        ref = b_full(st, *size)
        rc(ref, ref, b_send.at[st, 2], b_recv.at[(0, 18, 29)[st] + rsem], partner).wait_recv()

    def bd_start(st, k):
        b_copy(st, b_full(st, ALL, wrap(zk_of(k), NZ), c), 2,
               BD + (k, 0, max(0, (k - 1) // 2))[st], partner).start()

    pair = m + 1 - 2 * lax.rem(m, 2)

    def k_copy(ref, k):
        return rcx(ref, ref, k_send.at[min(k, 1)], k_recv.at[k], pair)

    def swap_start(k):
        zz = wrap(zk_of(k), NZ)
        rows = pl.ds(mine, TOK // 2)
        if k == 0:
            for i in range(1, NY):
                k_copy(kv.at[1, wrap(y + i, NY), zz, c, rows], k).start()
        else:
            k_copy(kv.at[1, :, zz, c, rows], k).start()

    def swap_last(k):
        some = kv.at[1, pl.ds(0, NY - 1) if k == 0 else ALL, 0, 0, pl.ds(0, TOK // 2)]
        k_copy(some, k).wait_recv()
        bd_start(0, k)

    def b_done(st, k):
        if st == 0:
            swap_start(k)
        else:
            bd_start(st, k)

    def by_last(st):
        b_wait_recv(st, BH, 0, 0, 0)
        b_done(st, 0)

    def bz_start(st):
        for w in range(2):
            r_copy(st, 1, w).start()
            l_copy(st, 1, w).start()

    def b_hop(st, h, w):
        b_wait_recv(st, BZ + 2 * (h - 1) + w, ALL if h < 4 else TWO, 0, 0)
        if h + 1 <= r_steps(w):
            r_copy(st, h + 1, w).start()
        if h + 1 <= l_steps(w):
            l_copy(st, h + 1, w).start()
        if w == 1:
            for k in (2 * h - 1, 2 * h):
                if k < NZ:
                    b_done(st, k)

    TASKS = {
        "zs": z_start, "zh": z_hop, "ys": y_send, "yp": y_pass, "yl": y_last,
        "bs": by_start, "bp": by_pass, "bl": by_last, "bz": bz_start, "bh": b_hop,
    }
    for name, *args in EARLY:
        TASKS[name](*args)

    need("hid")

    def norm_rows(i, _):
        r = pl.ds(pl.multiple_of(i * 16, 16), 16)
        x = hid[r, :].astype(F32)
        sq = x * x
        part = sq[:, 0:HEAD]
        for j in range(1, D // HEAD):
            part = part + sq[:, j * HEAD:(j + 1) * HEAD]
        innp[r, :] = part
        factor = lax.rsqrt(jnp.sum(part, axis=-1, keepdims=True) * (1.0 / D) + norm_eps)
        normed[r, :] = (x * factor * ag_ref[...]).astype(BF16)
        return 0

    lax.fori_loop(0, ROWS // 16, norm_rows, 0, unroll=4)

    need("kv")
    far_cos, far_sin = far_ref[0, pl.ds(s, 1), :], far_ref[1, pl.ds(s, 1), :]
    near_cos, near_sin = near_ref[0], near_ref[1]
    cos = near_cos * far_cos - near_sin * far_sin
    sin = near_sin * far_cos + near_cos * far_sin
    first = lax.broadcasted_iota(jnp.int32, sin.shape, 1) < HEAD // 2
    sin = jnp.where(first, -sin, sin)

    def rope(u):
        return u * cos + pltpu.roll(u, HEAD // 2, 1) * sin

    kv_all = jnp.dot(normed[...], kvw[...], preferred_element_type=F32)
    kb = kb_ref[pl.ds(kvi, 1), :]
    vb = vb_ref[pl.ds(kvi, 1), :]
    for sq in range(2):
        kk = kv_all[sq * TOK:(sq + 1) * TOK, 0:HEAD] + kb
        vv = kv_all[sq * TOK:(sq + 1) * TOK, HEAD:2 * HEAD] + vb
        kv[sq, y, z, c, :, 0:HEAD] = rope(kk).astype(BF16)
        kv[sq, y, z, c, :, HEAD:2 * HEAD] = vv.astype(BF16)

    for sq in range(2):
        mbuf[sq] = jnp.full((OWN_HEADS * TOK, HEAD), masked_score, F32)
        lbuf[sq] = jnp.zeros((OWN_HEADS * TOK, HEAD), F32)
        accbuf[sq] = jnp.zeros((OWN_HEADS * TOK, HEAD), F32)

    def queries():
        need("q")
        q_all = jnp.dot(normed[...], qw[...], preferred_element_type=F32) + qb_ref[...]
        for sq in range(2):
            for h in range(OWN_HEADS):
                u = q_all[sq * TOK:(sq + 1) * TOK, h * HEAD:(h + 1) * HEAD]
                qbuf[sq, h * TOK:(h + 1) * TOK, :] = rope(u).astype(BF16)

    def attend(sq, yks, zk, diagonal):
        pairs = [kv[sq, yk, zk] for yk in yks]
        kb_ = jnp.concatenate([p[:, :, 0:HEAD].reshape(2 * TOK, HEAD) for p in pairs], axis=0)
        vb_ = jnp.concatenate([p[:, :, HEAD:2 * HEAD].reshape(2 * TOK, HEAD) for p in pairs], axis=0)
        sc = lax.dot_general(qbuf[sq], kb_, (((1,), (1,)), ((), ())), preferred_element_type=F32)
        if diagonal:
            row = lax.rem(lax.broadcasted_iota(jnp.int32, sc.shape, 0), TOK) + c * TOK
            col = lax.broadcasted_iota(jnp.int32, sc.shape, 1)
            sc = jnp.where(col <= row, sc, masked_score)
        m_old = mbuf[sq]
        m_new = jnp.maximum(m_old, jnp.max(sc, axis=1, keepdims=True))
        p = jnp.exp2((sc - jnp.concatenate([m_new] * (2 * len(yks)), axis=1)) * EXP2_SCALE)
        alpha = jnp.exp2((m_old - m_new) * EXP2_SCALE)
        mbuf[sq] = m_new
        part = p[:, 0:HEAD]
        for i in range(1, 2 * len(yks)):
            part = part + p[:, i * HEAD:(i + 1) * HEAD]
        lbuf[sq] = lbuf[sq] * alpha + part
        accbuf[sq] = accbuf[sq] * alpha + jnp.dot(p.astype(BF16), vb_, preferred_element_type=F32)

    def attend_round(sq, k):
        zk = wrap(zk_of(k), NZ)

        @pl.when(k == 0)
        def _():
            attend(sq, (y,), zk, True)

        n = y + jnp.where(zk < z, 1, 0)

        for count in range(1, NY + 1):
            @pl.when(n == count)
            def _():
                attend(sq, tuple(range(count)), zk, False)

    def seq_rows(sq):
        return pl.ds(sq * TOK, TOK)

    right, left = wrap(m + 1, MP), wrap(m + MP - 1, MP)
    FROM_LEFT, FROM_RIGHT = 0, 1
    X_TR, X_RS, X_AG, X_AGH = range(4)

    def x_copy(src, dst, phase, sq, to):
        return rcx(src, dst, x_send.at[phase], x_recv.at[phase, sq], to)

    def x_wait(ref, phase, sq):
        x_copy(ref, ref, phase, sq, right).wait_recv()

    def o_project(sq):
        need("ow")
        for h in range(OWN_HEADS):
            r = slice(h * TOK, (h + 1) * TOK)
            attn[sq * TOK:(sq + 1) * TOK, h * HEAD:(h + 1) * HEAD] = (
                accbuf[sq, r, :] / jnp.sum(lbuf[sq, r, :], axis=1, keepdims=True)
            ).astype(BF16)
        here = attn[sq * TOK:(sq + 1) * TOK, :]
        for j in (2, 1, 3, 0):
            part = jnp.dot(here, ow[wrap(m + j, MP)], preferred_element_type=F32).astype(BF16)
            stage1[sq, j] = part
            if j == 1:
                for i, to in ((FROM_LEFT, right), (FROM_RIGHT, left)):
                    x_copy(stage1.at[sq, 2, pl.ds(i * (TOK // 2), TOK // 2)], tr1.at[sq, i], X_TR, sq, to).start()

    def rs1_mid(sq):
        x_wait(tr1.at[sq], X_TR, sq)
        for i, j, to in ((FROM_LEFT, 1, right), (FROM_RIGHT, 3, left)):
            r = slice(i * (TOK // 2), (i + 1) * (TOK // 2))
            both = stage1[sq, j, r, :].astype(F32) + tr1[sq, i].astype(F32)
            stage1[sq, j, r, :] = both.astype(BF16)
            x_copy(stage1.at[sq, j], rs1.at[i, seq_rows(sq)], X_RS, sq, to).start()

    def residual(sq):
        need("hidq")
        r = seq_rows(sq)
        x_wait(rs1.at[:, r], X_RS, sq)
        add = stage1[sq, 0].astype(F32) + rs1[0, r, :].astype(F32) + rs1[1, r, :].astype(F32)
        resid[m, r, :] = (hidq[r, :].astype(F32) + add).astype(BF16)
        for to in (right, left):
            x_copy(resid.at[m, r], resid.at[m, r], X_AG, sq, to).start()

    def ag_pass(sq):
        x_wait(resid.at[TWO, seq_rows(sq)], X_AG, sq)
        for i, src, to in ((0, left, right), (1, right, left)):
            ref = resid.at[src, pl.ds(sq * TOK + i * (TOK // 2), TOK // 2)]
            x_copy(ref, ref, X_AGH, sq, to).start()

    def second_norm(sq):
        x_wait(resid.at[0, seq_rows(sq)], X_AGH, sq)

        def norm2_rows(i, _):
            r = pl.ds(pl.multiple_of(sq * TOK + i * 16, 16), 16)
            xs = [resid[q, r, :].astype(F32) for q in range(MP)]
            part = None
            for x in xs:
                sqr = x * x
                for j in range(QUART // HEAD):
                    t = sqr[:, j * HEAD:(j + 1) * HEAD]
                    part = t if part is None else part + t
            factor = lax.rsqrt(jnp.sum(part, axis=-1, keepdims=True) * (1.0 / D) + norm_eps)
            for q in range(MP):
                cols = slice(q * QUART, (q + 1) * QUART)
                mlp_in[r, cols] = (xs[q] * factor * mg_ref[:, cols]).astype(BF16)
            return 0

        lax.fori_loop(0, TOK // 16, norm2_rows, 0, unroll=4)

    def gate_dot():
        a_wait_recv(1, DR, ALL, ALL, 0)
        rows = gu[:, :, :, :, 0:FFP].reshape(D, FFP)
        gbuf[...] = jnp.dot(mlp_in[...], rows, preferred_element_type=F32)

    def up_dot():
        b_wait_recv(1, BD, ALL, ALL, 0)
        rows = gu[:, :, :, :, FFP:2 * FFP].reshape(D, FFP)
        up_sum = jnp.dot(mlp_in[...], rows, preferred_element_type=F32)
        g = gbuf[...]
        act[...] = (g / (1.0 + jnp.exp(-g)) * up_sum).astype(BF16)

    odd = lax.rem(z, 2)

    def z_pair(i):
        turn = (0, 2 * odd - 1, 1 - 2 * odd, 2)[i]
        return wrap(z // 2 + turn, NZ // 2)

    def r_copy2(src, dst, ssem, rsem, to):
        return rcx(src, dst, r_send.at[ssem], r_recv.at[rsem], to)

    def down_stage(i):
        rounds = pl.ds(0, (3, 2, 2, 1)[i])
        a_wait_recv(2, DR + i, ALL, rounds, 0)
        b_wait_recv(2, BD + i, ALL, rounds, 0)
        p = z_pair(i)
        for q0 in (0, 2):
            rows = down[q0:q0 + 2, pl.ds(2 * p, 2)].reshape(2 * HEAD, FFP)
            part = lax.dot_general(
                act[...], rows, (((1,), (1,)), ((), ())), preferred_element_type=F32
            ).astype(BF16)
            stage2[i, q0] = part[:, 0:HEAD]
            stage2[i, q0 + 1] = part[:, HEAD:2 * HEAD]
        far_q = wrap(m + 2, MP)
        for w, to in ((FROM_LEFT, right), (FROM_RIGHT, left)):
            r_copy2(stage2.at[i, far_q, pl.ds(w * TOK, TOK)], tr2.at[i, w], 0, i, to).start()

    def rs2_mid(i):
        r_copy2(tr2.at[i], tr2.at[i], 0, i, right).wait_recv()
        for w, q in ((FROM_LEFT, right), (FROM_RIGHT, left)):
            r = slice(w * TOK, (w + 1) * TOK)
            both_ = stage2[i, q, r, :].astype(F32) + tr2[i, w].astype(F32)
            stage2[i, q, r, :] = both_.astype(BF16)
            r_copy2(stage2.at[i, q], rs2.at[i, w], 1, 4 + i, q).start()

    def layer_stage(i, so_far):
        r_copy2(rs2.at[i], rs2.at[i], 1, 4 + i, right).wait_recv()
        cols = pl.ds(pl.multiple_of(z_pair(i) * HEAD, HEAD), HEAD)
        add = stage2[i, m].astype(F32) + rs2[i, 0].astype(F32) + rs2[i, 1].astype(F32)
        layer = (resid[m, :, cols].astype(F32) + add).astype(BF16)
        layer_v[:, cols] = layer
        wide = layer.astype(F32)
        cp, op = hidq[:, cols].astype(F32) * wide, wide * wide
        return (cp, op) if so_far is None else (so_far[0] + cp, so_far[1] + op)

    TASKS.update(
        qp=queries, op=o_project, rm=rs1_mid, re=residual, ap=ag_pass, sn=second_norm, xl=swap_last, dm=rs2_mid, gd=gate_dot, ud=up_dot, ds=down_stage,
    )
    items, before, after = [], [], []
    for name, *args in LATER:
        if name == "at":
            items.append(args)
            before.append(after)
            after = []
        else:
            after.append((TASKS[name], args))

    def run(events):
        for act_, args in events:
            act_(*args)

    def pick(t, values):
        total = 0
        for i, v in enumerate(values):
            if v:
                total = total + jnp.where(t == i, v, 0)
        return total

    def item(t, _):
        for i, events in enumerate(before):
            if events:
                pl.when(t == i)(lambda events=events: run(events))
        sq = pick(t, [e[0] for e in items])
        k = pick(t, [e[1] for e in items])

        @pl.when(sq == 0)
        def _():
            a_wait_recv(0, DR + k, ALL, 0, 0)

        @pl.when(sq == 1)
        def _():
            b_all_wait(0, BD + k, ALL, 0, 0)

        attend_round(sq, k)
        return 0

    lax.fori_loop(0, len(items), item, 0)
    run(after)

    seven = pl.ds(0, NZ - 1)
    for st in range(3):
        a_copy(a_ref(st, 0, seven, 0), st, 0, 0, partner).wait_send()
        a_copy(a_ref(st, ALL, seven, ALL), st, 1, 0, partner).wait_send()
        b_copy(st, b_ref(st, 0, pl.ds(0, 3), 0), 0, 0, partner).wait_send()
        b_copy(st, b_ref(st, ALL, seven, 0), 1, 0, partner).wait_send()
        b_copy(st, b_full(st, ALL, ALL, 0), 2, 0, partner).wait_send()
    x_copy(rs1.at[0], rs1.at[0], X_TR, 0, right).wait_send()
    x_copy(rs1, rs1, X_RS, 0, right).wait_send()
    x_copy(rs1, rs1, X_AG, 0, right).wait_send()
    x_copy(rs1.at[0], rs1.at[0], X_AGH, 0, right).wait_send()
    k_copy(kv.at[1, pl.ds(0, NY - 1), 0, 0, pl.ds(0, TOK // 2)], 0).wait_send()
    k_copy(kv.at[1, :, seven, 0, pl.ds(0, TOK // 2)], 1).wait_send()

    def lane_sums(part):
        return jnp.sum(part.T, axis=0, keepdims=True)

    need("len")
    in_norm = lane_sums(innp[...])

    so_far = None
    for i in range(4):
        so_far = layer_stage(i, so_far)
    out_copy = pltpu.make_async_copy(layer_v, out_hbm, osem.at[0])
    rowi = lax.broadcasted_iota(jnp.int32, (8, ROWS), 0)
    sums[m] = jnp.where(rowi == 0, lane_sums(so_far[0]), lane_sums(so_far[1]))

    def s_copy(j):
        return rcx(sums.at[m], sums.at[m], s_sem.at[0], s_sem.at[1], wrap(m + j, MP))

    for j in (2, 1, 3):
        s_copy(j).start()
    out_copy.start()
    came = sums.at[pl.ds(0, MP - 1)]
    rcx(came, came, s_sem.at[0], s_sem.at[1], wrap(m + 1, MP)).wait()
    both = sums[0] + sums[1] + sums[2] + sums[3]
    cross, out_norm = both[0:1, :], both[1:2, :]
    cosine = cross / jnp.sqrt((in_norm + norm_eps) * (out_norm + norm_eps))
    lane = lax.broadcasted_iota(jnp.int32, (1, ROWS), 1)
    pos = s * TOK + lax.rem(lane, TOK)
    limit = jnp.where(lane < TOK, len_ref[0], len_ref[1])
    influence = jnp.where(pos < limit, 1.0 - cosine, 0.0)
    infl_ref[0:1, :] = influence[:, 0:TOK]
    infl_ref[1:2, :] = influence[:, TOK:2 * TOK]
    t0 = jnp.sum(influence[:, 0:TOK], axis=1, keepdims=True)
    t1 = jnp.sum(influence[:, TOK:2 * TOK], axis=1, keepdims=True)
    lane = lax.broadcasted_iota(jnp.int32, (1, HEAD), 1)
    one = pl.ds(0, 1)
    tot[s, one, :] = jnp.where(lane < HEAD // 2, t0, t1)

    for dy in (2, 1, 3, 0):
        for dz in (4, 3, 5, 2, 6, 1, 7, 0):
            for cc in (c, 1 - c):
                if dy == 0 and dz == 0 and cc is c:
                    continue
                ref = tot.at[s, one]
                rc(ref, ref, t_sem.at[0], t_sem.at[1], dev(y + dy, z + dz, cc)).start()
    every = tot.at[pl.ds(0, NS - 1), one]
    rc(every, every, t_sem.at[0], t_sem.at[1], partner).wait()
    total = jnp.sum(tot[:, 0, :], axis=0, keepdims=True)
    tokens = jnp.where(lane < HEAD // 2, len_ref[0], len_ref[1]).astype(F32)
    score = total / tokens
    score_ref[0] = jnp.sum(jnp.where(lane == 0, score, 0.0))
    score_ref[1] = jnp.sum(jnp.where(lane == HEAD - 1, score, 0.0))

    r_copy2(tr2, tr2, 0, 0, right).wait_send()
    r_copy2(rs2, rs2, 1, 0, right).wait_send()
    out_copy.wait()


def finish_kernel(layer_hbm, infl_hbm, score_hbm, out_hbm, infl_out, score_out, buf, sem):
    into = pltpu.make_async_copy(layer_hbm, buf, sem.at[0])
    small = [
        pltpu.make_async_copy(infl_hbm, infl_out, sem.at[1]),
        pltpu.make_async_copy(score_hbm, score_out, sem.at[2]),
    ]
    into.start()
    for copy in small:
        copy.start()
    into.wait()
    out = pltpu.make_async_copy(buf, out_hbm, sem.at[3])
    out.start()
    for copy in small:
        copy.wait()
    out.wait()


def local(
    hidden_in, attn_gain, q_weight, q_bias, k_weight, k_bias, v_weight, v_bias, o_weight,
    mlp_gain, gate_weight, up_weight, down_weight, lengths,
):
    seqs_n, tok_n, width = hidden_in.shape
    near, far = rotation_tables()

    hbm = pl.BlockSpec(memory_space=pltpu.HBM)
    vmem = pl.BlockSpec(memory_space=pltpu.VMEM)
    smem = pl.BlockSpec(memory_space=pltpu.SMEM)
    dma = pltpu.SemaphoreType.DMA
    results = (
        jax.ShapeDtypeStruct((ROWS, QUART), BF16),
        jax.ShapeDtypeStruct((2, TOK), F32),
        jax.ShapeDtypeStruct((2,), F32),
    )
    layer_part, influence, score = pl.pallas_call(
        layer_kernel,
        out_shape=results,
        in_specs=[hbm] * 16,
        out_specs=(hbm, vmem, smem),
        scratch_shapes=[
            pltpu.VMEM((ROWS, D), BF16),
            pltpu.VMEM((ROWS, QUART), BF16),
            pltpu.VMEM((ROWS, D), BF16),
            pltpu.VMEM((D, QCOLS), BF16),
            pltpu.VMEM((D, 2 * HEAD), BF16),
            pltpu.VMEM((MP, QCOLS, QUART), BF16),
            pltpu.VMEM((2, OWN_HEADS * TOK, HEAD), BF16),
            pltpu.VMEM((2, NY, NZ, 2, TOK, 2 * HEAD), BF16),
            pltpu.VMEM((NY, NZ, 2, WR, 2 * FFP), BF16),
            pltpu.VMEM((NY, NZ, 2, WR, FFP), BF16),
            pltpu.VMEM((2, OWN_HEADS * TOK, HEAD), F32),
            pltpu.VMEM((2, OWN_HEADS * TOK, HEAD), F32),
            pltpu.VMEM((2, OWN_HEADS * TOK, HEAD), F32),
            pltpu.VMEM((ROWS, QCOLS), BF16),
            pltpu.VMEM((2, MP, TOK, QUART), BF16),
            pltpu.VMEM((2, 2, TOK // 2, QUART), BF16),
            pltpu.VMEM((2, ROWS, QUART), BF16),
            pltpu.VMEM((MP, ROWS, QUART), BF16),
            pltpu.VMEM((4, MP, ROWS, HEAD), BF16),
            pltpu.VMEM((4, 2, TOK, HEAD), BF16),
            pltpu.VMEM((4, 2, ROWS, HEAD), BF16),
            pltpu.VMEM((ROWS, D), BF16),
            pltpu.VMEM((ROWS, FFP), BF16),
            pltpu.VMEM((ROWS, HEAD), F32),
            pltpu.VMEM((MP, 8, ROWS), F32),
            pltpu.VMEM((NS, 8, HEAD), F32),
            pltpu.VMEM((ROWS, FFP), F32),
            pltpu.VMEM((ROWS, QUART), BF16),
            pltpu.VMEM((1, D), F32),
            pltpu.VMEM((1, D), F32),
            pltpu.VMEM((1, QCOLS), F32),
            pltpu.VMEM((KV_HEADS, HEAD), F32),
            pltpu.VMEM((KV_HEADS, HEAD), F32),
            pltpu.VMEM((2, TOK, HEAD), F32),
            pltpu.VMEM((2, NS, HEAD), F32),
            pltpu.SMEM((2,), jnp.int32),
            dma((17,)),
            dma((1,)),
            dma((3, 2)),
            dma((73,)),
            dma((3, 3)),
            dma((43,)),
            dma((2,)),
            dma((NZ,)),
            dma((4,)),
            dma((4, 2)),
            dma((2,)),
            dma((8,)),
            dma((2,)),
            dma((2,)),
        ],
        compiler_params=pltpu.CompilerParams(
            collective_id=0, has_side_effects=True, vmem_limit_bytes=62 * 1024 * 1024
        ),
        name="layer",
    )(
        hidden_in.reshape(ROWS, width), attn_gain.reshape(1, width), q_weight,
        q_bias.reshape(1, QCOLS), k_weight, k_bias.reshape(KV_HEADS, HEAD), v_weight,
        v_bias.reshape(KV_HEADS, HEAD), o_weight, mlp_gain.reshape(1, width), gate_weight,
        up_weight, down_weight, near, far, lengths,
    )
    layer_part, influence, score = pl.pallas_call(
        finish_kernel,
        out_shape=results,
        in_specs=[hbm, hbm, hbm],
        out_specs=(hbm, hbm, hbm),
        scratch_shapes=[pltpu.VMEM((ROWS, QUART), BF16), dma((4,))],
        name="finish",
    )(layer_part, influence, score)
    return layer_part.reshape(seqs_n, tok_n, QUART), influence, score


def solution(mesh):
    placed = (
        P(None, "seq", None), P(), P(None, "mp"), P("mp"), P(), P(), P(), P(),
        P("mp", None), P(), P("seq", "mp"), P("seq", "mp"), P("seq", "mp"), P(),
    )
    return jax.shard_map(
        local, mesh=mesh, in_specs=placed,
        out_specs=(P(None, "seq", "mp"), P(None, "seq"), P()), check_vma=False,
    )
```
